32 devices in a mesh: rows: 16 (over z, y, x), cent: 2 (over core).
Axes of the slice: x: 2, y: 2, z: 4, core: 2. Of those that a mesh axis runs over, the one named last changes fastest.
Arguments:
- points: bfloat16 [16384, 1024], P('rows'), may hold values from -8 to 8
- centroids: bfloat16 [4096, 1024], P('cent'), may hold values from -8 to 8
- assign: int32 [16384], P('rows'), may hold values from 0 to 4095, as said below
Outputs:
- nearest: float32 [2, 16384], P(None, 'rows')
- updated: bfloat16 [4096, 1024], P('cent')
The draws below stay inside these ranges and needn't reach their ends.
Inputs may be any that keep to these rules, and one draw needn't show every extreme that they name: `assign`: split the points into aligned blocks of 1024 and the centroids into aligned groups of 128 consecutive ones: in each block at most 64 points are assigned into any one group, and in every block some group takes exactly 64 of them.
All inputs are finite; a program needn't handle non-finite values.
Results may differ from the reference program's by a relative error of at most 0.001.
Values may be sent and summed in bfloat16 or wider, within the bound.
A program may use at most 64 MiB of HBM per device.

```python
import jax
import jax.numpy as jnp
from jax import lax

D = 1024
K = 4096
PTS_DEV = 1024
P_SIZE = 16384
GROUPS = 32
SHARE = 128
CAP = 64


def centroid_field(key):
    key_dir, key_len = jax.random.split(jax.random.fold_in(key, 23), 2)
    raw = jax.random.normal(key_dir, (K, D), jnp.float32)
    length = jax.random.uniform(key_len, (K, 1), jnp.float32, 0.97, 1.03)
    return raw * (length * jnp.sqrt(jnp.float32(D)) / jnp.sqrt(jnp.sum(raw * raw, axis=1, keepdims=True)))


def draw_centroids(key, part):
    return centroid_field(key).astype(jnp.bfloat16)


def draw_points(key, part):
    key_val, key_scale, key_pick = jax.random.split(jax.random.fold_in(key, 37), 3)
    cents = centroid_field(key).astype(jnp.bfloat16).astype(jnp.float32)
    picks = jax.random.randint(key_pick, (P_SIZE,), 0, K)
    noise = jax.random.normal(key_val, (P_SIZE, D), jnp.float32)
    low, high = (0.2, 1.5)
    logs = jax.random.uniform(key_scale, (P_SIZE, 1), jnp.float32, jnp.log(low), jnp.log(high))
    scaled = jnp.clip(jnp.exp(logs) * cents[picks] + 0.3 * noise, -8.0, 8.0)
    return scaled.astype(jnp.bfloat16)


def draw_assign(key, part):
    blocks_total = P_SIZE // PTS_DEV
    key_block, key_order, key_shuffle, key_offset = jax.random.split(jax.random.fold_in(key, 11), 4)
    picked = jax.random.randint(key_block, (blocks_total,), 0, GROUPS)
    slot_group = jnp.repeat(jnp.arange(GROUPS, dtype=jnp.int32), CAP)

    def one_block(index):
        order = jax.random.permutation(jax.random.fold_in(key_order, index), GROUPS * CAP).astype(jnp.int32)
        forced = slot_group == picked[index]
        score = jnp.where(forced, order - GROUPS * CAP, order)
        chosen = slot_group[jnp.argsort(score, stable=True)[:PTS_DEV]]
        mixing = jax.random.permutation(jax.random.fold_in(key_shuffle, index), PTS_DEV)
        return chosen[mixing]
    groups_all = jax.vmap(one_block)(jnp.arange(blocks_total, dtype=jnp.int32))
    offsets = jax.random.randint(key_offset, (blocks_total, PTS_DEV), 0, SHARE)
    return (groups_all * SHARE + offsets).reshape(P_SIZE).astype(jnp.int32)


def setup_inputs(seed: int = 0) -> dict:
    arg_keys = jax.random.split(jax.random.key(seed), 4)
    return {
        "points": draw_points(jax.random.fold_in(arg_keys[3], 71), 0),
        "centroids": draw_centroids(jax.random.fold_in(arg_keys[3], 71), 0),
        "assign": draw_assign(jax.random.fold_in(arg_keys[3], 71), 0),
    }


def smallest(points, pnorm, cents):
    cnorm = jnp.sum(jnp.square(cents.astype(jnp.float32)), axis=1)
    size = P_SIZE
    if P_SIZE % 1024 == 0:
        size = 1024

    def one_block(pair):
        block, norms = pair
        dots = lax.dot_general(block, cents, (((1,), (1,)), ((), ())), preferred_element_type=jnp.float32)
        return jnp.min((norms[:, None] - 2.0 * dots + cnorm[None, :]) / D, axis=1)

    result = lax.map(one_block, (points.reshape(P_SIZE // size, size, D), pnorm.reshape(P_SIZE // size, size)))
    return result.reshape(P_SIZE)


def reference(points, centroids, assign):
    wide = points.astype(jnp.float32)
    pnorm = jnp.sum(jnp.square(wide), axis=1)
    first = smallest(points, pnorm, centroids)
    sums = jax.ops.segment_sum(wide, assign, num_segments=K)
    counts = jax.ops.segment_sum(jnp.ones((P_SIZE,), jnp.float32), assign, num_segments=K)
    updated = ((sums + centroids.astype(jnp.float32)) / (counts[:, None] + 1.0)).astype(jnp.bfloat16)
    second = smallest(points, pnorm, updated)
    return jnp.stack([first, second]), updated
```

```python
import functools

import jax
import jax.numpy as jnp
from jax import lax
from jax.experimental import pallas as pl
from jax.experimental.pallas import tpu as pltpu
from jax.sharding import PartitionSpec as P


def smallest(points, pnorm, cents):
    cnorm = jnp.sum(jnp.square(cents.astype(jnp.float32)), axis=1)
    dots = lax.dot_general(
        points, cents, (((1,), (1,)), ((), ())), preferred_element_type=jnp.float32
    )
    return jnp.min((pnorm[:, None] - 2.0 * dots + cnorm[None, :]) / points.shape[1], axis=1)


def block_min(values):
    return lax.pmin(values, "cent")


def renew(part_sums, part_counts, own_rows):
    return ((part_sums + own_rows.astype(jnp.float32)) / (part_counts[:, None] + 1.0)).astype(
        jnp.bfloat16
    )


def per_device(points, centroids, assign):
    blocksize = centroids.shape[0]
    count_pts = points.shape[0]
    pnorm = jnp.sum(jnp.square(points.astype(jnp.float32)), axis=1)
    first = smallest(points, pnorm, centroids)
    first = block_min(first)
    relative = assign - lax.axis_index("cent") * blocksize
    share = blocksize // lax.axis_size("rows")
    own = lax.dynamic_slice_in_dim(centroids, lax.axis_index("rows") * share, share, 0)
    rows_count = lax.axis_size("rows")
    groups = rows_count * lax.axis_size("cent")
    capacity = max(2, 2 * count_pts // groups)
    inside = (relative >= 0) & (relative < blocksize)
    owners = jnp.where(inside, relative // share, rows_count)
    offsets = jnp.where(inside, relative - relative // share * share, 0)
    owner_hot = owners[:, None] == lax.broadcasted_iota(jnp.int32, (count_pts, rows_count), 1)
    earlier = lax.broadcasted_iota(jnp.int32, (count_pts, count_pts), 1) < lax.broadcasted_iota(
        jnp.int32, (count_pts, count_pts), 0
    )
    before = jnp.dot(
        earlier.astype(jnp.bfloat16),
        owner_hot.astype(jnp.bfloat16),
        preferred_element_type=jnp.float32,
    )
    ranking = jnp.sum(jnp.where(owner_hot, before, 0.0), axis=1).astype(jnp.int32)
    slot_index = jnp.where(inside, owners * capacity + ranking, -1)
    placing = (
        lax.broadcasted_iota(jnp.int32, (rows_count * capacity, count_pts), 0)
        == slot_index[None, :]
    )
    outgoing = jnp.dot(
        placing.astype(jnp.bfloat16), points, preferred_element_type=jnp.float32
    ).astype(jnp.bfloat16)
    labels = (jnp.sum(jnp.where(placing, offsets[None, :] + 1, 0), axis=1) - 1).astype(jnp.bfloat16)
    arrived, arrived_labels = (
        lax.all_to_all(outgoing, "rows", split_axis=0, concat_axis=0, tiled=True),
        lax.all_to_all(labels, "rows", split_axis=0, concat_axis=0, tiled=True),
    )
    chosen = (
        lax.broadcasted_iota(jnp.int32, (share, arrived.shape[0]), 0)
        == arrived_labels.astype(jnp.int32)[None, :]
    )
    part_sums = jnp.dot(chosen.astype(jnp.bfloat16), arrived, preferred_element_type=jnp.float32)
    part_counts = jnp.sum(chosen.astype(jnp.float32), axis=1)
    updated = lax.all_gather(renew(part_sums, part_counts, own), "rows", axis=0, tiled=True)
    second = smallest(points, pnorm, updated)
    nearest = jnp.stack([first, block_min(second)])
    return (nearest, updated)


PLANE = 4
LANES = 128
VMEM_BYTES = 44 * 1024 * 1024
PARTS = 2


def nt_dot(a, b):
    return lax.dot_general(a, b, (((1,), (1,)), ((), ())), preferred_element_type=jnp.float32)


def column_min(cents, points):
    wide = cents.astype(jnp.float32)
    cnorm = jnp.sum(wide * wide, axis=1, keepdims=True)
    return jnp.min(cnorm - 2.0 * nt_dot(cents, points), axis=0, keepdims=True)


def flip(index, bits):
    low, high = index % 2, index // 2
    if bits % 2:
        low = 1 - low
    if bits // 2:
        high = 1 - high
    return high * 2 + low


def lloyd_kernel(
    rows, cap, share, assign_hbm, points_hbm, cents_hbm, near_ref, gath,
    assign_ref, points_ref, cents_ref, load_sem,
    placing_ref, send, lab_send, arrived, lab_arrived, klab,
    part_send, meta_send, part_got, meta_got, acc, mine, theirs, low,
    sent_pts, got_pts, sent_lab, got_lab, sent_part, got_part, sent_meta, got_meta,
    sent_up, sent_down, sent_x, sent_y, got_full, sent_dx, sent_dy, got_dx, got_dy, spare_sem, sent_min, got_min,
):
    count_pts, width = points_ref.shape
    blocksize = cents_ref.shape[0]
    planes = rows // PLANE
    wide = width // PARTS
    chunk = planes * cap
    me = lax.axis_index("rows")
    core = lax.axis_index("cent")
    z, q = me // PLANE, me % PLANE
    xpeer = z * PLANE + flip(q, 1)
    ypeer = z * PLANE + flip(q, 2)
    diag = z * PLANE + flip(q, 3)
    partner = 1 - core

    assign_in = pltpu.make_async_copy(assign_hbm, assign_ref, load_sem.at[2])
    assign_in.start()
    points_in = pltpu.make_async_copy(points_hbm, points_ref, load_sem.at[0])
    points_in.start()
    barrier = pltpu.get_barrier_semaphore()
    for bits in range(1, 4):
        pl.semaphore_signal(barrier, inc=1, device_id={"rows": z * PLANE + flip(q, bits)})
        pl.semaphore_signal(barrier, inc=1, device_id={"rows": flip(z, bits) * PLANE + q})
    pl.semaphore_signal(barrier, inc=1, device_id={"cent": partner})

    assign_in.wait()
    relative = (assign_ref[...] - core * blocksize).astype(jnp.float32)
    inside = (relative >= 0.0) & (relative < float(blocksize))
    owner = jnp.where(inside, jnp.floor(relative * (1.0 / share)), float(rows))
    offset1 = jnp.where(inside, relative - owner * share + 1.0, 0.0)
    hot = lax.broadcasted_iota(jnp.int32, (rows, count_pts), 0).astype(jnp.float32) == owner
    hot_f = jnp.where(hot, 1.0, 0.0)
    seg = 256
    tri = jnp.where(
        lax.broadcasted_iota(jnp.int32, (seg, seg), 0) < lax.broadcasted_iota(jnp.int32, (seg, seg), 1),
        1.0, 0.0,
    ).astype(jnp.bfloat16)
    carry = jnp.zeros((rows, 1), jnp.float32)
    pieces = []
    for s in range(count_pts // seg):
        part = hot_f[:, s * seg:(s + 1) * seg]
        before = jnp.dot(part.astype(jnp.bfloat16), tri, preferred_element_type=jnp.float32) + carry
        pieces.append(jnp.sum(part * before, axis=0, keepdims=True))
        carry = carry + jnp.sum(part, axis=1, keepdims=True)
    ranking = jnp.concatenate(pieces, axis=1)
    plane_to = jnp.floor(owner * (1.0 / PLANE))
    slot = jnp.where(inside, (owner - plane_to * PLANE) * chunk + plane_to * cap + ranking, -1.0)
    labels8 = jnp.broadcast_to(offset1, (8, count_pts)).astype(jnp.bfloat16)

    def ship(src, dst, ss, rs, axis, target):
        copy = pltpu.make_async_remote_copy(
            src_ref=src, dst_ref=dst, send_sem=ss, recv_sem=rs, device_id={axis: target}
        )
        copy.start()
        return copy

    def landed(ref, sem):
        pltpu.make_async_remote_copy(
            src_ref=ref, dst_ref=ref, send_sem=spare_sem.at[0], recv_sem=sem, device_id={"rows": xpeer}
        ).wait_recv()

    flying = []
    reach = (3, 1, 2)
    span = (2, 3, 1)

    def place(k):
        i = flip(q, k)
        hit = (
            lax.broadcasted_iota(jnp.int32, (chunk, count_pts), 0) + i * chunk
        ).astype(jnp.float32) == slot
        placing = jnp.where(hit, 1.0, 0.0).astype(jnp.bfloat16)
        placing_ref[k] = placing
        lab = nt_dot(labels8, placing)
        for t in range(chunk // LANES):
            piece = lab[:, t * LANES:(t + 1) * LANES]
            if k:
                lab_send[k, t] = piece
            else:
                lab_arrived[q, t] = piece

    def fill(h, k):
        rows_out = jnp.dot(
            placing_ref[k], points_ref[:, h * wide:(h + 1) * wide], preferred_element_type=jnp.float32
        ).astype(jnp.bfloat16)
        if k:
            send[h, k] = rows_out
        else:
            for t in range(planes):
                arrived[h, t, pl.ds(pl.multiple_of(q * cap, cap), cap), :] = rows_out[t * cap:(t + 1) * cap]

    def dispatch(h, j):
        t = flip(z, (span + (0,))[j])
        for k in reach:
            spot = pl.ds(pl.multiple_of(q * cap, cap), cap)
            flying.append(ship(
                send.at[h, k, pl.ds(pl.multiple_of(t * cap, cap), cap)], arrived.at[h, t, spot],
                sent_pts.at[h, j, k], got_pts.at[h, t, q], "rows", z * PLANE + flip(q, k),
            ))

    points_in.wait()
    cents_in = pltpu.make_async_copy(cents_hbm, cents_ref, load_sem.at[1])
    cents_in.start()
    for k in reach:
        place(k)
    for k in reach:
        fill(0, k)
    pl.semaphore_wait(barrier, 7)
    for k in reach:
        flying.append(ship(
            lab_send.at[k], lab_arrived.at[q], sent_lab.at[k], got_lab.at[q], "rows", z * PLANE + flip(q, k)
        ))
    for j in range(planes):
        dispatch(0, j)
    for h in range(1, PARTS):
        for k in reach:
            fill(h, k)
        for j in range(planes):
            dispatch(h, j)
    place(0)
    for h in range(PARTS):
        fill(h, 0)

    squares = jnp.square(points_ref[...].astype(jnp.float32))
    high = squares.astype(jnp.bfloat16)
    rest = (squares - high.astype(jnp.float32)).astype(jnp.bfloat16)
    ones = jnp.ones((8, width), jnp.bfloat16)
    pnorm = (nt_dot(ones, high) + nt_dot(ones, rest))[0:1, :]
    cents_in.wait()
    kb = 512
    low[...] = jnp.full(low.shape, jnp.inf, jnp.float32)

    def first_step(i, _):
        block = cents_ref[pl.ds(pl.multiple_of(i * kb, kb), kb), :]
        low[0:1, :] = jnp.minimum(low[0:1, :], column_min(block, points_ref[...]))
        return 0

    lax.fori_loop(0, blocksize // kb, first_step, 0)
    mine[0] = (pnorm + low[0:1, :]) / width
    min_copies = [ship(mine.at[0], theirs.at[0], sent_min.at[0], got_min.at[0], "cent", partner)]
    low[...] = jnp.full(low.shape, jnp.inf, jnp.float32)

    for k in reach:
        landed(lab_arrived.at[flip(q, k)], got_lab.at[flip(q, k)])
    lane = lax.broadcasted_iota(jnp.int32, (8, LANES), 1)
    for t in range(planes):
        for p in range(PLANE // 2):
            left, right = lab_arrived[2 * p, t // 2], lab_arrived[2 * p + 1, t // 2]
            if t % 2:
                left = pltpu.roll(left, cap, 1)
            else:
                right = pltpu.roll(right, cap, 1)
            klab[t, :, p * LANES:(p + 1) * LANES] = jnp.where(lane < cap, left, right)

    rowid1 = lax.broadcasted_iota(jnp.int32, (share, PLANE * cap), 0).astype(jnp.float32) + 1.0
    eye = lax.broadcasted_iota(jnp.int32, (share, LANES), 0) == lax.broadcasted_iota(
        jnp.int32, (share, LANES), 1
    )

    def to_row(column):
        return jnp.sum(jnp.where(eye, column, 0.0), axis=0, keepdims=True)

    def to_column(row):
        return jnp.sum(jnp.where(eye, row, 0.0), axis=1, keepdims=True)

    def gather_in(h, t):
        for k in reach:
            source = flip(q, k)
            landed(arrived.at[h, t, pl.ds(pl.multiple_of(source * cap, cap), cap)], got_pts.at[h, t, source])
        chosen = jnp.where(rowid1 == klab[t][0:1, :], 1.0, 0.0)
        counts = jnp.sum(chosen, axis=1, keepdims=True)
        total = jnp.dot(chosen.astype(jnp.bfloat16), arrived[h, t], preferred_element_type=jnp.float32)
        return total, counts

    def reduce_out(h):
        for j, bits in enumerate(span):
            t = flip(z, bits)
            total, counts = gather_in(h, t)
            peak = jnp.maximum(jnp.max(jnp.abs(total), axis=1, keepdims=True), 1e-30)
            grow = jnp.exp2(14.0 - jnp.floor(jnp.log2(peak)))
            grow = jnp.where(peak * grow >= 32767.0, grow * 0.5, grow)
            scaled = jnp.clip(jnp.round(total * grow), -32767.0, 32767.0)
            part_send[h, j] = scaled.astype(jnp.int32).astype(jnp.int16)
            first_row = lax.broadcasted_iota(jnp.int32, (8, LANES), 0) == 0
            meta_send[h, j] = jnp.where(first_row, to_row(1.0 / grow), to_row(counts))
            target = t * PLANE + q
            flying.append(ship(
                meta_send.at[h, j], meta_got.at[h, z], sent_meta.at[h, j], got_meta.at[h, z], "rows", target
            ))
            flying.append(ship(
                part_send.at[h, j], part_got.at[h, z], sent_part.at[h, j], got_part.at[h, z], "rows", target
            ))

    def renew_own(h):
        total, counts = gather_in(h, z)
        own_rows = cents_ref[pl.ds(pl.multiple_of(me * share, share), share), h * wide:(h + 1) * wide]
        acc[...] = total + own_rows.astype(jnp.float32)
        for bits in (1, 2, 3):
            t = flip(z, bits)
            landed(meta_got.at[h, t], got_meta.at[h, t])
            landed(part_got.at[h, t], got_part.at[h, t])
            meta = meta_got[h, t]
            counts = counts + to_column(meta[1:2, :])
            acc[...] += part_got[h, t].astype(jnp.int32).astype(jnp.float32) * to_column(meta[0:1, :])
        gath[me, :, h * wide:(h + 1) * wide] = (acc[...] / (counts + 1.0)).astype(jnp.bfloat16)

    half = share // 2
    upper, lower = pl.ds(0, half), pl.ds(half, half)
    top = z // 2
    visits = [z, z + 1 - 2 * (z % 2), 2 - top, 3 - 3 * top]
    climbs = []
    waiting = []

    def view(block, h, part=slice(None)):
        return gath.at[block, part, h * wide:(h + 1) * wide]

    def pass_on(h, block, n):
        for sem, target in ((sent_x, xpeer), (sent_y, ypeer)):
            flying.append(ship(view(block, h), view(block, h), sem.at[h, n], got_full.at[h, block], "rows", target))

    def climb(h, block, n, upward, downward):
        for allowed, sems, toward in ((upward, sent_up, PLANE), (downward, sent_down, -PLANE)):
            @pl.when(allowed)
            def _(sems=sems, toward=toward):
                ship(view(block, h), view(block, h), sems.at[h, n], got_full.at[h, block], "rows", me + toward)
            climbs.append((h, block, n, allowed, sems, toward))

    def await_full(h, block):
        landed(view(block, h), got_full.at[h, block])

    def absorb(h, *blocks):
        if h < PARTS - 1:
            return
        waiting.extend(blocks)
        while len(waiting) >= 2:
            drain(2)

    def drain(n):
        taken, waiting[:] = waiting[:n], waiting[n:]
        block = jnp.concatenate([gath[b] for b in taken], axis=0) if n > 1 else gath[taken[0]]
        low[0:1, :] = jnp.minimum(low[0:1, :], column_min(block, points_ref[...]))

    def cross(h, n):
        by, bx = visits[n] * PLANE + ypeer % PLANE, visits[n] * PLANE + xpeer % PLANE
        await_full(h, by)
        flying.append(ship(
            view(by, h, upper), view(by, h, upper), sent_dx.at[h, n], got_dx.at[h, by], "rows", xpeer
        ))
        await_full(h, bx)
        flying.append(ship(
            view(bx, h, lower), view(bx, h, lower), sent_dy.at[h, n], got_dy.at[h, bx], "rows", ypeer
        ))
        return by, bx

    def spread_start(h):
        climb(h, me, 0, z < planes - 1, z > 0)
        pass_on(h, me, 0)
        absorb(h, me)

    def spread_step(h, n):
        zs = visits[n]
        block = zs * PLANE + q
        await_full(h, block)
        climb(h, block, n, (zs < z) & (z < planes - 1), (zs > z) & (z > 0))
        pass_on(h, block, n)
        ready = cross(h, n - 1)
        absorb(h, block, *ready)

    def spread_end(h):
        absorb(h, *cross(h, planes - 1))

    def spread_rest(h):
        for zs in visits:
            bd = zs * PLANE + diag % PLANE
            landed(view(bd, h, upper), got_dx.at[h, bd])
            landed(view(bd, h, lower), got_dy.at[h, bd])
            absorb(h, bd)

    reduce_out(0)
    renew_own(0)
    spread_start(0)
    if PARTS == 1:
        for n in range(1, planes):
            spread_step(0, n)
        spread_end(0)
    else:
        reduce_out(1)
        spread_step(0, 1)
        renew_own(1)
        spread_start(1)
        spread_step(0, 2)
        spread_step(1, 1)
        spread_step(0, 3)
        spread_step(1, 2)
        spread_end(0)
        spread_step(1, 3)
        spread_rest(0)
        spread_end(1)
    spread_rest(PARTS - 1)
    if waiting:
        drain(len(waiting))

    mine[1] = (pnorm + low[0:1, :]) / width
    min_copies.append(ship(mine.at[1], theirs.at[1], sent_min.at[1], got_min.at[1], "cent", partner))
    for copy in flying:
        copy.wait_send()
    for h, block, n, allowed, sems, toward in climbs:
        @pl.when(allowed)
        def _(h=h, block=block, n=n, sems=sems, toward=toward):
            pltpu.make_async_remote_copy(
                src_ref=view(block, h), dst_ref=view(block, h), send_sem=sems.at[h, n],
                recv_sem=got_full.at[h, block], device_id={"rows": me + toward},
            ).wait_send()
    for n, copy in enumerate(min_copies):
        copy.wait()
        near_ref[n:n + 1, :] = jnp.minimum(mine[n], theirs[n])


def deliver(near_ref, gath_ref, near_out, upd_out, sems):
    copies = [
        pltpu.make_async_copy(gath_ref, upd_out, sems.at[0]),
        pltpu.make_async_copy(near_ref, near_out, sems.at[1]),
    ]
    for copy in copies:
        copy.start()
    for copy in copies:
        copy.wait()


def fused(points, centroids, assign, rows, cap, share):
    count_pts, width = points.shape
    planes = rows // PLANE
    hbm = pl.BlockSpec(memory_space=pltpu.HBM)
    vmem = pl.BlockSpec(memory_space=pltpu.VMEM)
    dma = pltpu.SemaphoreType.DMA
    chunk = planes * cap
    wide = width // PARTS
    shapes = (
        jax.ShapeDtypeStruct((2, count_pts), jnp.float32),
        jax.ShapeDtypeStruct((rows, share, width), jnp.bfloat16),
    )
    hops = planes - 1
    near, upd = pl.pallas_call(
        functools.partial(lloyd_kernel, rows, cap, share),
        out_shape=shapes,
        in_specs=[hbm, hbm, hbm],
        out_specs=(vmem, vmem),
        scratch_shapes=[
            pltpu.VMEM((1, count_pts), jnp.int32),
            pltpu.VMEM((count_pts, width), jnp.bfloat16),
            pltpu.VMEM(centroids.shape, jnp.bfloat16),
            dma((3,)),
            pltpu.VMEM((PLANE, chunk, count_pts), jnp.bfloat16),
            pltpu.VMEM((PARTS, PLANE, chunk, wide), jnp.bfloat16),
            pltpu.VMEM((PLANE, chunk // LANES, 8, LANES), jnp.float32),
            pltpu.VMEM((PARTS, planes, PLANE * cap, wide), jnp.bfloat16),
            pltpu.VMEM((PLANE, chunk // LANES, 8, LANES), jnp.float32),
            pltpu.VMEM((planes, 8, PLANE * cap), jnp.float32),
            pltpu.VMEM((PARTS, hops, share, wide), jnp.int16),
            pltpu.VMEM((PARTS, hops, 8, LANES), jnp.float32),
            pltpu.VMEM((PARTS, planes, share, wide), jnp.int16),
            pltpu.VMEM((PARTS, planes, 8, LANES), jnp.float32),
            pltpu.VMEM((share, wide), jnp.float32),
            pltpu.VMEM((2, 1, count_pts), jnp.float32),
            pltpu.VMEM((2, 1, count_pts), jnp.float32),
            pltpu.VMEM((8, count_pts), jnp.float32),
            dma((PARTS, planes, PLANE)), dma((PARTS, planes, PLANE)), dma((PLANE,)), dma((PLANE,)),
            dma((PARTS, hops)), dma((PARTS, planes)), dma((PARTS, hops)), dma((PARTS, planes)),
            dma((PARTS, planes)), dma((PARTS, planes)), dma((PARTS, planes)), dma((PARTS, planes)),
            dma((PARTS, rows)),
            dma((PARTS, planes)), dma((PARTS, planes)), dma((PARTS, rows)), dma((PARTS, rows)), dma((1,)),
            dma((2,)), dma((2,)),
        ],
        compiler_params=pltpu.CompilerParams(
            collective_id=0, has_side_effects=True, vmem_limit_bytes=VMEM_BYTES
        ),
    )(assign[None, :], points, centroids)
    near, upd = pl.pallas_call(
        deliver,
        out_shape=shapes,
        in_specs=[vmem, vmem],
        out_specs=(hbm, hbm),
        scratch_shapes=[dma((2,))],
    )(near, upd)
    return near, upd.reshape(rows * share, width)


def step(rows, cent, points, centroids, assign):
    count_pts = points.shape[0]
    blocksize = centroids.shape[0]
    share = blocksize // rows
    cap = max(2, 2 * count_pts // (rows * cent))
    fits = cent == 2 and rows == 4 * PLANE and share == LANES and 2 * cap == LANES
    even = count_pts % 256 == 0 and blocksize % 512 == 0 and points.shape[1] % (PARTS * LANES) == 0
    if fits and even:
        return fused(points, centroids, assign, rows, cap, share)
    return per_device(points, centroids, assign)


def solution(mesh):
    return jax.shard_map(
        functools.partial(step, mesh.shape["rows"], mesh.shape["cent"]),
        mesh=mesh,
        in_specs=(P("rows", None), P("cent", None), P("rows")),
        out_specs=(P(None, "rows"), P("cent", None)),
        check_vma=False,
    )
```

```python
import functools

import jax
import jax.numpy as jnp
from jax import lax
from jax.experimental import pallas as pl
from jax.experimental.pallas import tpu as pltpu
from jax.sharding import PartitionSpec as P


def smallest(points, pnorm, cents):
    cnorm = jnp.sum(jnp.square(cents.astype(jnp.float32)), axis=1)
    dots = lax.dot_general(
        points, cents, (((1,), (1,)), ((), ())), preferred_element_type=jnp.float32
    )
    return jnp.min((pnorm[:, None] - 2.0 * dots + cnorm[None, :]) / points.shape[1], axis=1)


def block_min(values):
    return lax.pmin(values, "cent")


def renew(part_sums, part_counts, own_rows):
    return ((part_sums + own_rows.astype(jnp.float32)) / (part_counts[:, None] + 1.0)).astype(
        jnp.bfloat16
    )


def per_device(points, centroids, assign):
    blocksize = centroids.shape[0]
    count_pts = points.shape[0]
    pnorm = jnp.sum(jnp.square(points.astype(jnp.float32)), axis=1)
    first = smallest(points, pnorm, centroids)
    first = block_min(first)
    relative = assign - lax.axis_index("cent") * blocksize
    share = blocksize // lax.axis_size("rows")
    own = lax.dynamic_slice_in_dim(centroids, lax.axis_index("rows") * share, share, 0)
    rows_count = lax.axis_size("rows")
    groups = rows_count * lax.axis_size("cent")
    capacity = max(2, 2 * count_pts // groups)
    inside = (relative >= 0) & (relative < blocksize)
    owners = jnp.where(inside, relative // share, rows_count)
    offsets = jnp.where(inside, relative - relative // share * share, 0)
    owner_hot = owners[:, None] == lax.broadcasted_iota(jnp.int32, (count_pts, rows_count), 1)
    earlier = lax.broadcasted_iota(jnp.int32, (count_pts, count_pts), 1) < lax.broadcasted_iota(
        jnp.int32, (count_pts, count_pts), 0
    )
    before = jnp.dot(
        earlier.astype(jnp.bfloat16),
        owner_hot.astype(jnp.bfloat16),
        preferred_element_type=jnp.float32,
    )
    ranking = jnp.sum(jnp.where(owner_hot, before, 0.0), axis=1).astype(jnp.int32)
    slot_index = jnp.where(inside, owners * capacity + ranking, -1)
    placing = (
        lax.broadcasted_iota(jnp.int32, (rows_count * capacity, count_pts), 0)
        == slot_index[None, :]
    )
    outgoing = jnp.dot(
        placing.astype(jnp.bfloat16), points, preferred_element_type=jnp.float32
    ).astype(jnp.bfloat16)
    labels = (jnp.sum(jnp.where(placing, offsets[None, :] + 1, 0), axis=1) - 1).astype(jnp.bfloat16)
    arrived, arrived_labels = (
        lax.all_to_all(outgoing, "rows", split_axis=0, concat_axis=0, tiled=True),
        lax.all_to_all(labels, "rows", split_axis=0, concat_axis=0, tiled=True),
    )
    chosen = (
        lax.broadcasted_iota(jnp.int32, (share, arrived.shape[0]), 0)
        == arrived_labels.astype(jnp.int32)[None, :]
    )
    part_sums = jnp.dot(chosen.astype(jnp.bfloat16), arrived, preferred_element_type=jnp.float32)
    part_counts = jnp.sum(chosen.astype(jnp.float32), axis=1)
    updated = lax.all_gather(renew(part_sums, part_counts, own), "rows", axis=0, tiled=True)
    second = smallest(points, pnorm, updated)
    nearest = jnp.stack([first, block_min(second)])
    return (nearest, updated)


PLANE = 4
LANES = 128
VMEM_BYTES = 44 * 1024 * 1024
PARTS = 2


def nt_dot(a, b):
    return lax.dot_general(a, b, (((1,), (1,)), ((), ())), preferred_element_type=jnp.float32)


def column_min(cents, points):
    wide = cents.astype(jnp.float32)
    cnorm = jnp.sum(wide * wide, axis=1, keepdims=True)
    return jnp.min(cnorm - 2.0 * nt_dot(cents, points), axis=0, keepdims=True)


def flip(index, bits):
    low, high = index % 2, index // 2
    if bits % 2:
        low = 1 - low
    if bits // 2:
        high = 1 - high
    return high * 2 + low


def lloyd_kernel(
    rows, cap, share, assign_hbm, points_hbm, cents_hbm, near_ref, gath,
    assign_ref, points_ref, cents_ref, load_sem,
    placing_ref, send, lab_send, arrived, lab_arrived, klab,
    part_send, meta_send, part_got, meta_got, acc, mine, theirs, low,
    sent_pts, got_pts, sent_lab, got_lab, sent_part, got_part, sent_meta, got_meta,
    sent_up, sent_down, sent_x, sent_y, got_full, sent_dx, sent_dy, got_dx, got_dy, spare_sem, sent_min, got_min,
):
    count_pts, width = points_ref.shape
    blocksize = cents_ref.shape[0]
    planes = rows // PLANE
    wide = width // PARTS
    chunk = planes * cap
    me = lax.axis_index("rows")
    core = lax.axis_index("cent")
    z, q = me // PLANE, me % PLANE
    xpeer = z * PLANE + flip(q, 1)
    ypeer = z * PLANE + flip(q, 2)
    diag = z * PLANE + flip(q, 3)
    partner = 1 - core

    assign_in = pltpu.make_async_copy(assign_hbm, assign_ref, load_sem.at[2])
    assign_in.start()
    points_in = pltpu.make_async_copy(points_hbm, points_ref, load_sem.at[0])
    points_in.start()
    barrier = pltpu.get_barrier_semaphore()
    for bits in range(1, 4):
        pl.semaphore_signal(barrier, inc=1, device_id={"rows": z * PLANE + flip(q, bits)})
        pl.semaphore_signal(barrier, inc=1, device_id={"rows": flip(z, bits) * PLANE + q})
    pl.semaphore_signal(barrier, inc=1, device_id={"cent": partner})

    assign_in.wait()
    relative = (assign_ref[...] - core * blocksize).astype(jnp.float32)
    inside = (relative >= 0.0) & (relative < float(blocksize))
    owner = jnp.where(inside, jnp.floor(relative * (1.0 / share)), float(rows))
    offset1 = jnp.where(inside, relative - owner * share + 1.0, 0.0)
    hot = lax.broadcasted_iota(jnp.int32, (rows, count_pts), 0).astype(jnp.float32) == owner
    hot_f = jnp.where(hot, 1.0, 0.0)
    seg = 256
    tri = jnp.where(
        lax.broadcasted_iota(jnp.int32, (seg, seg), 0) < lax.broadcasted_iota(jnp.int32, (seg, seg), 1),
        1.0, 0.0,
    ).astype(jnp.bfloat16)
    carry = jnp.zeros((rows, 1), jnp.float32)
    pieces = []
    for s in range(count_pts // seg):
        part = hot_f[:, s * seg:(s + 1) * seg]
        before = jnp.dot(part.astype(jnp.bfloat16), tri, preferred_element_type=jnp.float32) + carry
        pieces.append(jnp.sum(part * before, axis=0, keepdims=True))
        carry = carry + jnp.sum(part, axis=1, keepdims=True)
    ranking = jnp.concatenate(pieces, axis=1)
    plane_to = jnp.floor(owner * (1.0 / PLANE))
    slot = jnp.where(inside, (owner - plane_to * PLANE) * chunk + plane_to * cap + ranking, -1.0)
    labels8 = jnp.broadcast_to(offset1, (8, count_pts)).astype(jnp.bfloat16)

    def ship(src, dst, ss, rs, axis, target):
        copy = pltpu.make_async_remote_copy(
            src_ref=src, dst_ref=dst, send_sem=ss, recv_sem=rs, device_id={axis: target}
        )
        copy.start()
        return copy

    def landed(ref, sem):
        pltpu.make_async_remote_copy(
            src_ref=ref, dst_ref=ref, send_sem=spare_sem.at[0], recv_sem=sem, device_id={"rows": xpeer}
        ).wait_recv()

    flying = []
    reach = (3, 1, 2)
    span = (2, 3, 1)

    def place(k):
        i = flip(q, k)
        hit = (
            lax.broadcasted_iota(jnp.int32, (chunk, count_pts), 0) + i * chunk
        ).astype(jnp.float32) == slot
        placing = jnp.where(hit, 1.0, 0.0).astype(jnp.bfloat16)
        placing_ref[k] = placing
        lab = nt_dot(labels8, placing)
        for t in range(chunk // LANES):
            piece = lab[:, t * LANES:(t + 1) * LANES]
            if k:
                lab_send[k, t] = piece
            else:
                lab_arrived[q, t] = piece

    def fill(h, k):
        rows_out = jnp.dot(
            placing_ref[k], points_ref[:, h * wide:(h + 1) * wide], preferred_element_type=jnp.float32
        ).astype(jnp.bfloat16)
        if k:
            send[h, k] = rows_out
        else:
            for t in range(planes):
                arrived[h, t, pl.ds(pl.multiple_of(q * cap, cap), cap), :] = rows_out[t * cap:(t + 1) * cap]

    def dispatch(h, j, k):
        t = flip(z, (span + (0,))[j])
        spot = pl.ds(pl.multiple_of(q * cap, cap), cap)
        flying.append(ship(
            send.at[h, k, pl.ds(pl.multiple_of(t * cap, cap), cap)], arrived.at[h, t, spot],
            sent_pts.at[h, j, k], got_pts.at[h, t, q], "rows", z * PLANE + flip(q, k),
        ))

    points_in.wait()
    cents_in = pltpu.make_async_copy(cents_hbm, cents_ref, load_sem.at[1])
    cents_in.start()
    for k in reach:
        place(k)
        fill(0, k)
        if k == reach[0]:
            pl.semaphore_wait(barrier, 7)
        flying.append(ship(
            lab_send.at[k], lab_arrived.at[q], sent_lab.at[k], got_lab.at[q], "rows", z * PLANE + flip(q, k)
        ))
        for j in range(planes // 2):
            dispatch(0, j, k)
    for j in range(planes // 2, planes):
        for k in reach:
            dispatch(0, j, k)
    for h in range(1, PARTS):
        for k in reach:
            fill(h, k)
        for j in range(planes):
            for k in reach:
                dispatch(h, j, k)
    place(0)
    for h in range(PARTS):
        fill(h, 0)

    kb = 512
    pieces_first = blocksize // kb
    low[...] = jnp.full(low.shape, jnp.inf, jnp.float32)
    min_copies = []

    def first_piece(i):
        low[0:1, :] = jnp.minimum(low[0:1, :], column_min(cents_ref[i * kb:(i + 1) * kb, :], points_ref[...]))

    def point_norms():
        squares = jnp.square(points_ref[...].astype(jnp.float32))
        high = squares.astype(jnp.bfloat16)
        rest = (squares - high.astype(jnp.float32)).astype(jnp.bfloat16)
        ones = jnp.ones((8, width), jnp.bfloat16)
        return (nt_dot(ones, high) + nt_dot(ones, rest))[0:1, :]

    for k in reach:
        landed(lab_arrived.at[flip(q, k)], got_lab.at[flip(q, k)])
    lane = lax.broadcasted_iota(jnp.int32, (8, LANES), 1)
    for t in range(planes):
        for p in range(PLANE // 2):
            left, right = lab_arrived[2 * p, t // 2], lab_arrived[2 * p + 1, t // 2]
            if t % 2:
                left = pltpu.roll(left, cap, 1)
            else:
                right = pltpu.roll(right, cap, 1)
            klab[t, :, p * LANES:(p + 1) * LANES] = jnp.where(lane < cap, left, right)

    rowid1 = lax.broadcasted_iota(jnp.int32, (share, PLANE * cap), 0).astype(jnp.float32) + 1.0
    eye = lax.broadcasted_iota(jnp.int32, (share, LANES), 0) == lax.broadcasted_iota(
        jnp.int32, (share, LANES), 1
    )

    def to_row(column):
        return jnp.sum(jnp.where(eye, column, 0.0), axis=0, keepdims=True)

    def to_column(row):
        return jnp.sum(jnp.where(eye, row, 0.0), axis=1, keepdims=True)

    def gather_in(h, t):
        for k in reach:
            source = flip(q, k)
            landed(arrived.at[h, t, pl.ds(pl.multiple_of(source * cap, cap), cap)], got_pts.at[h, t, source])
        chosen = jnp.where(rowid1 == klab[t][0:1, :], 1.0, 0.0)
        counts = jnp.sum(chosen, axis=1, keepdims=True)
        total = jnp.dot(chosen.astype(jnp.bfloat16), arrived[h, t], preferred_element_type=jnp.float32)
        return total, counts

    def reduce_out(h, j):
        t = flip(z, span[j])
        total, counts = gather_in(h, t)
        peak = jnp.maximum(jnp.max(jnp.abs(total), axis=1, keepdims=True), 1e-30)
        grow = jnp.exp2(14.0 - jnp.floor(jnp.log2(peak)))
        grow = jnp.where(peak * grow >= 32767.0, grow * 0.5, grow)
        scaled = jnp.clip(jnp.round(total * grow), -32767.0, 32767.0)
        part_send[h, j] = scaled.astype(jnp.int32).astype(jnp.int16)
        first_row = lax.broadcasted_iota(jnp.int32, (8, LANES), 0) == 0
        meta_send[h, j] = jnp.where(first_row, to_row(1.0 / grow), to_row(counts))
        target = t * PLANE + q
        flying.append(ship(
            meta_send.at[h, j], meta_got.at[h, z], sent_meta.at[h, j], got_meta.at[h, z], "rows", target
        ))
        flying.append(ship(
            part_send.at[h, j], part_got.at[h, z], sent_part.at[h, j], got_part.at[h, z], "rows", target
        ))

    def reduce_own(h):
        total, counts = gather_in(h, z)
        own_rows = cents_ref[pl.ds(pl.multiple_of(me * share, share), share), h * wide:(h + 1) * wide]
        acc[h] = total + own_rows.astype(jnp.float32)
        return counts

    def renew_own(h, counts):
        for bits in (1, 2, 3):
            t = flip(z, bits)
            landed(meta_got.at[h, t], got_meta.at[h, t])
            landed(part_got.at[h, t], got_part.at[h, t])
            meta = meta_got[h, t]
            counts = counts + to_column(meta[1:2, :])
            acc[h] += part_got[h, t].astype(jnp.int32).astype(jnp.float32) * to_column(meta[0:1, :])
        gath[me, :, h * wide:(h + 1) * wide] = (acc[h] / (counts + 1.0)).astype(jnp.bfloat16)

    half = share // 2
    upper, lower = pl.ds(0, half), pl.ds(half, half)
    top = z // 2
    visits = [z, z + 1 - 2 * (z % 2), 2 - top, 3 - 3 * top]
    climbs = []
    waiting = []

    def view(block, h, part=slice(None)):
        return gath.at[block, part, h * wide:(h + 1) * wide]

    def pass_on(h, block, n):
        for sem, target in ((sent_x, xpeer), (sent_y, ypeer)):
            flying.append(ship(view(block, h), view(block, h), sem.at[h, n], got_full.at[h, block], "rows", target))

    def climb(h, block, n, upward, downward):
        for allowed, sems, toward in ((upward, sent_up, PLANE), (downward, sent_down, -PLANE)):
            @pl.when(allowed)
            def _(sems=sems, toward=toward):
                ship(view(block, h), view(block, h), sems.at[h, n], got_full.at[h, block], "rows", me + toward)
            climbs.append((h, block, n, allowed, sems, toward))

    def await_full(h, block):
        landed(view(block, h), got_full.at[h, block])

    def absorb(h, *blocks):
        if h < PARTS - 1:
            return
        waiting.extend(blocks)
        while len(waiting) >= 2:
            drain(2)

    def drain(n):
        taken, waiting[:] = waiting[:n], waiting[n:]
        block = jnp.concatenate([gath[b] for b in taken], axis=0) if n > 1 else gath[taken[0]]
        low[1:2, :] = jnp.minimum(low[1:2, :], column_min(block, points_ref[...]))

    def cross(h, n):
        by, bx = visits[n] * PLANE + ypeer % PLANE, visits[n] * PLANE + xpeer % PLANE
        await_full(h, by)
        flying.append(ship(
            view(by, h, upper), view(by, h, upper), sent_dx.at[h, n], got_dx.at[h, by], "rows", xpeer
        ))
        await_full(h, bx)
        flying.append(ship(
            view(bx, h, lower), view(bx, h, lower), sent_dy.at[h, n], got_dy.at[h, bx], "rows", ypeer
        ))
        return by, bx

    def spread_start(h):
        climb(h, me, 0, z < planes - 1, z > 0)
        pass_on(h, me, 0)
        absorb(h, me)

    def spread_step(h, n):
        zs = visits[n]
        block = zs * PLANE + q
        await_full(h, block)
        climb(h, block, n, (zs < z) & (z < planes - 1), (zs > z) & (z > 0))
        pass_on(h, block, n)
        ready = cross(h, n - 1)
        absorb(h, block, *ready)

    def spread_end(h):
        absorb(h, *cross(h, planes - 1))

    def spread_rest(h):
        for zs in visits:
            bd = zs * PLANE + diag % PLANE
            landed(view(bd, h, upper), got_dx.at[h, bd])
            landed(view(bd, h, lower), got_dy.at[h, bd])
            absorb(h, bd)

    cents_in.wait()
    for j in range(planes - 1):
        reduce_out(0, j)
        first_piece(j)
    counts = reduce_own(0)
    for i in range(planes - 1, pieces_first):
        first_piece(i)
    reduce_out(1, 0)
    renew_own(0, counts)
    spread_start(0)
    reduce_out(1, 1)
    pnorm = point_norms()
    mine[0] = (pnorm + low[0:1, :]) / width
    min_copies.append(ship(mine.at[0], theirs.at[0], sent_min.at[0], got_min.at[0], "cent", partner))
    reduce_out(1, 2)
    spread_step(0, 1)
    counts = reduce_own(1)
    renew_own(1, counts)
    spread_start(1)
    spread_step(0, 2)
    spread_step(1, 1)
    spread_step(0, 3)
    spread_step(1, 2)
    spread_end(0)
    spread_step(1, 3)
    spread_rest(0)
    spread_end(1)
    spread_rest(1)
    if waiting:
        drain(len(waiting))

    mine[1] = (pnorm + low[1:2, :]) / width
    min_copies.append(ship(mine.at[1], theirs.at[1], sent_min.at[1], got_min.at[1], "cent", partner))
    for copy in flying:
        copy.wait_send()
    for h, block, n, allowed, sems, toward in climbs:
        @pl.when(allowed)
        def _(h=h, block=block, n=n, sems=sems, toward=toward):
            pltpu.make_async_remote_copy(
                src_ref=view(block, h), dst_ref=view(block, h), send_sem=sems.at[h, n],
                recv_sem=got_full.at[h, block], device_id={"rows": me + toward},
            ).wait_send()
    for n, copy in enumerate(min_copies):
        copy.wait()
        near_ref[n:n + 1, :] = jnp.minimum(mine[n], theirs[n])


def deliver(near_ref, gath_ref, near_out, upd_out, sems):
    copies = [
        pltpu.make_async_copy(gath_ref, upd_out, sems.at[0]),
        pltpu.make_async_copy(near_ref, near_out, sems.at[1]),
    ]
    for copy in copies:
        copy.start()
    for copy in copies:
        copy.wait()


def fused(points, centroids, assign, rows, cap, share):
    count_pts, width = points.shape
    planes = rows // PLANE
    hbm = pl.BlockSpec(memory_space=pltpu.HBM)
    vmem = pl.BlockSpec(memory_space=pltpu.VMEM)
    dma = pltpu.SemaphoreType.DMA
    chunk = planes * cap
    wide = width // PARTS
    shapes = (
        jax.ShapeDtypeStruct((2, count_pts), jnp.float32),
        jax.ShapeDtypeStruct((rows, share, width), jnp.bfloat16),
    )
    hops = planes - 1
    near, upd = pl.pallas_call(
        functools.partial(lloyd_kernel, rows, cap, share),
        out_shape=shapes,
        in_specs=[hbm, hbm, hbm],
        out_specs=(vmem, vmem),
        scratch_shapes=[
            pltpu.VMEM((1, count_pts), jnp.int32),
            pltpu.VMEM((count_pts, width), jnp.bfloat16),
            pltpu.VMEM(centroids.shape, jnp.bfloat16),
            dma((3,)),
            pltpu.VMEM((PLANE, chunk, count_pts), jnp.bfloat16),
            pltpu.VMEM((PARTS, PLANE, chunk, wide), jnp.bfloat16),
            pltpu.VMEM((PLANE, chunk // LANES, 8, LANES), jnp.float32),
            pltpu.VMEM((PARTS, planes, PLANE * cap, wide), jnp.bfloat16),
            pltpu.VMEM((PLANE, chunk // LANES, 8, LANES), jnp.float32),
            pltpu.VMEM((planes, 8, PLANE * cap), jnp.float32),
            pltpu.VMEM((PARTS, hops, share, wide), jnp.int16),
            pltpu.VMEM((PARTS, hops, 8, LANES), jnp.float32),
            pltpu.VMEM((PARTS, planes, share, wide), jnp.int16),
            pltpu.VMEM((PARTS, planes, 8, LANES), jnp.float32),
            pltpu.VMEM((PARTS, share, wide), jnp.float32),
            pltpu.VMEM((2, 1, count_pts), jnp.float32),
            pltpu.VMEM((2, 1, count_pts), jnp.float32),
            pltpu.VMEM((8, count_pts), jnp.float32),
            dma((PARTS, planes, PLANE)), dma((PARTS, planes, PLANE)), dma((PLANE,)), dma((PLANE,)),
            dma((PARTS, hops)), dma((PARTS, planes)), dma((PARTS, hops)), dma((PARTS, planes)),
            dma((PARTS, planes)), dma((PARTS, planes)), dma((PARTS, planes)), dma((PARTS, planes)),
            dma((PARTS, rows)),
            dma((PARTS, planes)), dma((PARTS, planes)), dma((PARTS, rows)), dma((PARTS, rows)), dma((1,)),
            dma((2,)), dma((2,)),
        ],
        compiler_params=pltpu.CompilerParams(
            collective_id=0, has_side_effects=True, vmem_limit_bytes=VMEM_BYTES
        ),
    )(
        pltpu.with_memory_space_constraint(assign[None, :], pltpu.HBM),
        pltpu.with_memory_space_constraint(points, pltpu.HBM),
        pltpu.with_memory_space_constraint(centroids, pltpu.HBM),
    )
    near, upd = pl.pallas_call(
        deliver,
        out_shape=shapes,
        in_specs=[vmem, vmem],
        out_specs=(hbm, hbm),
        scratch_shapes=[dma((2,))],
        compiler_params=pltpu.CompilerParams(vmem_limit_bytes=1024 * 1024),
    )(near, upd)
    return near, upd.reshape(rows * share, width)


def step(rows, cent, points, centroids, assign):
    count_pts = points.shape[0]
    blocksize = centroids.shape[0]
    share = blocksize // rows
    cap = max(2, 2 * count_pts // (rows * cent))
    fits = cent == 2 and rows == 4 * PLANE and share == LANES and 2 * cap == LANES
    even = count_pts % 256 == 0 and blocksize % 512 == 0 and points.shape[1] % (PARTS * LANES) == 0
    if fits and even:
        return fused(points, centroids, assign, rows, cap, share)
    return per_device(points, centroids, assign)


def solution(mesh):
    return jax.shard_map(
        functools.partial(step, mesh.shape["rows"], mesh.shape["cent"]),
        mesh=mesh,
        in_specs=(P("rows", None), P("cent", None), P("rows")),
        out_specs=(P(None, "rows"), P("cent", None)),
        check_vma=False,
    )
```

```python
import functools

import jax
import jax.numpy as jnp
from jax import lax
from jax.experimental import pallas as pl
from jax.experimental.pallas import tpu as pltpu
from jax.sharding import PartitionSpec as P


def smallest(points, pnorm, cents):
    cnorm = jnp.sum(jnp.square(cents.astype(jnp.float32)), axis=1)
    dots = lax.dot_general(
        points, cents, (((1,), (1,)), ((), ())), preferred_element_type=jnp.float32
    )
    return jnp.min((pnorm[:, None] - 2.0 * dots + cnorm[None, :]) / points.shape[1], axis=1)


def block_min(values):
    return lax.pmin(values, "cent")


def renew(part_sums, part_counts, own_rows):
    return ((part_sums + own_rows.astype(jnp.float32)) / (part_counts[:, None] + 1.0)).astype(
        jnp.bfloat16
    )


def per_device(points, centroids, assign):
    blocksize = centroids.shape[0]
    count_pts = points.shape[0]
    pnorm = jnp.sum(jnp.square(points.astype(jnp.float32)), axis=1)
    first = smallest(points, pnorm, centroids)
    first = block_min(first)
    relative = assign - lax.axis_index("cent") * blocksize
    share = blocksize // lax.axis_size("rows")
    own = lax.dynamic_slice_in_dim(centroids, lax.axis_index("rows") * share, share, 0)
    rows_count = lax.axis_size("rows")
    groups = rows_count * lax.axis_size("cent")
    capacity = max(2, 2 * count_pts // groups)
    inside = (relative >= 0) & (relative < blocksize)
    owners = jnp.where(inside, relative // share, rows_count)
    offsets = jnp.where(inside, relative - relative // share * share, 0)
    owner_hot = owners[:, None] == lax.broadcasted_iota(jnp.int32, (count_pts, rows_count), 1)
    earlier = lax.broadcasted_iota(jnp.int32, (count_pts, count_pts), 1) < lax.broadcasted_iota(
        jnp.int32, (count_pts, count_pts), 0
    )
    before = jnp.dot(
        earlier.astype(jnp.bfloat16),
        owner_hot.astype(jnp.bfloat16),
        preferred_element_type=jnp.float32,
    )
    ranking = jnp.sum(jnp.where(owner_hot, before, 0.0), axis=1).astype(jnp.int32)
    slot_index = jnp.where(inside, owners * capacity + ranking, -1)
    placing = (
        lax.broadcasted_iota(jnp.int32, (rows_count * capacity, count_pts), 0)
        == slot_index[None, :]
    )
    outgoing = jnp.dot(
        placing.astype(jnp.bfloat16), points, preferred_element_type=jnp.float32
    ).astype(jnp.bfloat16)
    labels = (jnp.sum(jnp.where(placing, offsets[None, :] + 1, 0), axis=1) - 1).astype(jnp.bfloat16)
    arrived, arrived_labels = (
        lax.all_to_all(outgoing, "rows", split_axis=0, concat_axis=0, tiled=True),
        lax.all_to_all(labels, "rows", split_axis=0, concat_axis=0, tiled=True),
    )
    chosen = (
        lax.broadcasted_iota(jnp.int32, (share, arrived.shape[0]), 0)
        == arrived_labels.astype(jnp.int32)[None, :]
    )
    part_sums = jnp.dot(chosen.astype(jnp.bfloat16), arrived, preferred_element_type=jnp.float32)
    part_counts = jnp.sum(chosen.astype(jnp.float32), axis=1)
    updated = lax.all_gather(renew(part_sums, part_counts, own), "rows", axis=0, tiled=True)
    second = smallest(points, pnorm, updated)
    nearest = jnp.stack([first, block_min(second)])
    return (nearest, updated)


PLANE = 4
LANES = 128
VMEM_BYTES = 44 * 1024 * 1024
PARTS = 2


def nt_dot(a, b):
    return lax.dot_general(a, b, (((1,), (1,)), ((), ())), preferred_element_type=jnp.float32)


def column_min(cents, points):
    wide = cents.astype(jnp.float32)
    cnorm = jnp.sum(wide * wide, axis=1, keepdims=True)
    return jnp.min(cnorm - 2.0 * nt_dot(cents, points), axis=0, keepdims=True)


def flip(index, bits):
    low, high = index % 2, index // 2
    if bits % 2:
        low = 1 - low
    if bits // 2:
        high = 1 - high
    return high * 2 + low


def lloyd_kernel(
    rows, cap, share, assign_hbm, points_hbm, cents_hbm, near_ref, gath,
    assign_ref, points_ref, cents_ref, load_sem,
    placing_ref, send, lab_send, arrived, lab_arrived, klab,
    part_send, meta_send, part_got, meta_got, acc, held, mine, theirs, low,
    sent_pts, got_pts, sent_lab, got_lab, sent_part, got_part, sent_meta, got_meta,
    sent_up, sent_down, sent_x, sent_y, got_full, sent_dx, sent_dy, got_dx, got_dy, spare_sem, sent_min, got_min,
):
    count_pts, width = points_ref.shape
    blocksize = cents_ref.shape[0]
    planes = rows // PLANE
    wide = width // PARTS
    chunk = planes * cap
    me = lax.axis_index("rows")
    core = lax.axis_index("cent")
    z, q = me // PLANE, me % PLANE
    xpeer = z * PLANE + flip(q, 1)
    ypeer = z * PLANE + flip(q, 2)
    diag = z * PLANE + flip(q, 3)
    partner = 1 - core

    assign_in = pltpu.make_async_copy(assign_hbm, assign_ref, load_sem.at[2])
    assign_in.start()
    points_in = pltpu.make_async_copy(points_hbm, points_ref, load_sem.at[0])
    points_in.start()
    barrier = pltpu.get_barrier_semaphore()
    for bits in range(1, 4):
        pl.semaphore_signal(barrier, inc=1, device_id={"rows": z * PLANE + flip(q, bits)})
        pl.semaphore_signal(barrier, inc=1, device_id={"rows": flip(z, bits) * PLANE + q})
    pl.semaphore_signal(barrier, inc=1, device_id={"cent": partner})

    assign_in.wait()
    relative = (assign_ref[...] - core * blocksize).astype(jnp.float32)
    inside = (relative >= 0.0) & (relative < float(blocksize))
    owner = jnp.where(inside, jnp.floor(relative * (1.0 / share)), float(rows))
    offset1 = jnp.where(inside, relative - owner * share + 1.0, 0.0)
    hot = lax.broadcasted_iota(jnp.int32, (rows, count_pts), 0).astype(jnp.float32) == owner
    hot_f = jnp.where(hot, 1.0, 0.0)
    seg = 256
    tri = jnp.where(
        lax.broadcasted_iota(jnp.int32, (seg, seg), 0) < lax.broadcasted_iota(jnp.int32, (seg, seg), 1),
        1.0, 0.0,
    ).astype(jnp.bfloat16)
    carry = jnp.zeros((rows, 1), jnp.float32)
    pieces = []
    for s in range(count_pts // seg):
        part = hot_f[:, s * seg:(s + 1) * seg]
        before = jnp.dot(part.astype(jnp.bfloat16), tri, preferred_element_type=jnp.float32) + carry
        pieces.append(jnp.sum(part * before, axis=0, keepdims=True))
        carry = carry + jnp.sum(part, axis=1, keepdims=True)
    ranking = jnp.concatenate(pieces, axis=1)
    plane_to = jnp.floor(owner * (1.0 / PLANE))
    slot = jnp.where(inside, (owner - plane_to * PLANE) * chunk + plane_to * cap + ranking, -1.0)
    labels8 = jnp.broadcast_to(offset1, (8, count_pts)).astype(jnp.bfloat16)

    def ship(src, dst, ss, rs, axis, target):
        copy = pltpu.make_async_remote_copy(
            src_ref=src, dst_ref=dst, send_sem=ss, recv_sem=rs, device_id={axis: target}
        )
        copy.start()
        return copy

    def landed(ref, sem):
        pltpu.make_async_remote_copy(
            src_ref=ref, dst_ref=ref, send_sem=spare_sem.at[0], recv_sem=sem, device_id={"rows": xpeer}
        ).wait_recv()

    flying = []
    reach = (3, 1, 2)
    span = (3, 2, 1, 0)

    def place(k):
        i = flip(q, k)
        hit = (
            lax.broadcasted_iota(jnp.int32, (chunk, count_pts), 0) + i * chunk
        ).astype(jnp.float32) == slot
        placing = jnp.where(hit, 1.0, 0.0).astype(jnp.bfloat16)
        placing_ref[k] = placing
        lab = nt_dot(labels8, placing)
        for t in range(chunk // LANES):
            piece = lab[:, t * LANES:(t + 1) * LANES]
            if k:
                lab_send[k, t] = piece
            else:
                lab_arrived[q, t] = piece

    def fill(h, k):
        rows_out = jnp.dot(
            placing_ref[k], points_ref[:, h * wide:(h + 1) * wide], preferred_element_type=jnp.float32
        ).astype(jnp.bfloat16)
        if k:
            send[h, k] = rows_out
        else:
            for t in range(planes):
                arrived[h, t, pl.ds(pl.multiple_of(q * cap, cap), cap), :] = rows_out[t * cap:(t + 1) * cap]

    def dispatch(h, j, k):
        t = flip(z, span[j])
        spot = pl.ds(pl.multiple_of(q * cap, cap), cap)
        flying.append(ship(
            send.at[h, k, pl.ds(pl.multiple_of(t * cap, cap), cap)], arrived.at[h, t, spot],
            sent_pts.at[h, j, k], got_pts.at[h, t, q], "rows", z * PLANE + flip(q, k),
        ))

    points_in.wait()
    cents_in = pltpu.make_async_copy(cents_hbm, cents_ref, load_sem.at[1])
    cents_in.start()
    for k in reach:
        place(k)
        fill(0, k)
        if k == reach[0]:
            pl.semaphore_wait(barrier, 7)
        flying.append(ship(
            lab_send.at[k], lab_arrived.at[q], sent_lab.at[k], got_lab.at[q], "rows", z * PLANE + flip(q, k)
        ))
        dispatch(0, 0, k)
    for j in range(1, planes):
        for k in reach:
            dispatch(0, j, k)
    for h in range(1, PARTS):
        for k in reach:
            fill(h, k)
        for j in range(planes):
            for k in reach:
                dispatch(h, j, k)
    place(0)
    for h in range(PARTS):
        fill(h, 0)

    kb = 512
    pieces_first = blocksize // kb
    low[...] = jnp.full(low.shape, jnp.inf, jnp.float32)
    min_copies = []

    def first_piece(i):
        low[0:1, :] = jnp.minimum(low[0:1, :], column_min(cents_ref[i * kb:(i + 1) * kb, :], points_ref[...]))

    def point_norms():
        squares = jnp.square(points_ref[...].astype(jnp.float32))
        high = squares.astype(jnp.bfloat16)
        rest = (squares - high.astype(jnp.float32)).astype(jnp.bfloat16)
        ones = jnp.ones((8, width), jnp.bfloat16)
        return (nt_dot(ones, high) + nt_dot(ones, rest))[0:1, :]

    for k in reach:
        landed(lab_arrived.at[flip(q, k)], got_lab.at[flip(q, k)])
    lane = lax.broadcasted_iota(jnp.int32, (8, LANES), 1)
    for t in range(planes):
        for p in range(PLANE // 2):
            left, right = lab_arrived[2 * p, t // 2], lab_arrived[2 * p + 1, t // 2]
            if t % 2:
                left = pltpu.roll(left, cap, 1)
            else:
                right = pltpu.roll(right, cap, 1)
            klab[t, :, p * LANES:(p + 1) * LANES] = jnp.where(lane < cap, left, right)

    rowid1 = lax.broadcasted_iota(jnp.int32, (share, PLANE * cap), 0).astype(jnp.float32) + 1.0
    eye = lax.broadcasted_iota(jnp.int32, (share, LANES), 0) == lax.broadcasted_iota(
        jnp.int32, (share, LANES), 1
    )

    def to_row(column):
        return jnp.sum(jnp.where(eye, column, 0.0), axis=0, keepdims=True)

    def to_column(row):
        return jnp.sum(jnp.where(eye, row, 0.0), axis=1, keepdims=True)

    def gather_in(h, t):
        for k in reach:
            source = flip(q, k)
            landed(arrived.at[h, t, pl.ds(pl.multiple_of(source * cap, cap), cap)], got_pts.at[h, t, source])
        chosen = jnp.where(rowid1 == klab[t][0:1, :], 1.0, 0.0)
        counts = jnp.sum(chosen, axis=1, keepdims=True)
        total = jnp.dot(chosen.astype(jnp.bfloat16), arrived[h, t], preferred_element_type=jnp.float32)
        return total, counts

    def send_part(h, n, total, counts, target):
        peak = jnp.maximum(jnp.max(jnp.abs(total), axis=1, keepdims=True), 1e-30)
        grow = jnp.exp2(14.0 - jnp.floor(jnp.log2(peak)))
        grow = jnp.where(peak * grow >= 32767.0, grow * 0.5, grow)
        scaled = jnp.clip(jnp.round(total * grow), -32767.0, 32767.0)
        part_send[h, n] = scaled.astype(jnp.int32).astype(jnp.int16)
        first_row = lax.broadcasted_iota(jnp.int32, (8, LANES), 0) == 0
        meta_send[h, n] = jnp.where(first_row, to_row(1.0 / grow), to_row(counts))
        flying.append(ship(
            meta_send.at[h, n], meta_got.at[h, n], sent_meta.at[h, n], got_meta.at[h, n], "rows", target
        ))
        flying.append(ship(
            part_send.at[h, n], part_got.at[h, n], sent_part.at[h, n], got_part.at[h, n], "rows", target
        ))

    def take_part(h, n):
        landed(meta_got.at[h, n], got_meta.at[h, n])
        landed(part_got.at[h, n], got_part.at[h, n])
        meta = meta_got[h, n]
        return part_got[h, n].astype(jnp.int32).astype(jnp.float32) * to_column(meta[0:1, :]), to_column(meta[1:2, :])

    near_plane, far_plane = flip(z, 1) * PLANE + q, flip(z, 2) * PLANE + q

    def reduce_cross(h):
        send_part(h, 0, *gather_in(h, flip(z, 3)), near_plane)

    def reduce_hold(h):
        total, counts = gather_in(h, flip(z, 2))
        held[h] = total
        return counts

    def reduce_far(h, counts):
        more, extra = take_part(h, 0)
        send_part(h, 1, held[h] + more, counts + extra, far_plane)

    def reduce_near(h):
        send_part(h, 2, *gather_in(h, flip(z, 1)), near_plane)

    def reduce_own(h):
        total, counts = gather_in(h, z)
        own_rows = cents_ref[pl.ds(pl.multiple_of(me * share, share), share), h * wide:(h + 1) * wide]
        acc[h] = total + own_rows.astype(jnp.float32)
        return counts

    def renew_own(h, counts):
        total = acc[h]
        for n in (2, 1):
            more, extra = take_part(h, n)
            total, counts = total + more, counts + extra
        gath[me, :, h * wide:(h + 1) * wide] = (total / (counts + 1.0)).astype(jnp.bfloat16)

    half = share // 2
    upper, lower = pl.ds(0, half), pl.ds(half, half)
    top = z // 2
    visits = [z, z + 1 - 2 * (z % 2), 2 - top, 3 - 3 * top]
    climbs = []
    waiting = []

    def view(block, h, part=slice(None)):
        return gath.at[block, part, h * wide:(h + 1) * wide]

    def pass_on(h, block, n):
        for sem, target in ((sent_x, xpeer), (sent_y, ypeer)):
            flying.append(ship(view(block, h), view(block, h), sem.at[h, n], got_full.at[h, block], "rows", target))

    def climb(h, block, n, upward, downward):
        for allowed, sems, toward in ((upward, sent_up, PLANE), (downward, sent_down, -PLANE)):
            @pl.when(allowed)
            def _(sems=sems, toward=toward):
                ship(view(block, h), view(block, h), sems.at[h, n], got_full.at[h, block], "rows", me + toward)
            climbs.append((h, block, n, allowed, sems, toward))

    def await_full(h, block):
        landed(view(block, h), got_full.at[h, block])

    def absorb(h, *blocks):
        if h < PARTS - 1:
            return
        waiting.extend(blocks)
        while len(waiting) >= 2:
            drain(2)

    def drain(n):
        taken, waiting[:] = waiting[:n], waiting[n:]
        block = jnp.concatenate([gath[b] for b in taken], axis=0) if n > 1 else gath[taken[0]]
        low[1:2, :] = jnp.minimum(low[1:2, :], column_min(block, points_ref[...]))

    def cross(h, n):
        by, bx = visits[n] * PLANE + ypeer % PLANE, visits[n] * PLANE + xpeer % PLANE
        await_full(h, by)
        flying.append(ship(
            view(by, h, upper), view(by, h, upper), sent_dx.at[h, n], got_dx.at[h, by], "rows", xpeer
        ))
        await_full(h, bx)
        flying.append(ship(
            view(bx, h, lower), view(bx, h, lower), sent_dy.at[h, n], got_dy.at[h, bx], "rows", ypeer
        ))
        return by, bx

    def spread_start(h):
        climb(h, me, 0, z < planes - 1, z > 0)
        pass_on(h, me, 0)
        absorb(h, me)

    def spread_step(h, n):
        zs = visits[n]
        block = zs * PLANE + q
        await_full(h, block)
        climb(h, block, n, (zs < z) & (z < planes - 1), (zs > z) & (z > 0))
        pass_on(h, block, n)
        absorb(h, block)

    def spread_cross(h, n):
        absorb(h, *cross(h, n))

    def spread_rest(h):
        for zs in visits:
            bd = zs * PLANE + diag % PLANE
            landed(view(bd, h, upper), got_dx.at[h, bd])
            landed(view(bd, h, lower), got_dy.at[h, bd])
            absorb(h, bd)

    cents_in.wait()
    reduce_cross(0)
    first_piece(0)
    counts = reduce_hold(0)
    first_piece(1)
    reduce_far(0, counts)
    reduce_near(0)
    first_piece(2)
    counts = reduce_own(0)
    for i in range(planes - 1, pieces_first):
        first_piece(i)
    renew_own(0, counts)
    spread_start(0)
    reduce_cross(1)
    pnorm = point_norms()
    mine[0] = (pnorm + low[0:1, :]) / width
    min_copies.append(ship(mine.at[0], theirs.at[0], sent_min.at[0], got_min.at[0], "cent", partner))
    counts = reduce_hold(1)
    reduce_far(1, counts)
    reduce_near(1)
    spread_step(0, 1)
    counts = reduce_own(1)
    renew_own(1, counts)
    spread_start(1)
    spread_step(0, 2)
    spread_cross(0, 0)
    spread_step(1, 1)
    spread_step(0, 3)
    spread_cross(0, 1)
    spread_step(1, 2)
    spread_cross(1, 0)
    spread_cross(0, 2)
    spread_step(1, 3)
    spread_cross(1, 1)
    spread_cross(0, 3)
    spread_cross(1, 2)
    spread_rest(0)
    spread_cross(1, 3)
    spread_rest(1)
    if waiting:
        drain(len(waiting))

    mine[1] = (pnorm + low[1:2, :]) / width
    min_copies.append(ship(mine.at[1], theirs.at[1], sent_min.at[1], got_min.at[1], "cent", partner))
    for copy in flying:
        copy.wait_send()
    for h, block, n, allowed, sems, toward in climbs:
        @pl.when(allowed)
        def _(h=h, block=block, n=n, sems=sems, toward=toward):
            pltpu.make_async_remote_copy(
                src_ref=view(block, h), dst_ref=view(block, h), send_sem=sems.at[h, n],
                recv_sem=got_full.at[h, block], device_id={"rows": me + toward},
            ).wait_send()
    for n, copy in enumerate(min_copies):
        copy.wait()
        near_ref[n:n + 1, :] = jnp.minimum(mine[n], theirs[n])


def deliver(near_ref, gath_ref, near_out, upd_out, sems):
    copies = [
        pltpu.make_async_copy(gath_ref, upd_out, sems.at[0]),
        pltpu.make_async_copy(near_ref, near_out, sems.at[1]),
    ]
    for copy in copies:
        copy.start()
    for copy in copies:
        copy.wait()


def fused(points, centroids, assign, rows, cap, share):
    count_pts, width = points.shape
    planes = rows // PLANE
    hbm = pl.BlockSpec(memory_space=pltpu.HBM)
    vmem = pl.BlockSpec(memory_space=pltpu.VMEM)
    dma = pltpu.SemaphoreType.DMA
    chunk = planes * cap
    wide = width // PARTS
    shapes = (
        jax.ShapeDtypeStruct((2, count_pts), jnp.float32),
        jax.ShapeDtypeStruct((rows, share, width), jnp.bfloat16),
    )
    hops = planes - 1
    near, upd = pl.pallas_call(
        functools.partial(lloyd_kernel, rows, cap, share),
        out_shape=shapes,
        in_specs=[hbm, hbm, hbm],
        out_specs=(vmem, vmem),
        scratch_shapes=[
            pltpu.VMEM((1, count_pts), jnp.int32),
            pltpu.VMEM((count_pts, width), jnp.bfloat16),
            pltpu.VMEM(centroids.shape, jnp.bfloat16),
            dma((3,)),
            pltpu.VMEM((PLANE, chunk, count_pts), jnp.bfloat16),
            pltpu.VMEM((PARTS, PLANE, chunk, wide), jnp.bfloat16),
            pltpu.VMEM((PLANE, chunk // LANES, 8, LANES), jnp.float32),
            pltpu.VMEM((PARTS, planes, PLANE * cap, wide), jnp.bfloat16),
            pltpu.VMEM((PLANE, chunk // LANES, 8, LANES), jnp.float32),
            pltpu.VMEM((planes, 8, PLANE * cap), jnp.float32),
            pltpu.VMEM((PARTS, hops, share, wide), jnp.int16),
            pltpu.VMEM((PARTS, hops, 8, LANES), jnp.float32),
            pltpu.VMEM((PARTS, hops, share, wide), jnp.int16),
            pltpu.VMEM((PARTS, hops, 8, LANES), jnp.float32),
            pltpu.VMEM((PARTS, share, wide), jnp.float32),
            pltpu.VMEM((PARTS, share, wide), jnp.float32),
            pltpu.VMEM((2, 1, count_pts), jnp.float32),
            pltpu.VMEM((2, 1, count_pts), jnp.float32),
            pltpu.VMEM((8, count_pts), jnp.float32),
            dma((PARTS, planes, PLANE)), dma((PARTS, planes, PLANE)), dma((PLANE,)), dma((PLANE,)),
            dma((PARTS, hops)), dma((PARTS, hops)), dma((PARTS, hops)), dma((PARTS, hops)),
            dma((PARTS, planes)), dma((PARTS, planes)), dma((PARTS, planes)), dma((PARTS, planes)),
            dma((PARTS, rows)),
            dma((PARTS, planes)), dma((PARTS, planes)), dma((PARTS, rows)), dma((PARTS, rows)), dma((1,)),
            dma((2,)), dma((2,)),
        ],
        compiler_params=pltpu.CompilerParams(
            collective_id=0, has_side_effects=True, vmem_limit_bytes=VMEM_BYTES
        ),
    )(
        pltpu.with_memory_space_constraint(assign[None, :], pltpu.HBM),
        pltpu.with_memory_space_constraint(points, pltpu.HBM),
        pltpu.with_memory_space_constraint(centroids, pltpu.HBM),
    )
    near, upd = pl.pallas_call(
        deliver,
        out_shape=shapes,
        in_specs=[vmem, vmem],
        out_specs=(hbm, hbm),
        scratch_shapes=[dma((2,))],
        compiler_params=pltpu.CompilerParams(vmem_limit_bytes=1024 * 1024),
    )(near, upd)
    return near, upd.reshape(rows * share, width)


def step(rows, cent, points, centroids, assign):
    count_pts = points.shape[0]
    blocksize = centroids.shape[0]
    share = blocksize // rows
    cap = max(2, 2 * count_pts // (rows * cent))
    fits = cent == 2 and rows == 4 * PLANE and share == LANES and 2 * cap == LANES
    even = count_pts % 256 == 0 and blocksize % 512 == 0 and points.shape[1] % (PARTS * LANES) == 0
    if fits and even:
        return fused(points, centroids, assign, rows, cap, share)
    return per_device(points, centroids, assign)


def solution(mesh):
    return jax.shard_map(
        functools.partial(step, mesh.shape["rows"], mesh.shape["cent"]),
        mesh=mesh,
        in_specs=(P("rows", None), P("cent", None), P("rows")),
        out_specs=(P(None, "rows"), P("cent", None)),
        check_vma=False,
    )
```

```python
import functools

import jax
import jax.numpy as jnp
from jax import lax
from jax.experimental import pallas as pl
from jax.experimental.pallas import tpu as pltpu
from jax.sharding import PartitionSpec as P


def smallest(points, pnorm, cents):
    cnorm = jnp.sum(jnp.square(cents.astype(jnp.float32)), axis=1)
    dots = lax.dot_general(
        points, cents, (((1,), (1,)), ((), ())), preferred_element_type=jnp.float32
    )
    return jnp.min((pnorm[:, None] - 2.0 * dots + cnorm[None, :]) / points.shape[1], axis=1)


def block_min(values):
    return lax.pmin(values, "cent")


def renew(part_sums, part_counts, own_rows):
    return ((part_sums + own_rows.astype(jnp.float32)) / (part_counts[:, None] + 1.0)).astype(
        jnp.bfloat16
    )


def per_device(points, centroids, assign):
    blocksize = centroids.shape[0]
    count_pts = points.shape[0]
    pnorm = jnp.sum(jnp.square(points.astype(jnp.float32)), axis=1)
    first = smallest(points, pnorm, centroids)
    first = block_min(first)
    relative = assign - lax.axis_index("cent") * blocksize
    share = blocksize // lax.axis_size("rows")
    own = lax.dynamic_slice_in_dim(centroids, lax.axis_index("rows") * share, share, 0)
    rows_count = lax.axis_size("rows")
    groups = rows_count * lax.axis_size("cent")
    capacity = max(2, 2 * count_pts // groups)
    inside = (relative >= 0) & (relative < blocksize)
    owners = jnp.where(inside, relative // share, rows_count)
    offsets = jnp.where(inside, relative - relative // share * share, 0)
    owner_hot = owners[:, None] == lax.broadcasted_iota(jnp.int32, (count_pts, rows_count), 1)
    earlier = lax.broadcasted_iota(jnp.int32, (count_pts, count_pts), 1) < lax.broadcasted_iota(
        jnp.int32, (count_pts, count_pts), 0
    )
    before = jnp.dot(
        earlier.astype(jnp.bfloat16),
        owner_hot.astype(jnp.bfloat16),
        preferred_element_type=jnp.float32,
    )
    ranking = jnp.sum(jnp.where(owner_hot, before, 0.0), axis=1).astype(jnp.int32)
    slot_index = jnp.where(inside, owners * capacity + ranking, -1)
    placing = (
        lax.broadcasted_iota(jnp.int32, (rows_count * capacity, count_pts), 0)
        == slot_index[None, :]
    )
    outgoing = jnp.dot(
        placing.astype(jnp.bfloat16), points, preferred_element_type=jnp.float32
    ).astype(jnp.bfloat16)
    labels = (jnp.sum(jnp.where(placing, offsets[None, :] + 1, 0), axis=1) - 1).astype(jnp.bfloat16)
    arrived, arrived_labels = (
        lax.all_to_all(outgoing, "rows", split_axis=0, concat_axis=0, tiled=True),
        lax.all_to_all(labels, "rows", split_axis=0, concat_axis=0, tiled=True),
    )
    chosen = (
        lax.broadcasted_iota(jnp.int32, (share, arrived.shape[0]), 0)
        == arrived_labels.astype(jnp.int32)[None, :]
    )
    part_sums = jnp.dot(chosen.astype(jnp.bfloat16), arrived, preferred_element_type=jnp.float32)
    part_counts = jnp.sum(chosen.astype(jnp.float32), axis=1)
    updated = lax.all_gather(renew(part_sums, part_counts, own), "rows", axis=0, tiled=True)
    second = smallest(points, pnorm, updated)
    nearest = jnp.stack([first, block_min(second)])
    return (nearest, updated)


PLANE = 4
LANES = 128
VMEM_BYTES = 44 * 1024 * 1024
PARTS = 2
TALL = (0, 64)


def nt_dot(a, b):
    return lax.dot_general(a, b, (((1,), (1,)), ((), ())), preferred_element_type=jnp.float32)


def column_min(cents, points):
    wide = cents.astype(jnp.float32)
    cnorm = jnp.sum(wide * wide, axis=1, keepdims=True)
    return jnp.min(cnorm - 2.0 * nt_dot(cents, points), axis=0, keepdims=True)


def flip(index, bits):
    low, high = index % 2, index // 2
    if bits % 2:
        low = 1 - low
    if bits // 2:
        high = 1 - high
    return high * 2 + low


def lloyd_kernel(
    rows, cap, share, assign_hbm, points_hbm, cents_hbm, near_ref, gath,
    assign_ref, points_ref, cents_ref, load_sem,
    placing_ref, send, lab_send, arrived, lab_arrived, klab,
    part_send, meta_send, part_got, meta_got, acc, held, mine, theirs, low,
    sent_pts, got_pts, sent_lab, got_lab, sent_part, got_part, sent_meta, got_meta,
    sent_up, sent_down, got_col, sent_up_tall, sent_down_tall, got_tall, sent_x, sent_y, got_full, sent_dx, sent_dy, got_dx, got_dy, spare_sem, sent_min, got_min,
):
    count_pts, width = points_ref.shape
    blocksize = cents_ref.shape[0]
    planes = rows // PLANE
    wide = width // PARTS
    chunk = planes * cap
    me = lax.axis_index("rows")
    core = lax.axis_index("cent")
    z, q = me // PLANE, me % PLANE
    xpeer = z * PLANE + flip(q, 1)
    ypeer = z * PLANE + flip(q, 2)
    diag = z * PLANE + flip(q, 3)
    partner = 1 - core

    assign_in = pltpu.make_async_copy(assign_hbm, assign_ref, load_sem.at[2])
    assign_in.start()
    points_in = pltpu.make_async_copy(points_hbm, points_ref, load_sem.at[0])
    points_in.start()
    barrier = pltpu.get_barrier_semaphore()
    for bits in range(1, 4):
        pl.semaphore_signal(barrier, inc=1, device_id={"rows": z * PLANE + flip(q, bits)})
        pl.semaphore_signal(barrier, inc=1, device_id={"rows": flip(z, bits) * PLANE + q})
    pl.semaphore_signal(barrier, inc=1, device_id={"cent": partner})

    assign_in.wait()
    relative = (assign_ref[...] - core * blocksize).astype(jnp.float32)
    inside = (relative >= 0.0) & (relative < float(blocksize))
    owner = jnp.where(inside, jnp.floor(relative * (1.0 / share)), float(rows))
    offset1 = jnp.where(inside, relative - owner * share + 1.0, 0.0)
    hot = lax.broadcasted_iota(jnp.int32, (rows, count_pts), 0).astype(jnp.float32) == owner
    hot_f = jnp.where(hot, 1.0, 0.0)
    seg = 256
    tri = jnp.where(
        lax.broadcasted_iota(jnp.int32, (seg, seg), 0) < lax.broadcasted_iota(jnp.int32, (seg, seg), 1),
        1.0, 0.0,
    ).astype(jnp.bfloat16)
    carry = jnp.zeros((rows, 1), jnp.float32)
    pieces = []
    for s in range(count_pts // seg):
        part = hot_f[:, s * seg:(s + 1) * seg]
        before = jnp.dot(part.astype(jnp.bfloat16), tri, preferred_element_type=jnp.float32) + carry
        pieces.append(jnp.sum(part * before, axis=0, keepdims=True))
        carry = carry + jnp.sum(part, axis=1, keepdims=True)
    ranking = jnp.concatenate(pieces, axis=1)
    plane_to = jnp.floor(owner * (1.0 / PLANE))
    slot = jnp.where(inside, (owner - plane_to * PLANE) * chunk + plane_to * cap + ranking, -1.0)
    labels8 = jnp.broadcast_to(offset1, (8, count_pts)).astype(jnp.bfloat16)

    def ship(src, dst, ss, rs, axis, target):
        copy = pltpu.make_async_remote_copy(
            src_ref=src, dst_ref=dst, send_sem=ss, recv_sem=rs, device_id={axis: target}
        )
        copy.start()
        return copy

    def landed(ref, sem):
        pltpu.make_async_remote_copy(
            src_ref=ref, dst_ref=ref, send_sem=spare_sem.at[0], recv_sem=sem, device_id={"rows": xpeer}
        ).wait_recv()

    flying = []
    reach = (3, 1, 2)
    span = (3, 2, 1, 0)

    def place(k):
        i = flip(q, k)
        hit = (
            lax.broadcasted_iota(jnp.int32, (chunk, count_pts), 0) + i * chunk
        ).astype(jnp.float32) == slot
        placing = jnp.where(hit, 1.0, 0.0).astype(jnp.bfloat16)
        placing_ref[k] = placing
        lab = nt_dot(labels8, placing)
        for t in range(chunk // LANES):
            piece = lab[:, t * LANES:(t + 1) * LANES]
            if k:
                lab_send[k, t] = piece
            else:
                lab_arrived[q, t] = piece

    def fill(h, k):
        rows_out = jnp.dot(
            placing_ref[k], points_ref[:, h * wide:(h + 1) * wide], preferred_element_type=jnp.float32
        ).astype(jnp.bfloat16)
        if k:
            send[h, k] = rows_out
        else:
            for t in range(planes):
                arrived[h, t, pl.ds(pl.multiple_of(q * cap, cap), cap), :] = rows_out[t * cap:(t + 1) * cap]

    def dispatch(h, j, k):
        t = flip(z, span[j])
        spot = pl.ds(pl.multiple_of(q * cap, cap), cap)
        flying.append(ship(
            send.at[h, k, pl.ds(pl.multiple_of(t * cap, cap), cap)], arrived.at[h, t, spot],
            sent_pts.at[h, j, k], got_pts.at[h, t, q], "rows", z * PLANE + flip(q, k),
        ))

    points_in.wait()
    cents_in = pltpu.make_async_copy(cents_hbm, cents_ref, load_sem.at[1])
    cents_in.start()
    for k in reach:
        place(k)
        fill(0, k)
        if k == reach[0]:
            pl.semaphore_wait(barrier, 7)
        flying.append(ship(
            lab_send.at[k], lab_arrived.at[q], sent_lab.at[k], got_lab.at[q], "rows", z * PLANE + flip(q, k)
        ))
        dispatch(0, 0, k)
    for j in range(1, planes):
        for k in reach:
            dispatch(0, j, k)
    for h in range(1, PARTS):
        for k in reach:
            fill(h, k)
        for j in range(planes):
            for k in reach:
                dispatch(h, j, k)
    place(0)
    for h in range(PARTS):
        fill(h, 0)

    kb = 512
    pieces_first = blocksize // kb
    low[...] = jnp.full(low.shape, jnp.inf, jnp.float32)
    min_copies = []

    def first_piece(i):
        low[0:1, :] = jnp.minimum(low[0:1, :], column_min(cents_ref[i * kb:(i + 1) * kb, :], points_ref[...]))

    def point_norms():
        squares = jnp.square(points_ref[...].astype(jnp.float32))
        high = squares.astype(jnp.bfloat16)
        rest = (squares - high.astype(jnp.float32)).astype(jnp.bfloat16)
        ones = jnp.ones((8, width), jnp.bfloat16)
        return (nt_dot(ones, high) + nt_dot(ones, rest))[0:1, :]

    for k in reach:
        landed(lab_arrived.at[flip(q, k)], got_lab.at[flip(q, k)])
    lane = lax.broadcasted_iota(jnp.int32, (8, LANES), 1)
    for t in range(planes):
        for p in range(PLANE // 2):
            left, right = lab_arrived[2 * p, t // 2], lab_arrived[2 * p + 1, t // 2]
            if t % 2:
                left = pltpu.roll(left, cap, 1)
            else:
                right = pltpu.roll(right, cap, 1)
            klab[t, :, p * LANES:(p + 1) * LANES] = jnp.where(lane < cap, left, right)

    rowid1 = lax.broadcasted_iota(jnp.int32, (share, PLANE * cap), 0).astype(jnp.float32) + 1.0
    eye = lax.broadcasted_iota(jnp.int32, (share, LANES), 0) == lax.broadcasted_iota(
        jnp.int32, (share, LANES), 1
    )

    def to_row(column):
        return jnp.sum(jnp.where(eye, column, 0.0), axis=0, keepdims=True)

    def to_column(row):
        return jnp.sum(jnp.where(eye, row, 0.0), axis=1, keepdims=True)

    def gather_in(h, t):
        for k in reach:
            source = flip(q, k)
            landed(arrived.at[h, t, pl.ds(pl.multiple_of(source * cap, cap), cap)], got_pts.at[h, t, source])
        chosen = jnp.where(rowid1 == klab[t][0:1, :], 1.0, 0.0)
        counts = jnp.sum(chosen, axis=1, keepdims=True)
        total = jnp.dot(chosen.astype(jnp.bfloat16), arrived[h, t], preferred_element_type=jnp.float32)
        return total, counts

    def send_part(h, n, total, counts, target):
        peak = jnp.maximum(jnp.max(jnp.abs(total), axis=1, keepdims=True), 1e-30)
        grow = jnp.exp2(14.0 - jnp.floor(jnp.log2(peak)))
        grow = jnp.where(peak * grow >= 32767.0, grow * 0.5, grow)
        scaled = jnp.clip(jnp.round(total * grow), -32767.0, 32767.0)
        part_send[h, n] = scaled.astype(jnp.int32).astype(jnp.int16)
        first_row = lax.broadcasted_iota(jnp.int32, (8, LANES), 0) == 0
        meta_send[h, n] = jnp.where(first_row, to_row(1.0 / grow), to_row(counts))
        flying.append(ship(
            meta_send.at[h, n], meta_got.at[h, n], sent_meta.at[h, n], got_meta.at[h, n], "rows", target
        ))
        flying.append(ship(
            part_send.at[h, n], part_got.at[h, n], sent_part.at[h, n], got_part.at[h, n], "rows", target
        ))

    def take_part(h, n):
        landed(meta_got.at[h, n], got_meta.at[h, n])
        landed(part_got.at[h, n], got_part.at[h, n])
        meta = meta_got[h, n]
        return part_got[h, n].astype(jnp.int32).astype(jnp.float32) * to_column(meta[0:1, :]), to_column(meta[1:2, :])

    near_plane, far_plane = flip(z, 1) * PLANE + q, flip(z, 2) * PLANE + q

    def reduce_cross(h):
        send_part(h, 0, *gather_in(h, flip(z, 3)), near_plane)

    def reduce_hold(h):
        total, counts = gather_in(h, flip(z, 2))
        held[h] = total
        return counts

    def reduce_far(h, counts):
        more, extra = take_part(h, 0)
        send_part(h, 1, held[h] + more, counts + extra, far_plane)

    def reduce_near(h):
        send_part(h, 2, *gather_in(h, flip(z, 1)), near_plane)

    def reduce_own(h):
        total, counts = gather_in(h, z)
        own_rows = cents_ref[pl.ds(pl.multiple_of(me * share, share), share), h * wide:(h + 1) * wide]
        acc[h] = total + own_rows.astype(jnp.float32)
        return counts

    def renew_own(h, counts):
        total = acc[h]
        for n in (2, 1):
            more, extra = take_part(h, n)
            total, counts = total + more, counts + extra
        gath[me, :, h * wide:(h + 1) * wide] = (total / (counts + 1.0)).astype(jnp.bfloat16)

    top = z // 2
    visits = [z, z + 1 - 2 * (z % 2), 2 - top, 3 - 3 * top]
    climbs = []
    waiting = []
    missing = {}

    def flat(h, n):
        return share if n == 0 else share - TALL[h]

    def view(block, h, first=0, count=share):
        return gath.at[block, pl.ds(first, count), h * wide:(h + 1) * wide]

    def tall(block, h):
        return view(block, h, share - TALL[h], TALL[h])

    def pass_on(h, block, n):
        part = view(block, h, 0, flat(h, n))
        for sem, target in ((sent_x, xpeer), (sent_y, ypeer)):
            flying.append(ship(part, part, sem.at[h, n], got_full.at[h, block], "rows", target))

    def climb(part, got, n, send_up, send_down):
        zs = visits[n]
        upward, downward = (zs <= z) & (z < planes - 1), (zs >= z) & (z > 0)
        for allowed, sem, toward in ((upward, send_up, PLANE), (downward, send_down, -PLANE)):
            @pl.when(allowed)
            def _(sem=sem, toward=toward):
                ship(part, part, sem, got, "rows", me + toward)
            climbs.append((part, got, allowed, sem, toward))

    def settle(h, n, kind, block):
        key = (n, kind)
        missing.setdefault(key, PARTS + (1 if n and kind != "q" else 0) * sum(1 for r in TALL if r))
        missing[key] -= 1
        if missing[key] == 0:
            waiting.append(block)
        while len(waiting) >= 2:
            drain(2)

    def drain(n):
        taken, waiting[:] = waiting[:n], waiting[n:]
        block = jnp.concatenate([gath[b] for b in taken], axis=0) if n > 1 else gath[taken[0]]
        low[1:2, :] = jnp.minimum(low[1:2, :], column_min(block, points_ref[...]))

    def spread_start(h):
        climb(view(me, h), got_col.at[h, me], 0, sent_up.at[h, 0], sent_down.at[h, 0])
        pass_on(h, me, 0)
        settle(h, 0, "q", me)

    def spread_step(h, n):
        block = visits[n] * PLANE + q
        landed(view(block, h), got_col.at[h, block])
        climb(view(block, h), got_col.at[h, block], n, sent_up.at[h, n], sent_down.at[h, n])
        pass_on(h, block, n)
        settle(h, n, "q", block)

    def spread_cross(h, n):
        by, bx = visits[n] * PLANE + ypeer % PLANE, visits[n] * PLANE + xpeer % PLANE
        count, half = flat(h, n), flat(h, n) // 2
        landed(view(by, h, 0, count), got_full.at[h, by])
        part = view(by, h, 0, half)
        flying.append(ship(part, part, sent_dx.at[h, n], got_dx.at[h, by], "rows", xpeer))
        landed(view(bx, h, 0, count), got_full.at[h, bx])
        part = view(bx, h, half, half)
        flying.append(ship(part, part, sent_dy.at[h, n], got_dy.at[h, bx], "rows", ypeer))
        settle(h, n, "y", by)
        settle(h, n, "x", bx)

    def spread_diag(h, n):
        bd, half = visits[n] * PLANE + diag % PLANE, flat(h, n) // 2
        landed(view(bd, h, 0, half), got_dx.at[h, bd])
        landed(view(bd, h, half, half), got_dy.at[h, bd])
        settle(h, n, "d", bd)

    def spread_tall(h, n):
        for i, (kind, mate) in enumerate((("x", xpeer), ("y", ypeer), ("d", diag))):
            block = visits[n] * PLANE + mate % PLANE
            got = got_tall.at[h, block]
            if n:
                landed(tall(block, h), got)
            climb(tall(block, h), got, n, sent_up_tall.at[h, n, i], sent_down_tall.at[h, n, i])
            if n:
                settle(h, n, kind, block)

    cents_in.wait()
    reduce_cross(0)
    first_piece(0)
    counts = reduce_hold(0)
    first_piece(1)
    reduce_far(0, counts)
    reduce_near(0)
    first_piece(2)
    counts = reduce_own(0)
    for i in range(planes - 1, pieces_first):
        first_piece(i)
    renew_own(0, counts)
    spread_start(0)
    reduce_cross(1)
    pnorm = point_norms()
    mine[0] = (pnorm + low[0:1, :]) / width
    min_copies.append(ship(mine.at[0], theirs.at[0], sent_min.at[0], got_min.at[0], "cent", partner))
    counts = reduce_hold(1)
    reduce_far(1, counts)
    reduce_near(1)
    spread_step(0, 1)
    counts = reduce_own(1)
    renew_own(1, counts)
    spread_start(1)
    spread_cross(0, 0)
    spread_step(0, 2)
    spread_step(1, 1)
    spread_cross(1, 0)
    spread_cross(0, 1)
    spread_diag(1, 0)
    spread_tall(1, 0)
    spread_step(0, 3)
    spread_step(1, 2)
    spread_cross(0, 2)
    spread_tall(1, 1)
    spread_cross(1, 1)
    spread_step(1, 3)
    spread_cross(0, 3)
    spread_tall(1, 2)
    spread_cross(1, 2)
    for n in range(planes):
        spread_diag(0, n)
    spread_cross(1, 3)
    spread_diag(1, 1)
    spread_diag(1, 2)
    spread_tall(1, 3)
    spread_diag(1, 3)
    if waiting:
        drain(len(waiting))

    mine[1] = (pnorm + low[1:2, :]) / width
    min_copies.append(ship(mine.at[1], theirs.at[1], sent_min.at[1], got_min.at[1], "cent", partner))
    for copy in flying:
        copy.wait_send()
    for part, got, allowed, sem, toward in climbs:
        @pl.when(allowed)
        def _(part=part, got=got, sem=sem, toward=toward):
            pltpu.make_async_remote_copy(
                src_ref=part, dst_ref=part, send_sem=sem, recv_sem=got, device_id={"rows": me + toward}
            ).wait_send()
    for n, copy in enumerate(min_copies):
        copy.wait()
        near_ref[n:n + 1, :] = jnp.minimum(mine[n], theirs[n])


def deliver(near_ref, gath_ref, near_out, upd_out, sems):
    copies = [
        pltpu.make_async_copy(gath_ref, upd_out, sems.at[0]),
        pltpu.make_async_copy(near_ref, near_out, sems.at[1]),
    ]
    for copy in copies:
        copy.start()
    for copy in copies:
        copy.wait()


def fused(points, centroids, assign, rows, cap, share):
    count_pts, width = points.shape
    planes = rows // PLANE
    hbm = pl.BlockSpec(memory_space=pltpu.HBM)
    vmem = pl.BlockSpec(memory_space=pltpu.VMEM)
    dma = pltpu.SemaphoreType.DMA
    chunk = planes * cap
    wide = width // PARTS
    shapes = (
        jax.ShapeDtypeStruct((2, count_pts), jnp.float32),
        jax.ShapeDtypeStruct((rows, share, width), jnp.bfloat16),
    )
    hops = planes - 1
    near, upd = pl.pallas_call(
        functools.partial(lloyd_kernel, rows, cap, share),
        out_shape=shapes,
        in_specs=[hbm, hbm, hbm],
        out_specs=(vmem, vmem),
        scratch_shapes=[
            pltpu.VMEM((1, count_pts), jnp.int32),
            pltpu.VMEM((count_pts, width), jnp.bfloat16),
            pltpu.VMEM(centroids.shape, jnp.bfloat16),
            dma((3,)),
            pltpu.VMEM((PLANE, chunk, count_pts), jnp.bfloat16),
            pltpu.VMEM((PARTS, PLANE, chunk, wide), jnp.bfloat16),
            pltpu.VMEM((PLANE, chunk // LANES, 8, LANES), jnp.float32),
            pltpu.VMEM((PARTS, planes, PLANE * cap, wide), jnp.bfloat16),
            pltpu.VMEM((PLANE, chunk // LANES, 8, LANES), jnp.float32),
            pltpu.VMEM((planes, 8, PLANE * cap), jnp.float32),
            pltpu.VMEM((PARTS, hops, share, wide), jnp.int16),
            pltpu.VMEM((PARTS, hops, 8, LANES), jnp.float32),
            pltpu.VMEM((PARTS, hops, share, wide), jnp.int16),
            pltpu.VMEM((PARTS, hops, 8, LANES), jnp.float32),
            pltpu.VMEM((PARTS, share, wide), jnp.float32),
            pltpu.VMEM((PARTS, share, wide), jnp.float32),
            pltpu.VMEM((2, 1, count_pts), jnp.float32),
            pltpu.VMEM((2, 1, count_pts), jnp.float32),
            pltpu.VMEM((8, count_pts), jnp.float32),
            dma((PARTS, planes, PLANE)), dma((PARTS, planes, PLANE)), dma((PLANE,)), dma((PLANE,)),
            dma((PARTS, hops)), dma((PARTS, hops)), dma((PARTS, hops)), dma((PARTS, hops)),
            dma((PARTS, planes)), dma((PARTS, planes)), dma((PARTS, rows)),
            dma((PARTS, planes, 3)), dma((PARTS, planes, 3)), dma((PARTS, rows)),
            dma((PARTS, planes)), dma((PARTS, planes)), dma((PARTS, rows)),
            dma((PARTS, planes)), dma((PARTS, planes)), dma((PARTS, rows)), dma((PARTS, rows)), dma((1,)),
            dma((2,)), dma((2,)),
        ],
        compiler_params=pltpu.CompilerParams(
            collective_id=0, has_side_effects=True, vmem_limit_bytes=VMEM_BYTES
        ),
    )(
        pltpu.with_memory_space_constraint(assign[None, :], pltpu.HBM),
        pltpu.with_memory_space_constraint(points, pltpu.HBM),
        pltpu.with_memory_space_constraint(centroids, pltpu.HBM),
    )
    near, upd = pl.pallas_call(
        deliver,
        out_shape=shapes,
        in_specs=[vmem, vmem],
        out_specs=(hbm, hbm),
        scratch_shapes=[dma((2,))],
        compiler_params=pltpu.CompilerParams(vmem_limit_bytes=1024 * 1024),
    )(near, upd)
    return near, upd.reshape(rows * share, width)


def step(rows, cent, points, centroids, assign):
    count_pts = points.shape[0]
    blocksize = centroids.shape[0]
    share = blocksize // rows
    cap = max(2, 2 * count_pts // (rows * cent))
    fits = cent == 2 and rows == 4 * PLANE and share == LANES and 2 * cap == LANES
    even = count_pts % 256 == 0 and blocksize % 512 == 0 and points.shape[1] % (PARTS * LANES) == 0
    if fits and even:
        return fused(points, centroids, assign, rows, cap, share)
    return per_device(points, centroids, assign)


def solution(mesh):
    return jax.shard_map(
        functools.partial(step, mesh.shape["rows"], mesh.shape["cent"]),
        mesh=mesh,
        in_specs=(P("rows", None), P("cent", None), P("rows")),
        out_specs=(P(None, "rows"), P("cent", None)),
        check_vma=False,
    )
```

```python
import functools

import jax
import jax.numpy as jnp
from jax import lax
from jax.experimental import pallas as pl
from jax.experimental.pallas import tpu as pltpu
from jax.sharding import PartitionSpec as P


def smallest(points, pnorm, cents):
    cnorm = jnp.sum(jnp.square(cents.astype(jnp.float32)), axis=1)
    dots = lax.dot_general(
        points, cents, (((1,), (1,)), ((), ())), preferred_element_type=jnp.float32
    )
    return jnp.min((pnorm[:, None] - 2.0 * dots + cnorm[None, :]) / points.shape[1], axis=1)


def block_min(values):
    return lax.pmin(values, "cent")


def renew(part_sums, part_counts, own_rows):
    return ((part_sums + own_rows.astype(jnp.float32)) / (part_counts[:, None] + 1.0)).astype(
        jnp.bfloat16
    )


def per_device(points, centroids, assign):
    blocksize = centroids.shape[0]
    count_pts = points.shape[0]
    pnorm = jnp.sum(jnp.square(points.astype(jnp.float32)), axis=1)
    first = smallest(points, pnorm, centroids)
    first = block_min(first)
    relative = assign - lax.axis_index("cent") * blocksize
    share = blocksize // lax.axis_size("rows")
    own = lax.dynamic_slice_in_dim(centroids, lax.axis_index("rows") * share, share, 0)
    rows_count = lax.axis_size("rows")
    groups = rows_count * lax.axis_size("cent")
    capacity = max(2, 2 * count_pts // groups)
    inside = (relative >= 0) & (relative < blocksize)
    owners = jnp.where(inside, relative // share, rows_count)
    offsets = jnp.where(inside, relative - relative // share * share, 0)
    owner_hot = owners[:, None] == lax.broadcasted_iota(jnp.int32, (count_pts, rows_count), 1)
    earlier = lax.broadcasted_iota(jnp.int32, (count_pts, count_pts), 1) < lax.broadcasted_iota(
        jnp.int32, (count_pts, count_pts), 0
    )
    before = jnp.dot(
        earlier.astype(jnp.bfloat16),
        owner_hot.astype(jnp.bfloat16),
        preferred_element_type=jnp.float32,
    )
    ranking = jnp.sum(jnp.where(owner_hot, before, 0.0), axis=1).astype(jnp.int32)
    slot_index = jnp.where(inside, owners * capacity + ranking, -1)
    placing = (
        lax.broadcasted_iota(jnp.int32, (rows_count * capacity, count_pts), 0)
        == slot_index[None, :]
    )
    outgoing = jnp.dot(
        placing.astype(jnp.bfloat16), points, preferred_element_type=jnp.float32
    ).astype(jnp.bfloat16)
    labels = (jnp.sum(jnp.where(placing, offsets[None, :] + 1, 0), axis=1) - 1).astype(jnp.bfloat16)
    arrived, arrived_labels = (
        lax.all_to_all(outgoing, "rows", split_axis=0, concat_axis=0, tiled=True),
        lax.all_to_all(labels, "rows", split_axis=0, concat_axis=0, tiled=True),
    )
    chosen = (
        lax.broadcasted_iota(jnp.int32, (share, arrived.shape[0]), 0)
        == arrived_labels.astype(jnp.int32)[None, :]
    )
    part_sums = jnp.dot(chosen.astype(jnp.bfloat16), arrived, preferred_element_type=jnp.float32)
    part_counts = jnp.sum(chosen.astype(jnp.float32), axis=1)
    updated = lax.all_gather(renew(part_sums, part_counts, own), "rows", axis=0, tiled=True)
    second = smallest(points, pnorm, updated)
    nearest = jnp.stack([first, block_min(second)])
    return (nearest, updated)


PLANE = 4
LANES = 128
VMEM_BYTES = 44 * 1024 * 1024
PARTS = 2
TALL = (0, 32)


def nt_dot(a, b):
    return lax.dot_general(a, b, (((1,), (1,)), ((), ())), preferred_element_type=jnp.float32)


def column_min(cents, points):
    wide = cents.astype(jnp.float32)
    cnorm = jnp.sum(wide * wide, axis=1, keepdims=True)
    return jnp.min(cnorm - 2.0 * nt_dot(cents, points), axis=0, keepdims=True)


def flip(index, bits):
    low, high = index % 2, index // 2
    if bits % 2:
        low = 1 - low
    if bits // 2:
        high = 1 - high
    return high * 2 + low


def lloyd_kernel(
    rows, cap, share, assign_hbm, points_hbm, cents_hbm, near_ref, gath,
    assign_ref, points_ref, cents_ref, load_sem,
    placing_ref, send, lab_send, arrived, lab_arrived, klab,
    part_send, meta_send, part_got, meta_got, acc, held, mine, theirs, low,
    sent_pts, got_pts, sent_lab, got_lab, sent_part, got_part, sent_meta, got_meta,
    sent_col, got_col, sent_tall, got_tall, sent_x, sent_y, got_full, sent_dx, sent_dy, got_dx, got_dy, spare_sem, sent_min, got_min,
):
    count_pts, width = points_ref.shape
    blocksize = cents_ref.shape[0]
    planes = rows // PLANE
    wide = width // PARTS
    chunk = planes * cap
    me = lax.axis_index("rows")
    core = lax.axis_index("cent")
    z, q = me // PLANE, me % PLANE
    xpeer = z * PLANE + flip(q, 1)
    ypeer = z * PLANE + flip(q, 2)
    diag = z * PLANE + flip(q, 3)
    partner = 1 - core

    assign_in = pltpu.make_async_copy(assign_hbm, assign_ref, load_sem.at[2])
    assign_in.start()
    points_in = pltpu.make_async_copy(points_hbm, points_ref, load_sem.at[0])
    points_in.start()
    barrier = pltpu.get_barrier_semaphore()
    for bits in range(1, 4):
        pl.semaphore_signal(barrier, inc=1, device_id={"rows": z * PLANE + flip(q, bits)})
        pl.semaphore_signal(barrier, inc=1, device_id={"rows": flip(z, bits) * PLANE + q})
    pl.semaphore_signal(barrier, inc=1, device_id={"cent": partner})

    assign_in.wait()
    relative = (assign_ref[...] - core * blocksize).astype(jnp.float32)
    inside = (relative >= 0.0) & (relative < float(blocksize))
    owner = jnp.where(inside, jnp.floor(relative * (1.0 / share)), float(rows))
    offset1 = jnp.where(inside, relative - owner * share + 1.0, 0.0)
    hot = lax.broadcasted_iota(jnp.int32, (rows, count_pts), 0).astype(jnp.float32) == owner
    hot_f = jnp.where(hot, 1.0, 0.0)
    seg = 256
    tri = jnp.where(
        lax.broadcasted_iota(jnp.int32, (seg, seg), 0) < lax.broadcasted_iota(jnp.int32, (seg, seg), 1),
        1.0, 0.0,
    ).astype(jnp.bfloat16)
    carry = jnp.zeros((rows, 1), jnp.float32)
    pieces = []
    for s in range(count_pts // seg):
        part = hot_f[:, s * seg:(s + 1) * seg]
        before = jnp.dot(part.astype(jnp.bfloat16), tri, preferred_element_type=jnp.float32) + carry
        pieces.append(jnp.sum(part * before, axis=0, keepdims=True))
        carry = carry + jnp.sum(part, axis=1, keepdims=True)
    ranking = jnp.concatenate(pieces, axis=1)
    plane_to = jnp.floor(owner * (1.0 / PLANE))
    slot = jnp.where(inside, (owner - plane_to * PLANE) * chunk + plane_to * cap + ranking, -1.0)
    labels8 = jnp.broadcast_to(offset1, (8, count_pts)).astype(jnp.bfloat16)

    def ship(src, dst, ss, rs, axis, target):
        copy = pltpu.make_async_remote_copy(
            src_ref=src, dst_ref=dst, send_sem=ss, recv_sem=rs, device_id={axis: target}
        )
        copy.start()
        return copy

    def landed(ref, sem):
        pltpu.make_async_remote_copy(
            src_ref=ref, dst_ref=ref, send_sem=spare_sem.at[0], recv_sem=sem, device_id={"rows": xpeer}
        ).wait_recv()

    flying = []
    reach = (3, 1, 2)
    span = (3, 2, 1, 0)

    def place(k):
        i = flip(q, k)
        hit = (
            lax.broadcasted_iota(jnp.int32, (chunk, count_pts), 0) + i * chunk
        ).astype(jnp.float32) == slot
        placing = jnp.where(hit, 1.0, 0.0).astype(jnp.bfloat16)
        placing_ref[k] = placing
        lab = nt_dot(labels8, placing)
        for t in range(chunk // LANES):
            piece = lab[:, t * LANES:(t + 1) * LANES]
            if k:
                lab_send[k, t] = piece
            else:
                lab_arrived[q, t] = piece

    def fill(h, k):
        rows_out = jnp.dot(
            placing_ref[k], points_ref[:, h * wide:(h + 1) * wide], preferred_element_type=jnp.float32
        ).astype(jnp.bfloat16)
        if k:
            send[h, k] = rows_out
        else:
            for t in range(planes):
                arrived[h, t, pl.ds(pl.multiple_of(q * cap, cap), cap), :] = rows_out[t * cap:(t + 1) * cap]

    def dispatch(h, j, k):
        t = flip(z, span[j])
        spot = pl.ds(pl.multiple_of(q * cap, cap), cap)
        flying.append(ship(
            send.at[h, k, pl.ds(pl.multiple_of(t * cap, cap), cap)], arrived.at[h, t, spot],
            sent_pts.at[h, j, k], got_pts.at[h, t, q], "rows", z * PLANE + flip(q, k),
        ))

    points_in.wait()
    cents_in = pltpu.make_async_copy(cents_hbm, cents_ref, load_sem.at[1])
    cents_in.start()
    for k in reach:
        place(k)
        fill(0, k)
        if k == reach[0]:
            pl.semaphore_wait(barrier, 7)
        flying.append(ship(
            lab_send.at[k], lab_arrived.at[q], sent_lab.at[k], got_lab.at[q], "rows", z * PLANE + flip(q, k)
        ))
        dispatch(0, 0, k)
    for j in range(1, planes):
        for k in reach:
            dispatch(0, j, k)
    for h in range(1, PARTS):
        for k in reach:
            fill(h, k)
        for j in range(planes):
            for k in reach:
                dispatch(h, j, k)
    place(0)
    for h in range(PARTS):
        fill(h, 0)

    kb = 512
    pieces_first = blocksize // kb
    low[...] = jnp.full(low.shape, jnp.inf, jnp.float32)
    min_copies = []

    def first_piece(i):
        low[0:1, :] = jnp.minimum(low[0:1, :], column_min(cents_ref[i * kb:(i + 1) * kb, :], points_ref[...]))

    def point_norms():
        squares = jnp.square(points_ref[...].astype(jnp.float32))
        high = squares.astype(jnp.bfloat16)
        rest = (squares - high.astype(jnp.float32)).astype(jnp.bfloat16)
        ones = jnp.ones((8, width), jnp.bfloat16)
        return (nt_dot(ones, high) + nt_dot(ones, rest))[0:1, :]

    for k in reach:
        landed(lab_arrived.at[flip(q, k)], got_lab.at[flip(q, k)])
    lane = lax.broadcasted_iota(jnp.int32, (8, LANES), 1)
    for t in range(planes):
        for p in range(PLANE // 2):
            left, right = lab_arrived[2 * p, t // 2], lab_arrived[2 * p + 1, t // 2]
            if t % 2:
                left = pltpu.roll(left, cap, 1)
            else:
                right = pltpu.roll(right, cap, 1)
            klab[t, :, p * LANES:(p + 1) * LANES] = jnp.where(lane < cap, left, right)

    rowid1 = lax.broadcasted_iota(jnp.int32, (share, PLANE * cap), 0).astype(jnp.float32) + 1.0
    eye = lax.broadcasted_iota(jnp.int32, (share, LANES), 0) == lax.broadcasted_iota(
        jnp.int32, (share, LANES), 1
    )

    def to_row(column):
        return jnp.sum(jnp.where(eye, column, 0.0), axis=0, keepdims=True)

    def to_column(row):
        return jnp.sum(jnp.where(eye, row, 0.0), axis=1, keepdims=True)

    def gather_in(h, t):
        for k in reach:
            source = flip(q, k)
            landed(arrived.at[h, t, pl.ds(pl.multiple_of(source * cap, cap), cap)], got_pts.at[h, t, source])
        chosen = jnp.where(rowid1 == klab[t][0:1, :], 1.0, 0.0)
        counts = jnp.sum(chosen, axis=1, keepdims=True)
        total = jnp.dot(chosen.astype(jnp.bfloat16), arrived[h, t], preferred_element_type=jnp.float32)
        return total, counts

    def send_part(h, n, total, counts, target):
        peak = jnp.maximum(jnp.max(jnp.abs(total), axis=1, keepdims=True), 1e-30)
        grow = jnp.exp2(14.0 - jnp.floor(jnp.log2(peak)))
        grow = jnp.where(peak * grow >= 32767.0, grow * 0.5, grow)
        scaled = jnp.clip(jnp.round(total * grow), -32767.0, 32767.0)
        part_send[h, n] = scaled.astype(jnp.int32).astype(jnp.int16)
        first_row = lax.broadcasted_iota(jnp.int32, (8, LANES), 0) == 0
        meta_send[h, n] = jnp.where(first_row, to_row(1.0 / grow), to_row(counts))
        flying.append(ship(
            meta_send.at[h, n], meta_got.at[h, n], sent_meta.at[h, n], got_meta.at[h, n], "rows", target
        ))
        flying.append(ship(
            part_send.at[h, n], part_got.at[h, n], sent_part.at[h, n], got_part.at[h, n], "rows", target
        ))

    def take_part(h, n):
        landed(meta_got.at[h, n], got_meta.at[h, n])
        landed(part_got.at[h, n], got_part.at[h, n])
        meta = meta_got[h, n]
        return part_got[h, n].astype(jnp.int32).astype(jnp.float32) * to_column(meta[0:1, :]), to_column(meta[1:2, :])

    near_plane, far_plane = flip(z, 1) * PLANE + q, flip(z, 2) * PLANE + q

    def reduce_cross(h):
        send_part(h, 0, *gather_in(h, flip(z, 3)), near_plane)

    def reduce_hold(h):
        total, counts = gather_in(h, flip(z, 2))
        held[h] = total
        return counts

    def reduce_far(h, counts):
        more, extra = take_part(h, 0)
        send_part(h, 1, held[h] + more, counts + extra, far_plane)

    def reduce_near(h):
        send_part(h, 2, *gather_in(h, flip(z, 1)), near_plane)

    def reduce_own(h):
        total, counts = gather_in(h, z)
        own_rows = cents_ref[pl.ds(pl.multiple_of(me * share, share), share), h * wide:(h + 1) * wide]
        acc[h] = total + own_rows.astype(jnp.float32)
        return counts

    def renew_own(h, counts):
        total = acc[h]
        for n in (2, 1):
            more, extra = take_part(h, n)
            total, counts = total + more, counts + extra
        gath[me, :, h * wide:(h + 1) * wide] = (total / (counts + 1.0)).astype(jnp.bfloat16)

    top = z // 2
    visits = [z, z + 1 - 2 * (z % 2), 2 - top, 3 - 3 * top]
    waiting = []
    missing = {}

    def flat(h, n):
        return share if n == 0 else share - TALL[h]

    def view(block, h, first=0, count=share):
        return gath.at[block, pl.ds(first, count), h * wide:(h + 1) * wide]

    def tall(block, h):
        return view(block, h, share - TALL[h], TALL[h])

    def pass_on(h, block, n):
        part = view(block, h, 0, flat(h, n))
        for sem, target in ((sent_x, xpeer), (sent_y, ypeer)):
            flying.append(ship(part, part, sem.at[h, n], got_full.at[h, block], "rows", target))

    def climb(part, got, sems):
        for n in range(1, planes):
            flying.append(ship(part, part, sems(n), got, "rows", visits[n] * PLANE + q))

    def settle(h, n, kind, block):
        key = (n, kind)
        missing.setdefault(key, PARTS + (1 if n and kind != "q" else 0) * sum(1 for r in TALL if r))
        missing[key] -= 1
        if missing[key] == 0:
            waiting.append(block)
        while len(waiting) >= 2:
            drain(2)

    def drain(n):
        taken, waiting[:] = waiting[:n], waiting[n:]
        block = jnp.concatenate([gath[b] for b in taken], axis=0) if n > 1 else gath[taken[0]]
        low[1:2, :] = jnp.minimum(low[1:2, :], column_min(block, points_ref[...]))

    def spread_start(h):
        climb(view(me, h), got_col.at[h, me], lambda n: sent_col.at[h, n])
        pass_on(h, me, 0)
        settle(h, 0, "q", me)

    def spread_step(h, n):
        block = visits[n] * PLANE + q
        landed(view(block, h), got_col.at[h, block])
        pass_on(h, block, n)
        settle(h, n, "q", block)

    def spread_cross(h, n):
        by, bx = visits[n] * PLANE + ypeer % PLANE, visits[n] * PLANE + xpeer % PLANE
        count, half = flat(h, n), flat(h, n) // 2
        landed(view(by, h, 0, count), got_full.at[h, by])
        part = view(by, h, 0, half)
        flying.append(ship(part, part, sent_dx.at[h, n], got_dx.at[h, by], "rows", xpeer))
        landed(view(bx, h, 0, count), got_full.at[h, bx])
        part = view(bx, h, half, half)
        flying.append(ship(part, part, sent_dy.at[h, n], got_dy.at[h, bx], "rows", ypeer))
        settle(h, n, "y", by)
        settle(h, n, "x", bx)

    def spread_diag(h, n):
        bd, half = visits[n] * PLANE + diag % PLANE, flat(h, n) // 2
        landed(view(bd, h, 0, half), got_dx.at[h, bd])
        landed(view(bd, h, half, half), got_dy.at[h, bd])
        settle(h, n, "d", bd)

    def spread_tall(h, n):
        for i, (kind, mate) in enumerate((("x", xpeer), ("y", ypeer), ("d", diag))):
            block = visits[n] * PLANE + mate % PLANE
            got = got_tall.at[h, block]
            if n:
                landed(tall(block, h), got)
                settle(h, n, kind, block)
            else:
                climb(tall(block, h), got, lambda n, i=i: sent_tall.at[h, n, i])

    cents_in.wait()
    reduce_cross(0)
    first_piece(0)
    counts = reduce_hold(0)
    first_piece(1)
    reduce_far(0, counts)
    reduce_near(0)
    first_piece(2)
    counts = reduce_own(0)
    for i in range(planes - 1, pieces_first):
        first_piece(i)
    renew_own(0, counts)
    spread_start(0)
    reduce_cross(1)
    pnorm = point_norms()
    mine[0] = (pnorm + low[0:1, :]) / width
    min_copies.append(ship(mine.at[0], theirs.at[0], sent_min.at[0], got_min.at[0], "cent", partner))
    counts = reduce_hold(1)
    reduce_far(1, counts)
    reduce_near(1)
    spread_step(0, 1)
    counts = reduce_own(1)
    renew_own(1, counts)
    spread_start(1)
    spread_cross(0, 0)
    spread_step(0, 2)
    spread_step(0, 3)
    spread_step(1, 1)
    spread_cross(1, 0)
    spread_cross(0, 1)
    spread_step(1, 2)
    spread_diag(1, 0)
    spread_tall(1, 0)
    spread_step(1, 3)
    spread_cross(0, 2)
    spread_cross(0, 3)
    spread_cross(1, 1)
    spread_diag(0, 0)
    spread_diag(0, 1)
    spread_cross(1, 2)
    spread_tall(1, 1)
    spread_diag(0, 2)
    spread_diag(1, 1)
    spread_cross(1, 3)
    spread_tall(1, 2)
    spread_diag(0, 3)
    spread_diag(1, 2)
    spread_tall(1, 3)
    spread_diag(1, 3)
    if waiting:
        drain(len(waiting))

    mine[1] = (pnorm + low[1:2, :]) / width
    min_copies.append(ship(mine.at[1], theirs.at[1], sent_min.at[1], got_min.at[1], "cent", partner))
    for copy in flying:
        copy.wait_send()
    for n, copy in enumerate(min_copies):
        copy.wait()
        near_ref[n:n + 1, :] = jnp.minimum(mine[n], theirs[n])


def deliver(near_ref, gath_ref, near_out, upd_out, sems):
    copies = [
        pltpu.make_async_copy(gath_ref, upd_out, sems.at[0]),
        pltpu.make_async_copy(near_ref, near_out, sems.at[1]),
    ]
    for copy in copies:
        copy.start()
    for copy in copies:
        copy.wait()


def fused(points, centroids, assign, rows, cap, share):
    count_pts, width = points.shape
    planes = rows // PLANE
    hbm = pl.BlockSpec(memory_space=pltpu.HBM)
    vmem = pl.BlockSpec(memory_space=pltpu.VMEM)
    dma = pltpu.SemaphoreType.DMA
    chunk = planes * cap
    wide = width // PARTS
    shapes = (
        jax.ShapeDtypeStruct((2, count_pts), jnp.float32),
        jax.ShapeDtypeStruct((rows, share, width), jnp.bfloat16),
    )
    hops = planes - 1
    near, upd = pl.pallas_call(
        functools.partial(lloyd_kernel, rows, cap, share),
        out_shape=shapes,
        in_specs=[hbm, hbm, hbm],
        out_specs=(vmem, vmem),
        scratch_shapes=[
            pltpu.VMEM((1, count_pts), jnp.int32),
            pltpu.VMEM((count_pts, width), jnp.bfloat16),
            pltpu.VMEM(centroids.shape, jnp.bfloat16),
            dma((3,)),
            pltpu.VMEM((PLANE, chunk, count_pts), jnp.bfloat16),
            pltpu.VMEM((PARTS, PLANE, chunk, wide), jnp.bfloat16),
            pltpu.VMEM((PLANE, chunk // LANES, 8, LANES), jnp.float32),
            pltpu.VMEM((PARTS, planes, PLANE * cap, wide), jnp.bfloat16),
            pltpu.VMEM((PLANE, chunk // LANES, 8, LANES), jnp.float32),
            pltpu.VMEM((planes, 8, PLANE * cap), jnp.float32),
            pltpu.VMEM((PARTS, hops, share, wide), jnp.int16),
            pltpu.VMEM((PARTS, hops, 8, LANES), jnp.float32),
            pltpu.VMEM((PARTS, hops, share, wide), jnp.int16),
            pltpu.VMEM((PARTS, hops, 8, LANES), jnp.float32),
            pltpu.VMEM((PARTS, share, wide), jnp.float32),
            pltpu.VMEM((PARTS, share, wide), jnp.float32),
            pltpu.VMEM((2, 1, count_pts), jnp.float32),
            pltpu.VMEM((2, 1, count_pts), jnp.float32),
            pltpu.VMEM((8, count_pts), jnp.float32),
            dma((PARTS, planes, PLANE)), dma((PARTS, planes, PLANE)), dma((PLANE,)), dma((PLANE,)),
            dma((PARTS, hops)), dma((PARTS, hops)), dma((PARTS, hops)), dma((PARTS, hops)),
            dma((PARTS, planes)), dma((PARTS, rows)), dma((PARTS, planes, 3)), dma((PARTS, rows)),
            dma((PARTS, planes)), dma((PARTS, planes)), dma((PARTS, rows)),
            dma((PARTS, planes)), dma((PARTS, planes)), dma((PARTS, rows)), dma((PARTS, rows)), dma((1,)),
            dma((2,)), dma((2,)),
        ],
        compiler_params=pltpu.CompilerParams(
            collective_id=0, has_side_effects=True, vmem_limit_bytes=VMEM_BYTES
        ),
    )(
        pltpu.with_memory_space_constraint(assign[None, :], pltpu.HBM),
        pltpu.with_memory_space_constraint(points, pltpu.HBM),
        pltpu.with_memory_space_constraint(centroids, pltpu.HBM),
    )
    near, upd = pl.pallas_call(
        deliver,
        out_shape=shapes,
        in_specs=[vmem, vmem],
        out_specs=(hbm, hbm),
        scratch_shapes=[dma((2,))],
        compiler_params=pltpu.CompilerParams(vmem_limit_bytes=1024 * 1024),
    )(near, upd)
    return near, upd.reshape(rows * share, width)


def step(rows, cent, points, centroids, assign):
    count_pts = points.shape[0]
    blocksize = centroids.shape[0]
    share = blocksize // rows
    cap = max(2, 2 * count_pts // (rows * cent))
    fits = cent == 2 and rows == 4 * PLANE and share == LANES and 2 * cap == LANES
    even = count_pts % 256 == 0 and blocksize % 512 == 0 and points.shape[1] % (PARTS * LANES) == 0
    if fits and even:
        return fused(points, centroids, assign, rows, cap, share)
    return per_device(points, centroids, assign)


def solution(mesh):
    return jax.shard_map(
        functools.partial(step, mesh.shape["rows"], mesh.shape["cent"]),
        mesh=mesh,
        in_specs=(P("rows", None), P("cent", None), P("rows")),
        out_specs=(P(None, "rows"), P("cent", None)),
        check_vma=False,
    )
```

```python
import functools

import jax
import jax.numpy as jnp
from jax import lax
from jax.experimental import pallas as pl
from jax.experimental.pallas import tpu as pltpu
from jax.sharding import PartitionSpec as P


def smallest(points, pnorm, cents):
    cnorm = jnp.sum(jnp.square(cents.astype(jnp.float32)), axis=1)
    dots = lax.dot_general(
        points, cents, (((1,), (1,)), ((), ())), preferred_element_type=jnp.float32
    )
    return jnp.min((pnorm[:, None] - 2.0 * dots + cnorm[None, :]) / points.shape[1], axis=1)


def block_min(values):
    return lax.pmin(values, "cent")


def renew(part_sums, part_counts, own_rows):
    return ((part_sums + own_rows.astype(jnp.float32)) / (part_counts[:, None] + 1.0)).astype(
        jnp.bfloat16
    )


def per_device(points, centroids, assign):
    blocksize = centroids.shape[0]
    count_pts = points.shape[0]
    pnorm = jnp.sum(jnp.square(points.astype(jnp.float32)), axis=1)
    first = smallest(points, pnorm, centroids)
    first = block_min(first)
    relative = assign - lax.axis_index("cent") * blocksize
    share = blocksize // lax.axis_size("rows")
    own = lax.dynamic_slice_in_dim(centroids, lax.axis_index("rows") * share, share, 0)
    rows_count = lax.axis_size("rows")
    groups = rows_count * lax.axis_size("cent")
    capacity = max(2, 2 * count_pts // groups)
    inside = (relative >= 0) & (relative < blocksize)
    owners = jnp.where(inside, relative // share, rows_count)
    offsets = jnp.where(inside, relative - relative // share * share, 0)
    owner_hot = owners[:, None] == lax.broadcasted_iota(jnp.int32, (count_pts, rows_count), 1)
    earlier = lax.broadcasted_iota(jnp.int32, (count_pts, count_pts), 1) < lax.broadcasted_iota(
        jnp.int32, (count_pts, count_pts), 0
    )
    before = jnp.dot(
        earlier.astype(jnp.bfloat16),
        owner_hot.astype(jnp.bfloat16),
        preferred_element_type=jnp.float32,
    )
    ranking = jnp.sum(jnp.where(owner_hot, before, 0.0), axis=1).astype(jnp.int32)
    slot_index = jnp.where(inside, owners * capacity + ranking, -1)
    placing = (
        lax.broadcasted_iota(jnp.int32, (rows_count * capacity, count_pts), 0)
        == slot_index[None, :]
    )
    outgoing = jnp.dot(
        placing.astype(jnp.bfloat16), points, preferred_element_type=jnp.float32
    ).astype(jnp.bfloat16)
    labels = (jnp.sum(jnp.where(placing, offsets[None, :] + 1, 0), axis=1) - 1).astype(jnp.bfloat16)
    arrived, arrived_labels = (
        lax.all_to_all(outgoing, "rows", split_axis=0, concat_axis=0, tiled=True),
        lax.all_to_all(labels, "rows", split_axis=0, concat_axis=0, tiled=True),
    )
    chosen = (
        lax.broadcasted_iota(jnp.int32, (share, arrived.shape[0]), 0)
        == arrived_labels.astype(jnp.int32)[None, :]
    )
    part_sums = jnp.dot(chosen.astype(jnp.bfloat16), arrived, preferred_element_type=jnp.float32)
    part_counts = jnp.sum(chosen.astype(jnp.float32), axis=1)
    updated = lax.all_gather(renew(part_sums, part_counts, own), "rows", axis=0, tiled=True)
    second = smallest(points, pnorm, updated)
    nearest = jnp.stack([first, block_min(second)])
    return (nearest, updated)


PLANE = 4
LANES = 128
VMEM_BYTES = 44 * 1024 * 1024
PARTS = 2
TALL = (0, 0)


def nt_dot(a, b):
    return lax.dot_general(a, b, (((1,), (1,)), ((), ())), preferred_element_type=jnp.float32)


def column_min(cents, points):
    wide = cents.astype(jnp.float32)
    cnorm = jnp.sum(wide * wide, axis=1, keepdims=True)
    return jnp.min(cnorm - 2.0 * nt_dot(cents, points), axis=0, keepdims=True)


def flip(index, bits):
    low, high = index % 2, index // 2
    if bits % 2:
        low = 1 - low
    if bits // 2:
        high = 1 - high
    return high * 2 + low


def lloyd_kernel(
    rows, cap, share, assign_hbm, points_hbm, cents_hbm, near_ref, gath,
    assign_ref, points_ref, cents_ref, load_sem,
    placing_ref, send, lab_send, arrived, lab_arrived, klab,
    part_send, meta_send, part_got, meta_got, part_in, meta_in, held, tally, mine, theirs, low,
    sent_pts, got_pts, sent_lab, got_lab, sent_part, got_part, sent_meta, got_in,
    sent_gath, sent_col, sent_tall, got_col, got_tall, got_side, got_diag, spare_sem, sent_min, got_min,
):
    count_pts, width = points_ref.shape
    blocksize = cents_ref.shape[0]
    planes = rows // PLANE
    wide = width // PARTS
    chunk = planes * cap
    me = lax.axis_index("rows")
    core = lax.axis_index("cent")
    z, q = me // PLANE, me % PLANE
    xpeer = z * PLANE + flip(q, 1)
    ypeer = z * PLANE + flip(q, 2)
    diag = z * PLANE + flip(q, 3)
    partner = 1 - core

    assign_in = pltpu.make_async_copy(assign_hbm, assign_ref, load_sem.at[2])
    assign_in.start()
    points_in = pltpu.make_async_copy(points_hbm, points_ref, load_sem.at[0])
    points_in.start()
    barrier = pltpu.get_barrier_semaphore()
    for bits in range(1, 4):
        pl.semaphore_signal(barrier, inc=1, device_id={"rows": z * PLANE + flip(q, bits)})
        pl.semaphore_signal(barrier, inc=1, device_id={"rows": flip(z, bits) * PLANE + q})
    pl.semaphore_signal(barrier, inc=1, device_id={"cent": partner})

    assign_in.wait()
    relative = (assign_ref[...] - core * blocksize).astype(jnp.float32)
    inside = (relative >= 0.0) & (relative < float(blocksize))
    owner = jnp.where(inside, jnp.floor(relative * (1.0 / share)), float(rows))
    offset1 = jnp.where(inside, relative - owner * share + 1.0, 0.0)
    hot = lax.broadcasted_iota(jnp.int32, (rows, count_pts), 0).astype(jnp.float32) == owner
    hot_f = jnp.where(hot, 1.0, 0.0)
    seg = 256
    tri = jnp.where(
        lax.broadcasted_iota(jnp.int32, (seg, seg), 0) < lax.broadcasted_iota(jnp.int32, (seg, seg), 1),
        1.0, 0.0,
    ).astype(jnp.bfloat16)
    carry = jnp.zeros((rows, 1), jnp.float32)
    pieces = []
    for s in range(count_pts // seg):
        part = hot_f[:, s * seg:(s + 1) * seg]
        before = jnp.dot(part.astype(jnp.bfloat16), tri, preferred_element_type=jnp.float32) + carry
        pieces.append(jnp.sum(part * before, axis=0, keepdims=True))
        carry = carry + jnp.sum(part, axis=1, keepdims=True)
    ranking = jnp.concatenate(pieces, axis=1)
    side_to = jnp.floor(owner * (1.0 / (2 * PLANE)))
    pair_to = jnp.floor(owner * 0.5)
    column_to, lane_to = pair_to - side_to * PLANE, side_to * 2.0 + owner - pair_to * 2.0
    slot = jnp.where(inside, column_to * chunk + lane_to * cap + ranking, -1.0)
    labels8 = jnp.broadcast_to(offset1, (8, count_pts)).astype(jnp.bfloat16)

    def ship(src, dst, ss, rs, axis, target):
        copy = pltpu.make_async_remote_copy(
            src_ref=src, dst_ref=dst, send_sem=ss, recv_sem=rs, device_id={axis: target}
        )
        copy.start()
        return copy

    def landed(ref, sem):
        pltpu.make_async_remote_copy(
            src_ref=ref, dst_ref=ref, send_sem=spare_sem.at[0], recv_sem=sem, device_id={"rows": xpeer}
        ).wait_recv()

    def sent_all(ref, sem):
        pltpu.make_async_remote_copy(
            src_ref=ref, dst_ref=ref, send_sem=sem, recv_sem=spare_sem.at[0], device_id={"rows": xpeer}
        ).wait_send()

    reach = (3, 1, 2)
    side = z // 2
    inner = (z > 0) & (z < planes - 1)
    outer = jnp.logical_not(inner)
    beside, across = flip(z, 1) * PLANE + q, (planes - 1 - z) * PLANE + q
    order = (2 - 2 * side, 3 - 2 * side, 2 * side, 2 * side + 1)

    def place(k):
        i = flip(q, k)
        hit = (
            lax.broadcasted_iota(jnp.int32, (chunk, count_pts), 0) + i * chunk
        ).astype(jnp.float32) == slot
        placing = jnp.where(hit, 1.0, 0.0).astype(jnp.bfloat16)
        placing_ref[k] = placing
        lab = nt_dot(labels8, placing)
        for t in range(chunk // LANES):
            piece = lab[:, t * LANES:(t + 1) * LANES]
            if k:
                lab_send[k, t] = piece
            else:
                lab_arrived[q, t] = piece

    def fill(h, k):
        rows_out = jnp.dot(
            placing_ref[k], points_ref[:, h * wide:(h + 1) * wide], preferred_element_type=jnp.float32
        ).astype(jnp.bfloat16)
        if k:
            send[h, k] = rows_out
        else:
            for t in range(planes):
                arrived[h, t, pl.ds(pl.multiple_of(q * cap, cap), cap), :] = rows_out[t * cap:(t + 1) * cap]

    def dispatch(h, j, k):
        t = order[j]
        spot = pl.ds(pl.multiple_of(q * cap, cap), cap)
        ship(
            send.at[h, k, pl.ds(pl.multiple_of(t * cap, cap), cap)], arrived.at[h, t, spot],
            sent_pts.at[0], got_pts.at[h, t], "rows", z * PLANE + flip(q, k),
        )

    place(reach[0])
    points_in.wait()
    cents_in = pltpu.make_async_copy(cents_hbm, cents_ref, load_sem.at[1])
    cents_in.start()
    for k in reach:
        if k != reach[0]:
            place(k)
        fill(0, k)
        if k == reach[0]:
            pl.semaphore_wait(barrier, 7)
        ship(
            lab_send.at[k], lab_arrived.at[q], sent_lab.at[0], got_lab.at[0], "rows", z * PLANE + flip(q, k)
        )
        dispatch(0, 0, k)
    for j in range(1, planes):
        for k in reach:
            dispatch(0, j, k)
    for h in range(1, PARTS):
        for k in reach:
            fill(h, k)
        for j in range(planes):
            for k in reach:
                dispatch(h, j, k)
    place(0)
    for h in range(PARTS):
        fill(h, 0)

    kb = 512
    pieces_first = blocksize // kb
    low[...] = jnp.full(low.shape, jnp.inf, jnp.float32)
    min_copies = []

    def first_piece(i):
        low[0:1, :] = jnp.minimum(low[0:1, :], column_min(cents_ref[i * kb:(i + 1) * kb, :], points_ref[...]))

    def point_norms():
        squares = jnp.square(points_ref[...].astype(jnp.float32))
        high = squares.astype(jnp.bfloat16)
        rest = (squares - high.astype(jnp.float32)).astype(jnp.bfloat16)
        ones = jnp.ones((8, width), jnp.bfloat16)
        return (nt_dot(ones, high) + nt_dot(ones, rest))[0:1, :]

    landed(lab_arrived.at[0:PLANE - 1], got_lab.at[0])
    lane = lax.broadcasted_iota(jnp.int32, (8, LANES), 1)
    for t in range(planes):
        for p in range(PLANE // 2):
            left, right = lab_arrived[2 * p, t // 2], lab_arrived[2 * p + 1, t // 2]
            if t % 2:
                left = pltpu.roll(left, cap, 1)
            else:
                right = pltpu.roll(right, cap, 1)
            klab[t, :, p * LANES:(p + 1) * LANES] = jnp.where(lane < cap, left, right)

    rowid1 = lax.broadcasted_iota(jnp.int32, (share, PLANE * cap), 0).astype(jnp.float32) + 1.0
    eye = lax.broadcasted_iota(jnp.int32, (share, LANES), 0) == lax.broadcasted_iota(
        jnp.int32, (share, LANES), 1
    )

    def to_row(column):
        return jnp.sum(jnp.where(eye, column, 0.0), axis=0, keepdims=True)

    def to_column(row):
        return jnp.sum(jnp.where(eye, row, 0.0), axis=1, keepdims=True)

    def gather_in(h, t):
        landed(arrived.at[h, t, 0:(PLANE - 1) * cap], got_pts.at[h, t])
        chosen = jnp.where(rowid1 == klab[t][0:1, :], 1.0, 0.0)
        counts = jnp.sum(chosen, axis=1, keepdims=True)
        total = jnp.dot(chosen.astype(jnp.bfloat16), arrived[h, t], preferred_element_type=jnp.float32)
        return total, counts

    def send_part(h, j, total, counts, part_to, meta_to, got, target):
        peak = jnp.maximum(jnp.max(jnp.abs(total), axis=1, keepdims=True), 1e-30)
        grow = jnp.exp2(14.0 - jnp.floor(jnp.log2(peak)))
        grow = jnp.where(peak * grow >= 32767.0, grow * 0.5, grow)
        scaled = jnp.clip(jnp.round(total * grow), -32767.0, 32767.0)
        part_send[h, j] = scaled.astype(jnp.int32).astype(jnp.int16)
        first_row = lax.broadcasted_iota(jnp.int32, (8, LANES), 0) == 0
        meta_send[h, j] = jnp.where(first_row, to_row(1.0 / grow), to_row(counts))
        ship(meta_send.at[h, j], meta_to, sent_meta.at[0], got.at[1], "rows", target)
        ship(part_send.at[h, j], part_to, sent_part.at[0], got.at[0], "rows", target)

    def take_part(part_from, meta_from, got):
        landed(meta_from, got.at[1])
        landed(part_from, got.at[0])
        meta = meta_from[...]
        return part_from[...].astype(jnp.int32).astype(jnp.float32) * to_column(meta[0:1, :]), to_column(meta[1:2, :])

    def reduce_in(h, j):
        t = order[j]
        total, counts = gather_in(h, t)

        @pl.when(outer)
        def _():
            send_part(h, j, total, counts, part_got.at[h, t], meta_got.at[h, t], got_part.at[h, t], beside)

        @pl.when(inner)
        def _():
            held[h, j] = total
            tally[h, j] = counts

    def reduce_far(h, j):
        @pl.when(inner)
        def _():
            t = order[j]
            more, extra = take_part(part_got.at[h, t], meta_got.at[h, t], got_part.at[h, t])
            send_part(
                h, j, held[h, j] + more, tally[h, j] + extra, part_in.at[h, j], meta_in.at[h, j], got_in.at[h, j], across
            )

    def renew(h):
        @pl.when(inner)
        def _():
            for p in range(2):
                block, t = side * 2 * PLANE + 2 * q + p, order[2 + p]
                rows_own = cents_ref[pl.ds(pl.multiple_of(block * share, share), share), h * wide:(h + 1) * wide]
                total, counts = held[h, 2 + p] + rows_own.astype(jnp.float32), tally[h, 2 + p]
                more, extra = take_part(part_got.at[h, t], meta_got.at[h, t], got_part.at[h, t])
                total, counts = total + more, counts + extra
                more, extra = take_part(part_in.at[h, p], meta_in.at[h, p], got_in.at[h, p])
                total, counts = total + more, counts + extra
                gath[block, :, h * wide:(h + 1) * wide] = (total / (counts + 1.0)).astype(jnp.bfloat16)

    waiting = {}

    def sides(n):
        return (side, 1 - side)[n]

    def cols(h):
        return slice(h * wide, (h + 1) * wide)

    def pair(h, n, mate, first=0, count=share):
        return gath.at[pl.ds(sides(n) * 2 * PLANE + 2 * (mate % PLANE), 2), pl.ds(first, count), cols(h)]

    def one(h, n, p):
        return gath.at[sides(n) * 2 * PLANE + 2 * q + p, :, cols(h)]

    def pile(h, blocks, count):
        return gath.at[0:blocks, pl.ds(0, count), cols(h)]

    def flat(h, n, within):
        return share if within and n == 0 else share - TALL[h]

    def by_role(body):
        @pl.when(inner)
        def _():
            body(True)

        @pl.when(outer)
        def _():
            body(False)

    def settle(h, n, kind, mate):
        key = (n, kind)
        waiting.setdefault(key, PARTS + (0 if kind == "q" else sum(1 for r in TALL if r)))
        waiting[key] -= 1
        if waiting[key] == 0:
            first = sides(n) * 2 * PLANE + 2 * (mate % PLANE)
            block = jnp.concatenate([gath[first], gath[first + 1]], axis=0)
            low[1:2, :] = jnp.minimum(low[1:2, :], column_min(block, points_ref[...]))

    def pass_on(h, n, count):
        part = pair(h, n, me, 0, count)
        for target in (xpeer, ypeer):
            ship(part, part, sent_gath.at[h], got_side.at[h, n], "rows", target)

    def start_inner(h):
        @pl.when(inner)
        def _():
            for p in range(2):
                ship(one(h, 0, p), one(h, 0, p), sent_col.at[h], got_col.at[h, 1, p], "rows", across)
                ship(one(h, 0, p), one(h, 0, p), sent_col.at[h], got_col.at[h, 0, p], "rows", beside)
            pass_on(h, 0, share)

    def start_outer(h):
        @pl.when(outer)
        def _():
            for p in range(2):
                landed(one(h, 0, p), got_col.at[h, 0, p])
            pass_on(h, 0, flat(h, 0, False))
        settle(h, 0, "q", me)

    def next_inner(h):
        @pl.when(inner)
        def _():
            for p in range(2):
                landed(one(h, 1, p), got_col.at[h, 1, p])
                ship(one(h, 1, p), one(h, 1, p), sent_col.at[h], got_col.at[h, 1, p], "rows", beside)
            pass_on(h, 1, flat(h, 1, True))

    def next_outer(h):
        @pl.when(outer)
        def _():
            for p in range(2):
                landed(one(h, 1, p), got_col.at[h, 1, p])
            pass_on(h, 1, flat(h, 1, False))
        settle(h, 1, "q", me)

    def spread_cross(h, n):
        def body(within):
            count = flat(h, n, within)
            landed(pile(h, 4, count), got_side.at[h, n])
            for mate, first, target in ((ypeer, 0, xpeer), (xpeer, count // 2, ypeer)):
                part = pair(h, n, mate, first, count // 2)
                ship(part, part, sent_gath.at[h], got_diag.at[h, n], "rows", target)
        if n == 0 and TALL[h]:
            by_role(body)
        else:
            body(False)
        settle(h, n, "y", ypeer)
        settle(h, n, "x", xpeer)

    def spread_diag(h, n):
        def body(within):
            landed(pile(h, 2, flat(h, n, within)), got_diag.at[h, n])
        if n == 0 and TALL[h]:
            by_role(body)
        else:
            body(False)
        settle(h, n, "d", diag)

    def spread_tall(h, n):
        count = TALL[h]
        if n == 0:
            @pl.when(outer)
            def _():
                landed(pile(h, 6, count), got_tall.at[h, 0])
        else:
            landed(pile(h, 6, count), got_tall.at[h, 1])

        @pl.when(inner)
        def _():
            for mate in (xpeer, ypeer, diag):
                part = pair(h, n, mate, share - count, count)
                if n == 0:
                    ship(part, part, sent_tall.at[h], got_tall.at[h, 1], "rows", across)
                ship(part, part, sent_tall.at[h], got_tall.at[h, n], "rows", beside)
        for kind, mate in (("x", xpeer), ("y", ypeer), ("d", diag)):
            settle(h, n, kind, mate)

    cents_in.wait()
    reduce_in(0, 0)
    first_piece(0)
    reduce_in(0, 1)
    first_piece(1)
    reduce_far(0, 0)
    reduce_in(0, 2)
    first_piece(2)
    reduce_far(0, 1)
    reduce_in(0, 3)
    for i in range(planes - 1, pieces_first):
        first_piece(i)
    renew(0)
    start_inner(0)
    reduce_in(1, 0)
    pnorm = point_norms()
    mine[0] = (pnorm + low[0:1, :]) / width
    min_copies.append(ship(mine.at[0], theirs.at[0], sent_min.at[0], got_min.at[0], "cent", partner))
    reduce_in(1, 1)
    reduce_far(1, 0)
    reduce_in(1, 2)
    reduce_far(1, 1)
    next_inner(0)
    start_outer(0)
    reduce_in(1, 3)
    renew(1)
    start_inner(1)
    next_outer(0)
    spread_cross(0, 0)
    spread_cross(0, 1)
    next_inner(1)
    start_outer(1)
    next_outer(1)
    spread_cross(1, 0)
    spread_cross(1, 1)
    spread_diag(0, 0)
    spread_diag(0, 1)
    spread_diag(1, 0)
    spread_diag(1, 1)

    mine[1] = (pnorm + low[1:2, :]) / width
    min_copies.append(ship(mine.at[1], theirs.at[1], sent_min.at[1], got_min.at[1], "cent", partner))
    sent_all(send.at[:, 1:], sent_pts.at[0])
    sent_all(lab_send.at[1:], sent_lab.at[0])

    @pl.when(outer)
    def _():
        sent_all(part_send, sent_part.at[0])
        sent_all(meta_send, sent_meta.at[0])
        for h in range(PARTS):
            sent_all(pile(h, 3 * PLANE, flat(h, 0, False)), sent_gath.at[h])

    @pl.when(inner)
    def _():
        sent_all(part_send.at[:, 0:2], sent_part.at[0])
        sent_all(meta_send.at[:, 0:2], sent_meta.at[0])
        for h in range(PARTS):
            sent_all(pile(h, 3 * PLANE, (share + flat(h, 1, True)) // 2), sent_gath.at[h])
            sent_all(pile(h, 6, share), sent_col.at[h])
            if TALL[h]:
                sent_all(pile(h, 9, 2 * TALL[h]), sent_tall.at[h])

    for n, copy in enumerate(min_copies):
        copy.wait()
        near_ref[n:n + 1, :] = jnp.minimum(mine[n], theirs[n])


def deliver(near_ref, gath_ref, near_out, upd_out, sems):
    copies = [
        pltpu.make_async_copy(gath_ref, upd_out, sems.at[0]),
        pltpu.make_async_copy(near_ref, near_out, sems.at[1]),
    ]
    for copy in copies:
        copy.start()
    for copy in copies:
        copy.wait()


def fused(points, centroids, assign, rows, cap, share):
    count_pts, width = points.shape
    planes = rows // PLANE
    hbm = pl.BlockSpec(memory_space=pltpu.HBM)
    vmem = pl.BlockSpec(memory_space=pltpu.VMEM)
    dma = pltpu.SemaphoreType.DMA
    chunk = planes * cap
    wide = width // PARTS
    shapes = (
        jax.ShapeDtypeStruct((2, count_pts), jnp.float32),
        jax.ShapeDtypeStruct((rows, share, width), jnp.bfloat16),
    )
    near, upd = pl.pallas_call(
        functools.partial(lloyd_kernel, rows, cap, share),
        out_shape=shapes,
        in_specs=[hbm, hbm, hbm],
        out_specs=(vmem, vmem),
        scratch_shapes=[
            pltpu.VMEM((1, count_pts), jnp.int32),
            pltpu.VMEM((count_pts, width), jnp.bfloat16),
            pltpu.VMEM(centroids.shape, jnp.bfloat16),
            dma((3,)),
            pltpu.VMEM((PLANE, chunk, count_pts), jnp.bfloat16),
            pltpu.VMEM((PARTS, PLANE, chunk, wide), jnp.bfloat16),
            pltpu.VMEM((PLANE, chunk // LANES, 8, LANES), jnp.float32),
            pltpu.VMEM((PARTS, planes, PLANE * cap, wide), jnp.bfloat16),
            pltpu.VMEM((PLANE, chunk // LANES, 8, LANES), jnp.float32),
            pltpu.VMEM((planes, 8, PLANE * cap), jnp.float32),
            pltpu.VMEM((PARTS, planes, share, wide), jnp.int16),
            pltpu.VMEM((PARTS, planes, 8, LANES), jnp.float32),
            pltpu.VMEM((PARTS, planes, share, wide), jnp.int16),
            pltpu.VMEM((PARTS, planes, 8, LANES), jnp.float32),
            pltpu.VMEM((PARTS, 2, share, wide), jnp.int16),
            pltpu.VMEM((PARTS, 2, 8, LANES), jnp.float32),
            pltpu.VMEM((PARTS, planes, share, wide), jnp.float32),
            pltpu.VMEM((PARTS, planes, share, 1), jnp.float32),
            pltpu.VMEM((2, 1, count_pts), jnp.float32),
            pltpu.VMEM((2, 1, count_pts), jnp.float32),
            pltpu.VMEM((8, count_pts), jnp.float32),
            dma((1,)), dma((PARTS, planes)), dma((1,)), dma((1,)),
            dma((1,)), dma((PARTS, planes, 2)), dma((1,)), dma((PARTS, 2, 2)),
            dma((PARTS,)), dma((PARTS,)), dma((PARTS,)),
            dma((PARTS, 2, 2)), dma((PARTS, 2)), dma((PARTS, 2)), dma((PARTS, 2)),
            dma((1,)), dma((2,)), dma((2,)),
        ],
        compiler_params=pltpu.CompilerParams(
            collective_id=0, has_side_effects=True, vmem_limit_bytes=VMEM_BYTES
        ),
    )(
        pltpu.with_memory_space_constraint(assign[None, :], pltpu.HBM),
        pltpu.with_memory_space_constraint(points, pltpu.HBM),
        pltpu.with_memory_space_constraint(centroids, pltpu.HBM),
    )
    near, upd = pl.pallas_call(
        deliver,
        out_shape=shapes,
        in_specs=[vmem, vmem],
        out_specs=(hbm, hbm),
        scratch_shapes=[dma((2,))],
        compiler_params=pltpu.CompilerParams(vmem_limit_bytes=1024 * 1024),
    )(near, upd)
    return near, upd.reshape(rows * share, width)


def step(rows, cent, points, centroids, assign):
    count_pts = points.shape[0]
    blocksize = centroids.shape[0]
    share = blocksize // rows
    cap = max(2, 2 * count_pts // (rows * cent))
    fits = cent == 2 and rows == 4 * PLANE and share == LANES and 2 * cap == LANES
    even = count_pts % 256 == 0 and blocksize % 512 == 0 and points.shape[1] % (PARTS * LANES) == 0
    if fits and even:
        return fused(points, centroids, assign, rows, cap, share)
    return per_device(points, centroids, assign)


def solution(mesh):
    return jax.shard_map(
        functools.partial(step, mesh.shape["rows"], mesh.shape["cent"]),
        mesh=mesh,
        in_specs=(P("rows", None), P("cent", None), P("rows")),
        out_specs=(P(None, "rows"), P("cent", None)),
        check_vma=False,
    )
```

```python
import functools

import jax
import jax.numpy as jnp
from jax import lax
from jax.experimental import pallas as pl
from jax.experimental.pallas import tpu as pltpu
from jax.sharding import PartitionSpec as P


def smallest(points, pnorm, cents):
    cnorm = jnp.sum(jnp.square(cents.astype(jnp.float32)), axis=1)
    dots = lax.dot_general(
        points, cents, (((1,), (1,)), ((), ())), preferred_element_type=jnp.float32
    )
    return jnp.min((pnorm[:, None] - 2.0 * dots + cnorm[None, :]) / points.shape[1], axis=1)


def block_min(values):
    return lax.pmin(values, "cent")


def renew(part_sums, part_counts, own_rows):
    return ((part_sums + own_rows.astype(jnp.float32)) / (part_counts[:, None] + 1.0)).astype(
        jnp.bfloat16
    )


def per_device(points, centroids, assign):
    blocksize = centroids.shape[0]
    count_pts = points.shape[0]
    pnorm = jnp.sum(jnp.square(points.astype(jnp.float32)), axis=1)
    first = smallest(points, pnorm, centroids)
    first = block_min(first)
    relative = assign - lax.axis_index("cent") * blocksize
    share = blocksize // lax.axis_size("rows")
    own = lax.dynamic_slice_in_dim(centroids, lax.axis_index("rows") * share, share, 0)
    rows_count = lax.axis_size("rows")
    groups = rows_count * lax.axis_size("cent")
    capacity = max(2, 2 * count_pts // groups)
    inside = (relative >= 0) & (relative < blocksize)
    owners = jnp.where(inside, relative // share, rows_count)
    offsets = jnp.where(inside, relative - relative // share * share, 0)
    owner_hot = owners[:, None] == lax.broadcasted_iota(jnp.int32, (count_pts, rows_count), 1)
    earlier = lax.broadcasted_iota(jnp.int32, (count_pts, count_pts), 1) < lax.broadcasted_iota(
        jnp.int32, (count_pts, count_pts), 0
    )
    before = jnp.dot(
        earlier.astype(jnp.bfloat16),
        owner_hot.astype(jnp.bfloat16),
        preferred_element_type=jnp.float32,
    )
    ranking = jnp.sum(jnp.where(owner_hot, before, 0.0), axis=1).astype(jnp.int32)
    slot_index = jnp.where(inside, owners * capacity + ranking, -1)
    placing = (
        lax.broadcasted_iota(jnp.int32, (rows_count * capacity, count_pts), 0)
        == slot_index[None, :]
    )
    outgoing = jnp.dot(
        placing.astype(jnp.bfloat16), points, preferred_element_type=jnp.float32
    ).astype(jnp.bfloat16)
    labels = (jnp.sum(jnp.where(placing, offsets[None, :] + 1, 0), axis=1) - 1).astype(jnp.bfloat16)
    arrived, arrived_labels = (
        lax.all_to_all(outgoing, "rows", split_axis=0, concat_axis=0, tiled=True),
        lax.all_to_all(labels, "rows", split_axis=0, concat_axis=0, tiled=True),
    )
    chosen = (
        lax.broadcasted_iota(jnp.int32, (share, arrived.shape[0]), 0)
        == arrived_labels.astype(jnp.int32)[None, :]
    )
    part_sums = jnp.dot(chosen.astype(jnp.bfloat16), arrived, preferred_element_type=jnp.float32)
    part_counts = jnp.sum(chosen.astype(jnp.float32), axis=1)
    updated = lax.all_gather(renew(part_sums, part_counts, own), "rows", axis=0, tiled=True)
    second = smallest(points, pnorm, updated)
    nearest = jnp.stack([first, block_min(second)])
    return (nearest, updated)


PLANE = 4
LANES = 128
VMEM_BYTES = 44 * 1024 * 1024
PARTS = 2
TALL = ((64, 32), (0, 0))


def nt_dot(a, b):
    return lax.dot_general(a, b, (((1,), (1,)), ((), ())), preferred_element_type=jnp.float32)


def column_min(cents, points):
    wide = cents.astype(jnp.float32)
    cnorm = jnp.sum(wide * wide, axis=1, keepdims=True)
    return jnp.min(cnorm - 2.0 * nt_dot(cents, points), axis=0, keepdims=True)


def flip(index, bits):
    low, high = index % 2, index // 2
    if bits % 2:
        low = 1 - low
    if bits // 2:
        high = 1 - high
    return high * 2 + low


def lloyd_kernel(
    rows, cap, share, assign_hbm, points_hbm, cents_hbm, near_ref, gath,
    assign_ref, points_ref, cents_ref, load_sem,
    placing_ref, send, lab_send, arrived, lab_arrived, klab,
    part_send, meta_send, part_got, meta_got, part_in, meta_in, held, tally, mine, theirs, low,
    sent_pts, got_pts, sent_lab, got_lab, sent_part, got_part, sent_meta, got_in,
    sent_gath, sent_col, sent_tall, got_col, got_tall, got_side, got_diag, spare_sem, sent_min, got_min,
):
    count_pts, width = points_ref.shape
    blocksize = cents_ref.shape[0]
    planes = rows // PLANE
    wide = width // PARTS
    chunk = planes * cap
    me = lax.axis_index("rows")
    core = lax.axis_index("cent")
    z, q = me // PLANE, me % PLANE
    xpeer = z * PLANE + flip(q, 1)
    ypeer = z * PLANE + flip(q, 2)
    diag = z * PLANE + flip(q, 3)
    partner = 1 - core

    assign_in = pltpu.make_async_copy(assign_hbm, assign_ref, load_sem.at[2])
    assign_in.start()
    points_in = pltpu.make_async_copy(points_hbm, points_ref, load_sem.at[0])
    points_in.start()
    barrier = pltpu.get_barrier_semaphore()
    for bits in range(1, 4):
        pl.semaphore_signal(barrier, inc=1, device_id={"rows": z * PLANE + flip(q, bits)})
        pl.semaphore_signal(barrier, inc=1, device_id={"rows": flip(z, bits) * PLANE + q})
    pl.semaphore_signal(barrier, inc=1, device_id={"cent": partner})

    assign_in.wait()
    relative = (assign_ref[...] - core * blocksize).astype(jnp.float32)
    inside = (relative >= 0.0) & (relative < float(blocksize))
    owner = jnp.where(inside, jnp.floor(relative * (1.0 / share)), float(rows))
    offset1 = jnp.where(inside, relative - owner * share + 1.0, 0.0)
    hot = lax.broadcasted_iota(jnp.int32, (rows, count_pts), 0).astype(jnp.float32) == owner
    hot_f = jnp.where(hot, 1.0, 0.0)
    seg = 256
    tri = jnp.where(
        lax.broadcasted_iota(jnp.int32, (seg, seg), 0) < lax.broadcasted_iota(jnp.int32, (seg, seg), 1),
        1.0, 0.0,
    ).astype(jnp.bfloat16)
    carry = jnp.zeros((rows, 1), jnp.float32)
    pieces = []
    for s in range(count_pts // seg):
        part = hot_f[:, s * seg:(s + 1) * seg]
        before = jnp.dot(part.astype(jnp.bfloat16), tri, preferred_element_type=jnp.float32) + carry
        pieces.append(jnp.sum(part * before, axis=0, keepdims=True))
        carry = carry + jnp.sum(part, axis=1, keepdims=True)
    ranking = jnp.concatenate(pieces, axis=1)
    side_to = jnp.floor(owner * (1.0 / (2 * PLANE)))
    pair_to = jnp.floor(owner * 0.5)
    column_to, lane_to = pair_to - side_to * PLANE, side_to * 2.0 + owner - pair_to * 2.0
    slot = jnp.where(inside, column_to * chunk + lane_to * cap + ranking, -1.0)
    labels8 = jnp.broadcast_to(offset1, (8, count_pts)).astype(jnp.bfloat16)

    def ship(src, dst, ss, rs, axis, target):
        copy = pltpu.make_async_remote_copy(
            src_ref=src, dst_ref=dst, send_sem=ss, recv_sem=rs, device_id={axis: target}
        )
        copy.start()
        return copy

    def landed(ref, sem):
        pltpu.make_async_remote_copy(
            src_ref=ref, dst_ref=ref, send_sem=spare_sem.at[0], recv_sem=sem, device_id={"rows": xpeer}
        ).wait_recv()

    def sent_all(ref, sem):
        pltpu.make_async_remote_copy(
            src_ref=ref, dst_ref=ref, send_sem=sem, recv_sem=spare_sem.at[0], device_id={"rows": xpeer}
        ).wait_send()

    reach = (3, 1, 2)
    side = z // 2
    inner = (z > 0) & (z < planes - 1)
    outer = jnp.logical_not(inner)
    beside, across = flip(z, 1) * PLANE + q, (planes - 1 - z) * PLANE + q
    order = (2 - 2 * side, 3 - 2 * side, 2 * side, 2 * side + 1)

    def place(k):
        i = flip(q, k)
        hit = (
            lax.broadcasted_iota(jnp.int32, (chunk, count_pts), 0) + i * chunk
        ).astype(jnp.float32) == slot
        placing = jnp.where(hit, 1.0, 0.0).astype(jnp.bfloat16)
        placing_ref[k] = placing
        lab = nt_dot(labels8, placing)
        for t in range(chunk // LANES):
            piece = lab[:, t * LANES:(t + 1) * LANES]
            if k:
                lab_send[k, t] = piece
            else:
                lab_arrived[q, t] = piece

    def fill(h, k):
        rows_out = jnp.dot(
            placing_ref[k], points_ref[:, h * wide:(h + 1) * wide], preferred_element_type=jnp.float32
        ).astype(jnp.bfloat16)
        if k:
            send[h, k] = rows_out
        else:
            for t in range(planes):
                arrived[h, t, pl.ds(pl.multiple_of(q * cap, cap), cap), :] = rows_out[t * cap:(t + 1) * cap]

    def dispatch(h, j, k):
        t = order[j]
        spot = pl.ds(pl.multiple_of(q * cap, cap), cap)
        ship(
            send.at[h, k, pl.ds(pl.multiple_of(t * cap, cap), cap)], arrived.at[h, t, spot],
            sent_pts.at[0], got_pts.at[h, t], "rows", z * PLANE + flip(q, k),
        )

    place(reach[0])
    points_in.wait()
    cents_in = pltpu.make_async_copy(cents_hbm, cents_ref, load_sem.at[1])
    cents_in.start()
    for k in reach:
        if k != reach[0]:
            place(k)
        fill(0, k)
        if k == reach[0]:
            pl.semaphore_wait(barrier, 7)
        ship(
            lab_send.at[k], lab_arrived.at[q], sent_lab.at[0], got_lab.at[0], "rows", z * PLANE + flip(q, k)
        )
        dispatch(0, 0, k)
    for j in range(1, planes):
        for k in reach:
            dispatch(0, j, k)
    for h in range(1, PARTS):
        for k in reach:
            fill(h, k)
        for j in range(planes):
            for k in reach:
                dispatch(h, j, k)
    place(0)
    for h in range(PARTS):
        fill(h, 0)

    kb = 512
    pieces_first = blocksize // kb
    low[...] = jnp.full(low.shape, jnp.inf, jnp.float32)
    min_copies = []

    def first_piece(i):
        low[0:1, :] = jnp.minimum(low[0:1, :], column_min(cents_ref[i * kb:(i + 1) * kb, :], points_ref[...]))

    def point_norms():
        squares = jnp.square(points_ref[...].astype(jnp.float32))
        high = squares.astype(jnp.bfloat16)
        rest = (squares - high.astype(jnp.float32)).astype(jnp.bfloat16)
        ones = jnp.ones((8, width), jnp.bfloat16)
        return (nt_dot(ones, high) + nt_dot(ones, rest))[0:1, :]

    landed(lab_arrived.at[0:PLANE - 1], got_lab.at[0])
    lane = lax.broadcasted_iota(jnp.int32, (8, LANES), 1)
    for t in range(planes):
        for p in range(PLANE // 2):
            left, right = lab_arrived[2 * p, t // 2], lab_arrived[2 * p + 1, t // 2]
            if t % 2:
                left = pltpu.roll(left, cap, 1)
            else:
                right = pltpu.roll(right, cap, 1)
            klab[t, :, p * LANES:(p + 1) * LANES] = jnp.where(lane < cap, left, right)

    rowid1 = lax.broadcasted_iota(jnp.int32, (share, PLANE * cap), 0).astype(jnp.float32) + 1.0
    eye = lax.broadcasted_iota(jnp.int32, (share, LANES), 0) == lax.broadcasted_iota(
        jnp.int32, (share, LANES), 1
    )

    def to_row(column):
        return jnp.sum(jnp.where(eye, column, 0.0), axis=0, keepdims=True)

    def to_column(row):
        return jnp.sum(jnp.where(eye, row, 0.0), axis=1, keepdims=True)

    def gather_in(h, t):
        landed(arrived.at[h, t, 0:(PLANE - 1) * cap], got_pts.at[h, t])
        chosen = jnp.where(rowid1 == klab[t][0:1, :], 1.0, 0.0)
        counts = jnp.sum(chosen, axis=1, keepdims=True)
        total = jnp.dot(chosen.astype(jnp.bfloat16), arrived[h, t], preferred_element_type=jnp.float32)
        return total, counts

    def send_part(h, j, total, counts, part_to, meta_to, got, target):
        peak = jnp.maximum(jnp.max(jnp.abs(total), axis=1, keepdims=True), 1e-30)
        grow = jnp.exp2(14.0 - jnp.floor(jnp.log2(peak)))
        grow = jnp.where(peak * grow >= 32767.0, grow * 0.5, grow)
        scaled = jnp.clip(jnp.round(total * grow), -32767.0, 32767.0)
        part_send[h, j] = scaled.astype(jnp.int32).astype(jnp.int16)
        first_row = lax.broadcasted_iota(jnp.int32, (8, LANES), 0) == 0
        meta_send[h, j] = jnp.where(first_row, to_row(1.0 / grow), to_row(counts))
        ship(meta_send.at[h, j], meta_to, sent_meta.at[0], got.at[1], "rows", target)
        ship(part_send.at[h, j], part_to, sent_part.at[0], got.at[0], "rows", target)

    def take_part(part_from, meta_from, got):
        landed(meta_from, got.at[1])
        landed(part_from, got.at[0])
        meta = meta_from[...]
        return part_from[...].astype(jnp.int32).astype(jnp.float32) * to_column(meta[0:1, :]), to_column(meta[1:2, :])

    def reduce_in(h, j):
        t = order[j]
        total, counts = gather_in(h, t)

        @pl.when(outer)
        def _():
            send_part(h, j, total, counts, part_got.at[h, t], meta_got.at[h, t], got_part.at[h, t], beside)

        @pl.when(inner)
        def _():
            held[h, j] = total
            tally[h, j] = counts

    def reduce_far(h, j):
        @pl.when(inner)
        def _():
            t = order[j]
            more, extra = take_part(part_got.at[h, t], meta_got.at[h, t], got_part.at[h, t])
            send_part(
                h, j, held[h, j] + more, tally[h, j] + extra, part_in.at[h, j], meta_in.at[h, j], got_in.at[h, j], across
            )

    def renew(h):
        @pl.when(inner)
        def _():
            for p in range(2):
                block, t = side * 2 * PLANE + 2 * q + p, order[2 + p]
                rows_own = cents_ref[pl.ds(pl.multiple_of(block * share, share), share), h * wide:(h + 1) * wide]
                total, counts = held[h, 2 + p] + rows_own.astype(jnp.float32), tally[h, 2 + p]
                more, extra = take_part(part_got.at[h, t], meta_got.at[h, t], got_part.at[h, t])
                total, counts = total + more, counts + extra
                more, extra = take_part(part_in.at[h, p], meta_in.at[h, p], got_in.at[h, p])
                total, counts = total + more, counts + extra
                gath[block, :, h * wide:(h + 1) * wide] = (total / (counts + 1.0)).astype(jnp.bfloat16)

    def sides(n):
        return (side, 1 - side)[n]

    def cols(h):
        return slice(h * wide, (h + 1) * wide)

    def pair(h, n, mate, first=0, count=share):
        return gath.at[pl.ds(sides(n) * 2 * PLANE + 2 * (mate % PLANE), 2), pl.ds(first, count), cols(h)]

    def one(h, n, mate, p, first=0, count=share):
        return gath.at[sides(n) * 2 * PLANE + 2 * (mate % PLANE) + p, pl.ds(first, count), cols(h)]

    def pile(h, blocks, count):
        return gath.at[0:blocks, pl.ds(0, count), cols(h)]

    def flat(h, n, within):
        if within:
            return share - TALL[h][0] * n
        return share - TALL[h][1]

    def pass_on(h, n, within):
        for p in range(2):
            part = one(h, n, me, p, 0, flat(h, n, within))
            for target in (xpeer, ypeer):
                ship(part, part, sent_gath.at[h], got_side.at[h, n, p], "rows", target)

    def own_start(h):
        for p in range(2):
            part = one(h, 0, me, p)
            ship(part, part, sent_col.at[h], got_col.at[h, 1, p], "rows", across)
            ship(part, part, sent_col.at[h], got_col.at[h, 0, p], "rows", beside)

    def column_in(h, n, within):
        for p in range(2):
            part = one(h, n, me, p)
            landed(part, got_col.at[h, n, p])
            if within:
                ship(part, part, sent_col.at[h], got_col.at[h, n, p], "rows", beside)

    def cross(h, n, within):
        count = flat(h, n, within)
        for p in range(2):
            landed(pile(h, 2, count), got_side.at[h, n, p])
            for mate, first, target in ((ypeer, 0, xpeer), (xpeer, count // 2, ypeer)):
                part = one(h, n, mate, p, first, count // 2)
                ship(part, part, sent_gath.at[h], got_diag.at[h, n], "rows", target)

    def spread_tall(h, n, within):
        near, far = TALL[h][1], TALL[h][0]
        if not within or n:
            landed(pile(h, 6, far if within else near), got_tall.at[h, n])
        if within:
            for mate in (xpeer, ypeer, diag):
                if n == 0:
                    part = pair(h, n, mate, share - far, far)
                    ship(part, part, sent_tall.at[h], got_tall.at[h, 1], "rows", across)
            if n:
                tall_out(h, n)

    def tall_out(h, n):
        near = TALL[h][1]
        for mate in (xpeer, ypeer, diag):
            part = pair(h, n, mate, share - near, near)
            ship(part, part, sent_tall.at[h], got_tall.at[h, n], "rows", beside)

    def run(within, steps):
        missing = {}
        for n in range(2):
            missing[n, "q"] = 1 + (n and not within)
            for kind in "xyd":
                missing[n, kind] = PARTS + (0 if within and n == 0 else sum(1 for r in TALL if r[0]))

        def settle(n, kinds):
            for kind in kinds:
                missing[n, kind] -= 1
                if missing[n, kind] == 0:
                    mate = {"q": me, "x": xpeer, "y": ypeer, "d": diag}[kind]
                    first = sides(n) * 2 * PLANE + 2 * (mate % PLANE)
                    block = jnp.concatenate([gath[first], gath[first + 1]], axis=0)
                    low[1:2, :] = jnp.minimum(low[1:2, :], column_min(block, points_ref[...]))

        for what, h, n in steps:
            if what == "S":
                own_start(h)
                settle(n, "q")
            elif what == "I":
                column_in(h, n, within)
                settle(n, "q")
            elif what == "P":
                pass_on(h, n, within)
            elif what == "X":
                cross(h, n, within)
                settle(n, "xy")
            elif what == "D":
                landed(pile(h, 2, flat(h, n, within)), got_diag.at[h, n])
                settle(n, "d")
            elif what == "U":
                tall_out(h, n)
            else:
                spread_tall(h, n, within)
                if not (within and n == 0):
                    settle(n, "xyd")

    cents_in.wait()
    reduce_in(0, 0)
    first_piece(0)
    reduce_in(0, 1)
    first_piece(1)
    reduce_far(0, 0)
    reduce_in(0, 2)
    first_piece(2)
    reduce_far(0, 1)
    reduce_in(0, 3)
    for i in range(planes - 1, pieces_first):
        first_piece(i)
    renew(0)

    @pl.when(inner)
    def _():
        own_start(0)
        pass_on(0, 0, True)

    reduce_in(1, 0)
    pnorm = point_norms()
    mine[0] = (pnorm + low[0:1, :]) / width
    min_copies.append(ship(mine.at[0], theirs.at[0], sent_min.at[0], got_min.at[0], "cent", partner))
    reduce_in(1, 1)
    reduce_far(1, 0)
    reduce_in(1, 2)
    reduce_far(1, 1)

    @pl.when(inner)
    def _():
        column_in(0, 1, True)
        pass_on(0, 1, True)

    reduce_in(1, 3)

    @pl.when(outer)
    def _():
        column_in(0, 0, False)
        pass_on(0, 0, False)

    renew(1)

    @pl.when(inner)
    def _():
        run(True, (
            ("S", 1, 0), ("X", 0, 0), ("P", 1, 0), ("D", 0, 0), ("T", 0, 0), ("I", 1, 1), ("U", 0, 0), ("P", 1, 1),
            ("X", 1, 0), ("X", 0, 1), ("T", 0, 1), ("D", 1, 0), ("D", 0, 1), ("X", 1, 1), ("D", 1, 1),
        ))

    @pl.when(outer)
    def _():
        run(False, (
            ("I", 0, 1), ("P", 0, 1), ("X", 0, 0), ("I", 1, 0), ("P", 1, 0), ("X", 0, 1), ("I", 1, 1), ("P", 1, 1),
            ("D", 0, 0), ("X", 1, 0), ("T", 0, 0), ("D", 0, 1), ("X", 1, 1), ("D", 1, 0), ("T", 0, 1), ("D", 1, 1),
        ))

    mine[1] = (pnorm + low[1:2, :]) / width
    min_copies.append(ship(mine.at[1], theirs.at[1], sent_min.at[1], got_min.at[1], "cent", partner))
    sent_all(send.at[:, 1:], sent_pts.at[0])
    sent_all(lab_send.at[1:], sent_lab.at[0])

    @pl.when(outer)
    def _():
        sent_all(part_send, sent_part.at[0])
        sent_all(meta_send, sent_meta.at[0])
        for h in range(PARTS):
            sent_all(pile(h, 3 * PLANE, flat(h, 0, False)), sent_gath.at[h])

    @pl.when(inner)
    def _():
        sent_all(part_send.at[:, 0:2], sent_part.at[0])
        sent_all(meta_send.at[:, 0:2], sent_meta.at[0])
        for h in range(PARTS):
            sent_all(pile(h, 3 * PLANE, (share + flat(h, 1, True)) // 2), sent_gath.at[h])
            sent_all(pile(h, 6, share), sent_col.at[h])
            if TALL[h][0]:
                sent_all(pile(h, 6, TALL[h][0] + 2 * TALL[h][1]), sent_tall.at[h])

    for n, copy in enumerate(min_copies):
        copy.wait()
        near_ref[n:n + 1, :] = jnp.minimum(mine[n], theirs[n])


def deliver(near_ref, gath_ref, near_out, upd_out, sems):
    copies = [
        pltpu.make_async_copy(gath_ref, upd_out, sems.at[0]),
        pltpu.make_async_copy(near_ref, near_out, sems.at[1]),
    ]
    for copy in copies:
        copy.start()
    for copy in copies:
        copy.wait()


def fused(points, centroids, assign, rows, cap, share):
    count_pts, width = points.shape
    planes = rows // PLANE
    hbm = pl.BlockSpec(memory_space=pltpu.HBM)
    vmem = pl.BlockSpec(memory_space=pltpu.VMEM)
    dma = pltpu.SemaphoreType.DMA
    chunk = planes * cap
    wide = width // PARTS
    shapes = (
        jax.ShapeDtypeStruct((2, count_pts), jnp.float32),
        jax.ShapeDtypeStruct((rows, share, width), jnp.bfloat16),
    )
    near, upd = pl.pallas_call(
        functools.partial(lloyd_kernel, rows, cap, share),
        out_shape=shapes,
        in_specs=[hbm, hbm, hbm],
        out_specs=(vmem, vmem),
        scratch_shapes=[
            pltpu.VMEM((1, count_pts), jnp.int32),
            pltpu.VMEM((count_pts, width), jnp.bfloat16),
            pltpu.VMEM(centroids.shape, jnp.bfloat16),
            dma((3,)),
            pltpu.VMEM((PLANE, chunk, count_pts), jnp.bfloat16),
            pltpu.VMEM((PARTS, PLANE, chunk, wide), jnp.bfloat16),
            pltpu.VMEM((PLANE, chunk // LANES, 8, LANES), jnp.float32),
            pltpu.VMEM((PARTS, planes, PLANE * cap, wide), jnp.bfloat16),
            pltpu.VMEM((PLANE, chunk // LANES, 8, LANES), jnp.float32),
            pltpu.VMEM((planes, 8, PLANE * cap), jnp.float32),
            pltpu.VMEM((PARTS, planes, share, wide), jnp.int16),
            pltpu.VMEM((PARTS, planes, 8, LANES), jnp.float32),
            pltpu.VMEM((PARTS, planes, share, wide), jnp.int16),
            pltpu.VMEM((PARTS, planes, 8, LANES), jnp.float32),
            pltpu.VMEM((PARTS, 2, share, wide), jnp.int16),
            pltpu.VMEM((PARTS, 2, 8, LANES), jnp.float32),
            pltpu.VMEM((PARTS, planes, share, wide), jnp.float32),
            pltpu.VMEM((PARTS, planes, share, 1), jnp.float32),
            pltpu.VMEM((2, 1, count_pts), jnp.float32),
            pltpu.VMEM((2, 1, count_pts), jnp.float32),
            pltpu.VMEM((8, count_pts), jnp.float32),
            dma((1,)), dma((PARTS, planes)), dma((1,)), dma((1,)),
            dma((1,)), dma((PARTS, planes, 2)), dma((1,)), dma((PARTS, 2, 2)),
            dma((PARTS,)), dma((PARTS,)), dma((PARTS,)),
            dma((PARTS, 2, 2)), dma((PARTS, 2)), dma((PARTS, 2, 2)), dma((PARTS, 2)),
            dma((1,)), dma((2,)), dma((2,)),
        ],
        compiler_params=pltpu.CompilerParams(
            collective_id=0, has_side_effects=True, vmem_limit_bytes=VMEM_BYTES
        ),
    )(
        pltpu.with_memory_space_constraint(assign[None, :], pltpu.HBM),
        pltpu.with_memory_space_constraint(points, pltpu.HBM),
        pltpu.with_memory_space_constraint(centroids, pltpu.HBM),
    )
    near, upd = pl.pallas_call(
        deliver,
        out_shape=shapes,
        in_specs=[vmem, vmem],
        out_specs=(hbm, hbm),
        scratch_shapes=[dma((2,))],
        compiler_params=pltpu.CompilerParams(vmem_limit_bytes=1024 * 1024),
    )(near, upd)
    return near, upd.reshape(rows * share, width)


def step(rows, cent, points, centroids, assign):
    count_pts = points.shape[0]
    blocksize = centroids.shape[0]
    share = blocksize // rows
    cap = max(2, 2 * count_pts // (rows * cent))
    fits = cent == 2 and rows == 4 * PLANE and share == LANES and 2 * cap == LANES
    even = count_pts % 256 == 0 and blocksize % 512 == 0 and points.shape[1] % (PARTS * LANES) == 0
    if fits and even:
        return fused(points, centroids, assign, rows, cap, share)
    return per_device(points, centroids, assign)


def solution(mesh):
    return jax.shard_map(
        functools.partial(step, mesh.shape["rows"], mesh.shape["cent"]),
        mesh=mesh,
        in_specs=(P("rows", None), P("cent", None), P("rows")),
        out_specs=(P(None, "rows"), P("cent", None)),
        check_vma=False,
    )
```

```python
import functools

import jax
import jax.numpy as jnp
from jax import lax
from jax.experimental import pallas as pl
from jax.experimental.pallas import tpu as pltpu
from jax.sharding import PartitionSpec as P


def smallest(points, pnorm, cents):
    cnorm = jnp.sum(jnp.square(cents.astype(jnp.float32)), axis=1)
    dots = lax.dot_general(
        points, cents, (((1,), (1,)), ((), ())), preferred_element_type=jnp.float32
    )
    return jnp.min((pnorm[:, None] - 2.0 * dots + cnorm[None, :]) / points.shape[1], axis=1)


def block_min(values):
    return lax.pmin(values, "cent")


def renew(part_sums, part_counts, own_rows):
    return ((part_sums + own_rows.astype(jnp.float32)) / (part_counts[:, None] + 1.0)).astype(
        jnp.bfloat16
    )


def per_device(points, centroids, assign):
    blocksize = centroids.shape[0]
    count_pts = points.shape[0]
    pnorm = jnp.sum(jnp.square(points.astype(jnp.float32)), axis=1)
    first = smallest(points, pnorm, centroids)
    first = block_min(first)
    relative = assign - lax.axis_index("cent") * blocksize
    share = blocksize // lax.axis_size("rows")
    own = lax.dynamic_slice_in_dim(centroids, lax.axis_index("rows") * share, share, 0)
    rows_count = lax.axis_size("rows")
    groups = rows_count * lax.axis_size("cent")
    capacity = max(2, 2 * count_pts // groups)
    inside = (relative >= 0) & (relative < blocksize)
    owners = jnp.where(inside, relative // share, rows_count)
    offsets = jnp.where(inside, relative - relative // share * share, 0)
    owner_hot = owners[:, None] == lax.broadcasted_iota(jnp.int32, (count_pts, rows_count), 1)
    earlier = lax.broadcasted_iota(jnp.int32, (count_pts, count_pts), 1) < lax.broadcasted_iota(
        jnp.int32, (count_pts, count_pts), 0
    )
    before = jnp.dot(
        earlier.astype(jnp.bfloat16),
        owner_hot.astype(jnp.bfloat16),
        preferred_element_type=jnp.float32,
    )
    ranking = jnp.sum(jnp.where(owner_hot, before, 0.0), axis=1).astype(jnp.int32)
    slot_index = jnp.where(inside, owners * capacity + ranking, -1)
    placing = (
        lax.broadcasted_iota(jnp.int32, (rows_count * capacity, count_pts), 0)
        == slot_index[None, :]
    )
    outgoing = jnp.dot(
        placing.astype(jnp.bfloat16), points, preferred_element_type=jnp.float32
    ).astype(jnp.bfloat16)
    labels = (jnp.sum(jnp.where(placing, offsets[None, :] + 1, 0), axis=1) - 1).astype(jnp.bfloat16)
    arrived, arrived_labels = (
        lax.all_to_all(outgoing, "rows", split_axis=0, concat_axis=0, tiled=True),
        lax.all_to_all(labels, "rows", split_axis=0, concat_axis=0, tiled=True),
    )
    chosen = (
        lax.broadcasted_iota(jnp.int32, (share, arrived.shape[0]), 0)
        == arrived_labels.astype(jnp.int32)[None, :]
    )
    part_sums = jnp.dot(chosen.astype(jnp.bfloat16), arrived, preferred_element_type=jnp.float32)
    part_counts = jnp.sum(chosen.astype(jnp.float32), axis=1)
    updated = lax.all_gather(renew(part_sums, part_counts, own), "rows", axis=0, tiled=True)
    second = smallest(points, pnorm, updated)
    nearest = jnp.stack([first, block_min(second)])
    return (nearest, updated)


PLANE = 4
LANES = 128
VMEM_BYTES = 44 * 1024 * 1024
PARTS = 2
TALL = ((64, 32), (0, 0))


def nt_dot(a, b):
    return lax.dot_general(a, b, (((1,), (1,)), ((), ())), preferred_element_type=jnp.float32)


def column_min(cents, points):
    wide = cents.astype(jnp.float32)
    cnorm = jnp.sum(wide * wide, axis=1, keepdims=True)
    return jnp.min(cnorm - 2.0 * nt_dot(cents, points), axis=0, keepdims=True)


def flip(index, bits):
    low, high = index % 2, index // 2
    if bits % 2:
        low = 1 - low
    if bits // 2:
        high = 1 - high
    return high * 2 + low


def lloyd_kernel(
    rows, cap, share, assign_hbm, points_hbm, cents_hbm, near_ref, gath,
    assign_ref, points_ref, cents_ref, load_sem,
    placing_ref, send, lab_send, arrived, lab_arrived, klab,
    part_send, meta_send, part_got, meta_got, part_in, meta_in, held, tally, mine, theirs, low,
    sent_pts, got_pts, sent_lab, got_lab, sent_part, got_part, sent_meta, got_in,
    sent_gath, sent_col, sent_tall, got_col, got_tall, got_side, got_diag, spare_sem, sent_min, got_min,
):
    count_pts, width = points_ref.shape
    blocksize = cents_ref.shape[0]
    planes = rows // PLANE
    wide = width // PARTS
    chunk = planes * cap
    me = lax.axis_index("rows")
    core = lax.axis_index("cent")
    z, q = me // PLANE, me % PLANE
    xpeer = z * PLANE + flip(q, 1)
    ypeer = z * PLANE + flip(q, 2)
    diag = z * PLANE + flip(q, 3)
    partner = 1 - core

    assign_in = pltpu.make_async_copy(assign_hbm, assign_ref, load_sem.at[2])
    assign_in.start()
    points_in = pltpu.make_async_copy(points_hbm, points_ref, load_sem.at[0])
    points_in.start()
    barrier = pltpu.get_barrier_semaphore()
    for bits in range(1, 4):
        pl.semaphore_signal(barrier, inc=1, device_id={"rows": z * PLANE + flip(q, bits)})
        pl.semaphore_signal(barrier, inc=1, device_id={"rows": flip(z, bits) * PLANE + q})
    pl.semaphore_signal(barrier, inc=1, device_id={"cent": partner})

    assign_in.wait()
    relative = (assign_ref[...] - core * blocksize).astype(jnp.float32)
    inside = (relative >= 0.0) & (relative < float(blocksize))
    owner = jnp.where(inside, jnp.floor(relative * (1.0 / share)), float(rows))
    offset1 = jnp.where(inside, relative - owner * share + 1.0, 0.0)
    hot = lax.broadcasted_iota(jnp.int32, (rows, count_pts), 0).astype(jnp.float32) == owner
    hot_f = jnp.where(hot, 1.0, 0.0)
    seg = 256
    tri = jnp.where(
        lax.broadcasted_iota(jnp.int32, (seg, seg), 0) < lax.broadcasted_iota(jnp.int32, (seg, seg), 1),
        1.0, 0.0,
    ).astype(jnp.bfloat16)
    carry = jnp.zeros((rows, 1), jnp.float32)
    pieces = []
    for s in range(count_pts // seg):
        part = hot_f[:, s * seg:(s + 1) * seg]
        before = jnp.dot(part.astype(jnp.bfloat16), tri, preferred_element_type=jnp.float32) + carry
        pieces.append(jnp.sum(part * before, axis=0, keepdims=True))
        carry = carry + jnp.sum(part, axis=1, keepdims=True)
    ranking = jnp.concatenate(pieces, axis=1)
    side_to = jnp.floor(owner * (1.0 / (2 * PLANE)))
    pair_to = jnp.floor(owner * 0.5)
    column_to, lane_to = pair_to - side_to * PLANE, side_to * 2.0 + owner - pair_to * 2.0
    slot = jnp.where(inside, column_to * chunk + lane_to * cap + ranking, -1.0)
    labels8 = jnp.broadcast_to(offset1, (8, count_pts)).astype(jnp.bfloat16)

    def ship(src, dst, ss, rs, axis, target):
        copy = pltpu.make_async_remote_copy(
            src_ref=src, dst_ref=dst, send_sem=ss, recv_sem=rs, device_id={axis: target}
        )
        copy.start()
        return copy

    def landed(ref, sem):
        pltpu.make_async_remote_copy(
            src_ref=ref, dst_ref=ref, send_sem=spare_sem.at[0], recv_sem=sem, device_id={"rows": xpeer}
        ).wait_recv()

    def sent_all(ref, sem):
        pltpu.make_async_remote_copy(
            src_ref=ref, dst_ref=ref, send_sem=sem, recv_sem=spare_sem.at[0], device_id={"rows": xpeer}
        ).wait_send()

    reach = (3, 1, 2)
    side = z // 2
    inner = (z > 0) & (z < planes - 1)
    outer = jnp.logical_not(inner)
    beside, across = flip(z, 1) * PLANE + q, (planes - 1 - z) * PLANE + q
    order = (2 - 2 * side, 3 - 2 * side, 2 * side, 2 * side + 1)

    def place(k):
        i = flip(q, k)
        hit = (
            lax.broadcasted_iota(jnp.int32, (chunk, count_pts), 0) + i * chunk
        ).astype(jnp.float32) == slot
        placing = jnp.where(hit, 1.0, 0.0).astype(jnp.bfloat16)
        placing_ref[k] = placing
        lab = nt_dot(labels8, placing)
        for t in range(chunk // LANES):
            piece = lab[:, t * LANES:(t + 1) * LANES]
            if k:
                lab_send[k, t] = piece
            else:
                lab_arrived[q, t] = piece

    def fill(h, k):
        rows_out = jnp.dot(
            placing_ref[k], points_ref[:, h * wide:(h + 1) * wide], preferred_element_type=jnp.float32
        ).astype(jnp.bfloat16)
        if k:
            send[h, k] = rows_out
        else:
            for t in range(planes):
                arrived[h, t, pl.ds(pl.multiple_of(q * cap, cap), cap), :] = rows_out[t * cap:(t + 1) * cap]

    def dispatch(h, j, k):
        t = order[j]
        spot = pl.ds(pl.multiple_of(q * cap, cap), cap)
        ship(
            send.at[h, k, pl.ds(pl.multiple_of(t * cap, cap), cap)], arrived.at[h, t, spot],
            sent_pts.at[0], got_pts.at[h, t], "rows", z * PLANE + flip(q, k),
        )

    place(reach[0])
    points_in.wait()
    cents_in = pltpu.make_async_copy(cents_hbm, cents_ref, load_sem.at[1])
    cents_in.start()
    for k in reach:
        if k != reach[0]:
            place(k)
        fill(0, k)
        if k == reach[0]:
            pl.semaphore_wait(barrier, 7)
        ship(
            lab_send.at[k], lab_arrived.at[q], sent_lab.at[0], got_lab.at[0], "rows", z * PLANE + flip(q, k)
        )
        dispatch(0, 0, k)
    for j in range(1, planes):
        for k in reach:
            dispatch(0, j, k)
    for h in range(1, PARTS):
        for k in reach:
            fill(h, k)
        for j in range(planes):
            for k in reach:
                dispatch(h, j, k)
    place(0)
    for h in range(PARTS):
        fill(h, 0)

    kb = 512
    pieces_first = blocksize // kb
    low[...] = jnp.full(low.shape, jnp.inf, jnp.float32)
    min_copies = []

    def first_piece(i):
        low[0:1, :] = jnp.minimum(low[0:1, :], column_min(cents_ref[i * kb:(i + 1) * kb, :], points_ref[...]))

    def point_norms():
        squares = jnp.square(points_ref[...].astype(jnp.float32))
        high = squares.astype(jnp.bfloat16)
        rest = (squares - high.astype(jnp.float32)).astype(jnp.bfloat16)
        ones = jnp.ones((8, width), jnp.bfloat16)
        return (nt_dot(ones, high) + nt_dot(ones, rest))[0:1, :]

    landed(lab_arrived.at[0:PLANE - 1], got_lab.at[0])
    lane = lax.broadcasted_iota(jnp.int32, (8, LANES), 1)
    for t in range(planes):
        for p in range(PLANE // 2):
            left, right = lab_arrived[2 * p, t // 2], lab_arrived[2 * p + 1, t // 2]
            if t % 2:
                left = pltpu.roll(left, cap, 1)
            else:
                right = pltpu.roll(right, cap, 1)
            klab[t, :, p * LANES:(p + 1) * LANES] = jnp.where(lane < cap, left, right)

    rowid1 = lax.broadcasted_iota(jnp.int32, (share, PLANE * cap), 0).astype(jnp.float32) + 1.0
    eye = lax.broadcasted_iota(jnp.int32, (share, LANES), 0) == lax.broadcasted_iota(
        jnp.int32, (share, LANES), 1
    )

    def to_row(column):
        return jnp.sum(jnp.where(eye, column, 0.0), axis=0, keepdims=True)

    def to_column(row):
        return jnp.sum(jnp.where(eye, row, 0.0), axis=1, keepdims=True)

    def gather_in(h, t):
        landed(arrived.at[h, t, 0:(PLANE - 1) * cap], got_pts.at[h, t])
        chosen = jnp.where(rowid1 == klab[t][0:1, :], 1.0, 0.0)
        counts = jnp.sum(chosen, axis=1, keepdims=True)
        total = jnp.dot(chosen.astype(jnp.bfloat16), arrived[h, t], preferred_element_type=jnp.float32)
        return total, counts

    def send_part(h, j, total, counts, part_to, meta_to, got, target):
        peak = jnp.maximum(jnp.max(jnp.abs(total), axis=1, keepdims=True), 1e-30)
        grow = jnp.exp2(14.0 - jnp.floor(jnp.log2(peak)))
        grow = jnp.where(peak * grow >= 32767.0, grow * 0.5, grow)
        scaled = jnp.clip(jnp.round(total * grow), -32767.0, 32767.0)
        part_send[h, j] = scaled.astype(jnp.int32).astype(jnp.int16)
        first_row = lax.broadcasted_iota(jnp.int32, (8, LANES), 0) == 0
        meta_send[h, j] = jnp.where(first_row, to_row(1.0 / grow), to_row(counts))
        ship(meta_send.at[h, j], meta_to, sent_meta.at[0], got.at[1], "rows", target)
        ship(part_send.at[h, j], part_to, sent_part.at[0], got.at[0], "rows", target)

    def take_part(part_from, meta_from, got):
        landed(meta_from, got.at[1])
        landed(part_from, got.at[0])
        meta = meta_from[...]
        return part_from[...].astype(jnp.int32).astype(jnp.float32) * to_column(meta[0:1, :]), to_column(meta[1:2, :])

    def reduce_in(h, j):
        t = order[j]
        total, counts = gather_in(h, t)

        @pl.when(outer)
        def _():
            send_part(h, j, total, counts, part_got.at[h, t], meta_got.at[h, t], got_part.at[h, t], beside)

        @pl.when(inner)
        def _():
            held[h, j] = total
            tally[h, j] = counts

    def reduce_far(h, j):
        @pl.when(inner)
        def _():
            t = order[j]
            more, extra = take_part(part_got.at[h, t], meta_got.at[h, t], got_part.at[h, t])
            send_part(
                h, j, held[h, j] + more, tally[h, j] + extra, part_in.at[h, j], meta_in.at[h, j], got_in.at[h, j], across
            )

    def renew(h):
        @pl.when(inner)
        def _():
            for p in range(2):
                block, t = side * 2 * PLANE + 2 * q + p, order[2 + p]
                rows_own = cents_ref[pl.ds(pl.multiple_of(block * share, share), share), h * wide:(h + 1) * wide]
                total, counts = held[h, 2 + p] + rows_own.astype(jnp.float32), tally[h, 2 + p]
                more, extra = take_part(part_got.at[h, t], meta_got.at[h, t], got_part.at[h, t])
                total, counts = total + more, counts + extra
                more, extra = take_part(part_in.at[h, p], meta_in.at[h, p], got_in.at[h, p])
                total, counts = total + more, counts + extra
                gath[block, :, h * wide:(h + 1) * wide] = (total / (counts + 1.0)).astype(jnp.bfloat16)

    def sides(n):
        return (side, 1 - side)[n]

    def cols(h):
        return slice(h * wide, (h + 1) * wide)

    def pair(h, n, mate, first=0, count=share):
        return gath.at[pl.ds(sides(n) * 2 * PLANE + 2 * (mate % PLANE), 2), pl.ds(first, count), cols(h)]

    def one(h, n, mate, p, first=0, count=share):
        return gath.at[sides(n) * 2 * PLANE + 2 * (mate % PLANE) + p, pl.ds(first, count), cols(h)]

    def pile(h, blocks, count):
        return gath.at[0:blocks, pl.ds(0, count), cols(h)]

    def flat(h, n, within):
        if within:
            return share - TALL[h][0] * n
        return share - TALL[h][1]

    def pass_block(h, n, p, within):
        part = one(h, n, me, p, 0, flat(h, n, within))
        for target in (xpeer, ypeer):
            ship(part, part, sent_gath.at[h], got_side.at[h, n, p], "rows", target)

    def pass_on(h, n, within):
        for p in range(2):
            pass_block(h, n, p, within)

    def own_start(h):
        for p in range(2):
            part = one(h, 0, me, p)
            ship(part, part, sent_col.at[h], got_col.at[h, 1, p], "rows", across)
            ship(part, part, sent_col.at[h], got_col.at[h, 0, p], "rows", beside)

    def column_in(h, n, within):
        for p in range(2):
            part = one(h, n, me, p)
            landed(part, got_col.at[h, n, p])
            if within:
                ship(part, part, sent_col.at[h], got_col.at[h, n, p], "rows", beside)
            pass_block(h, n, p, within)

    def cross(h, n, within):
        count = flat(h, n, within)
        for p in range(2):
            landed(pile(h, 2, count), got_side.at[h, n, p])
            for mate, first, target in ((ypeer, 0, xpeer), (xpeer, count // 2, ypeer)):
                part = one(h, n, mate, p, first, count // 2)
                ship(part, part, sent_gath.at[h], got_diag.at[h, n], "rows", target)

    def spread_tall(h, n, within):
        near, far = TALL[h][1], TALL[h][0]
        if not within or n:
            landed(pile(h, 6, far if within else near), got_tall.at[h, n])
        if within:
            for mate in (xpeer, ypeer, diag):
                if n == 0:
                    part = pair(h, n, mate, share - far, far)
                    ship(part, part, sent_tall.at[h], got_tall.at[h, 1], "rows", across)
            if n:
                tall_out(h, n)

    def tall_out(h, n):
        near = TALL[h][1]
        for mate in (xpeer, ypeer, diag):
            part = pair(h, n, mate, share - near, near)
            ship(part, part, sent_tall.at[h], got_tall.at[h, n], "rows", beside)

    def run(within, steps):
        missing = {}
        for n in range(2):
            missing[n, "q"] = 1 + (n and not within)
            for kind in "xyd":
                missing[n, kind] = PARTS + (0 if within and n == 0 else sum(1 for r in TALL if r[0]))

        def settle(n, kinds):
            for kind in kinds:
                missing[n, kind] -= 1
                if missing[n, kind] == 0:
                    mate = {"q": me, "x": xpeer, "y": ypeer, "d": diag}[kind]
                    first = sides(n) * 2 * PLANE + 2 * (mate % PLANE)
                    block = jnp.concatenate([gath[first], gath[first + 1]], axis=0)
                    low[1:2, :] = jnp.minimum(low[1:2, :], column_min(block, points_ref[...]))

        for what, h, n in steps:
            if what == "S":
                own_start(h)
                settle(n, "q")
            elif what == "I":
                column_in(h, n, within)
                settle(n, "q")
            elif what == "P":
                pass_on(h, n, within)
            elif what == "X":
                cross(h, n, within)
                settle(n, "xy")
            elif what == "D":
                landed(pile(h, 2, flat(h, n, within)), got_diag.at[h, n])
                settle(n, "d")
            elif what == "U":
                tall_out(h, n)
            else:
                spread_tall(h, n, within)
                if not (within and n == 0):
                    settle(n, "xyd")

    cents_in.wait()
    reduce_in(0, 0)
    first_piece(0)
    reduce_in(0, 1)
    first_piece(1)
    reduce_far(0, 0)
    reduce_in(0, 2)
    first_piece(2)
    reduce_far(0, 1)
    reduce_in(0, 3)
    for i in range(planes - 1, pieces_first):
        first_piece(i)
    renew(0)

    @pl.when(inner)
    def _():
        own_start(0)
        pass_on(0, 0, True)

    reduce_in(1, 0)
    pnorm = point_norms()
    mine[0] = (pnorm + low[0:1, :]) / width
    min_copies.append(ship(mine.at[0], theirs.at[0], sent_min.at[0], got_min.at[0], "cent", partner))
    reduce_in(1, 1)
    reduce_far(1, 0)
    reduce_in(1, 2)
    reduce_far(1, 1)

    @pl.when(inner)
    def _():
        column_in(0, 1, True)

    reduce_in(1, 3)

    @pl.when(outer)
    def _():
        column_in(0, 0, False)

    renew(1)

    @pl.when(inner)
    def _():
        run(True, (
            ("S", 1, 0), ("X", 0, 0), ("P", 1, 0), ("D", 0, 0), ("T", 0, 0), ("I", 1, 1), ("U", 0, 0), ("X", 1, 0),
            ("X", 0, 1), ("T", 0, 1), ("D", 1, 0), ("D", 0, 1), ("X", 1, 1), ("D", 1, 1),
        ))

    @pl.when(outer)
    def _():
        run(False, (
            ("I", 0, 1), ("X", 0, 0), ("I", 1, 0), ("X", 0, 1), ("I", 1, 1), ("X", 1, 0), ("X", 1, 1), ("T", 0, 0),
            ("D", 0, 0), ("D", 0, 1), ("T", 0, 1), ("D", 1, 0), ("D", 1, 1),
        ))

    mine[1] = (pnorm + low[1:2, :]) / width
    min_copies.append(ship(mine.at[1], theirs.at[1], sent_min.at[1], got_min.at[1], "cent", partner))
    sent_all(send.at[:, 1:], sent_pts.at[0])
    sent_all(lab_send.at[1:], sent_lab.at[0])

    @pl.when(outer)
    def _():
        sent_all(part_send, sent_part.at[0])
        sent_all(meta_send, sent_meta.at[0])
        for h in range(PARTS):
            sent_all(pile(h, 3 * PLANE, flat(h, 0, False)), sent_gath.at[h])

    @pl.when(inner)
    def _():
        sent_all(part_send.at[:, 0:2], sent_part.at[0])
        sent_all(meta_send.at[:, 0:2], sent_meta.at[0])
        for h in range(PARTS):
            sent_all(pile(h, 3 * PLANE, (share + flat(h, 1, True)) // 2), sent_gath.at[h])
            sent_all(pile(h, 6, share), sent_col.at[h])
            if TALL[h][0]:
                sent_all(pile(h, 6, TALL[h][0] + 2 * TALL[h][1]), sent_tall.at[h])

    for n, copy in enumerate(min_copies):
        copy.wait()
        near_ref[n:n + 1, :] = jnp.minimum(mine[n], theirs[n])


def deliver(near_ref, gath_ref, near_out, upd_out, sems):
    copies = [
        pltpu.make_async_copy(gath_ref, upd_out, sems.at[0]),
        pltpu.make_async_copy(near_ref, near_out, sems.at[1]),
    ]
    for copy in copies:
        copy.start()
    for copy in copies:
        copy.wait()


def fused(points, centroids, assign, rows, cap, share):
    count_pts, width = points.shape
    planes = rows // PLANE
    hbm = pl.BlockSpec(memory_space=pltpu.HBM)
    vmem = pl.BlockSpec(memory_space=pltpu.VMEM)
    dma = pltpu.SemaphoreType.DMA
    chunk = planes * cap
    wide = width // PARTS
    shapes = (
        jax.ShapeDtypeStruct((2, count_pts), jnp.float32),
        jax.ShapeDtypeStruct((rows, share, width), jnp.bfloat16),
    )
    near, upd = pl.pallas_call(
        functools.partial(lloyd_kernel, rows, cap, share),
        out_shape=shapes,
        in_specs=[hbm, hbm, hbm],
        out_specs=(vmem, vmem),
        scratch_shapes=[
            pltpu.VMEM((1, count_pts), jnp.int32),
            pltpu.VMEM((count_pts, width), jnp.bfloat16),
            pltpu.VMEM(centroids.shape, jnp.bfloat16),
            dma((3,)),
            pltpu.VMEM((PLANE, chunk, count_pts), jnp.bfloat16),
            pltpu.VMEM((PARTS, PLANE, chunk, wide), jnp.bfloat16),
            pltpu.VMEM((PLANE, chunk // LANES, 8, LANES), jnp.float32),
            pltpu.VMEM((PARTS, planes, PLANE * cap, wide), jnp.bfloat16),
            pltpu.VMEM((PLANE, chunk // LANES, 8, LANES), jnp.float32),
            pltpu.VMEM((planes, 8, PLANE * cap), jnp.float32),
            pltpu.VMEM((PARTS, planes, share, wide), jnp.int16),
            pltpu.VMEM((PARTS, planes, 8, LANES), jnp.float32),
            pltpu.VMEM((PARTS, planes, share, wide), jnp.int16),
            pltpu.VMEM((PARTS, planes, 8, LANES), jnp.float32),
            pltpu.VMEM((PARTS, 2, share, wide), jnp.int16),
            pltpu.VMEM((PARTS, 2, 8, LANES), jnp.float32),
            pltpu.VMEM((PARTS, planes, share, wide), jnp.float32),
            pltpu.VMEM((PARTS, planes, share, 1), jnp.float32),
            pltpu.VMEM((2, 1, count_pts), jnp.float32),
            pltpu.VMEM((2, 1, count_pts), jnp.float32),
            pltpu.VMEM((8, count_pts), jnp.float32),
            dma((1,)), dma((PARTS, planes)), dma((1,)), dma((1,)),
            dma((1,)), dma((PARTS, planes, 2)), dma((1,)), dma((PARTS, 2, 2)),
            dma((PARTS,)), dma((PARTS,)), dma((PARTS,)),
            dma((PARTS, 2, 2)), dma((PARTS, 2)), dma((PARTS, 2, 2)), dma((PARTS, 2)),
            dma((1,)), dma((2,)), dma((2,)),
        ],
        compiler_params=pltpu.CompilerParams(
            collective_id=0, has_side_effects=True, vmem_limit_bytes=VMEM_BYTES
        ),
    )(
        pltpu.with_memory_space_constraint(assign[None, :], pltpu.HBM),
        pltpu.with_memory_space_constraint(points, pltpu.HBM),
        pltpu.with_memory_space_constraint(centroids, pltpu.HBM),
    )
    near, upd = pl.pallas_call(
        deliver,
        out_shape=shapes,
        in_specs=[vmem, vmem],
        out_specs=(hbm, hbm),
        scratch_shapes=[dma((2,))],
        compiler_params=pltpu.CompilerParams(vmem_limit_bytes=1024 * 1024),
    )(near, upd)
    return near, upd.reshape(rows * share, width)


def step(rows, cent, points, centroids, assign):
    count_pts = points.shape[0]
    blocksize = centroids.shape[0]
    share = blocksize // rows
    cap = max(2, 2 * count_pts // (rows * cent))
    fits = cent == 2 and rows == 4 * PLANE and share == LANES and 2 * cap == LANES
    even = count_pts % 256 == 0 and blocksize % 512 == 0 and points.shape[1] % (PARTS * LANES) == 0
    if fits and even:
        return fused(points, centroids, assign, rows, cap, share)
    return per_device(points, centroids, assign)


def solution(mesh):
    return jax.shard_map(
        functools.partial(step, mesh.shape["rows"], mesh.shape["cent"]),
        mesh=mesh,
        in_specs=(P("rows", None), P("cent", None), P("rows")),
        out_specs=(P(None, "rows"), P("cent", None)),
        check_vma=False,
    )
```

```python
import functools

import jax
import jax.numpy as jnp
from jax import lax
from jax.experimental import pallas as pl
from jax.experimental.pallas import tpu as pltpu
from jax.sharding import PartitionSpec as P


def smallest(points, pnorm, cents):
    cnorm = jnp.sum(jnp.square(cents.astype(jnp.float32)), axis=1)
    dots = lax.dot_general(
        points, cents, (((1,), (1,)), ((), ())), preferred_element_type=jnp.float32
    )
    return jnp.min((pnorm[:, None] - 2.0 * dots + cnorm[None, :]) / points.shape[1], axis=1)


def block_min(values):
    return lax.pmin(values, "cent")


def renew(part_sums, part_counts, own_rows):
    return ((part_sums + own_rows.astype(jnp.float32)) / (part_counts[:, None] + 1.0)).astype(
        jnp.bfloat16
    )


def per_device(points, centroids, assign):
    blocksize = centroids.shape[0]
    count_pts = points.shape[0]
    pnorm = jnp.sum(jnp.square(points.astype(jnp.float32)), axis=1)
    first = smallest(points, pnorm, centroids)
    first = block_min(first)
    relative = assign - lax.axis_index("cent") * blocksize
    share = blocksize // lax.axis_size("rows")
    own = lax.dynamic_slice_in_dim(centroids, lax.axis_index("rows") * share, share, 0)
    rows_count = lax.axis_size("rows")
    groups = rows_count * lax.axis_size("cent")
    capacity = max(2, 2 * count_pts // groups)
    inside = (relative >= 0) & (relative < blocksize)
    owners = jnp.where(inside, relative // share, rows_count)
    offsets = jnp.where(inside, relative - relative // share * share, 0)
    owner_hot = owners[:, None] == lax.broadcasted_iota(jnp.int32, (count_pts, rows_count), 1)
    earlier = lax.broadcasted_iota(jnp.int32, (count_pts, count_pts), 1) < lax.broadcasted_iota(
        jnp.int32, (count_pts, count_pts), 0
    )
    before = jnp.dot(
        earlier.astype(jnp.bfloat16),
        owner_hot.astype(jnp.bfloat16),
        preferred_element_type=jnp.float32,
    )
    ranking = jnp.sum(jnp.where(owner_hot, before, 0.0), axis=1).astype(jnp.int32)
    slot_index = jnp.where(inside, owners * capacity + ranking, -1)
    placing = (
        lax.broadcasted_iota(jnp.int32, (rows_count * capacity, count_pts), 0)
        == slot_index[None, :]
    )
    outgoing = jnp.dot(
        placing.astype(jnp.bfloat16), points, preferred_element_type=jnp.float32
    ).astype(jnp.bfloat16)
    labels = (jnp.sum(jnp.where(placing, offsets[None, :] + 1, 0), axis=1) - 1).astype(jnp.bfloat16)
    arrived, arrived_labels = (
        lax.all_to_all(outgoing, "rows", split_axis=0, concat_axis=0, tiled=True),
        lax.all_to_all(labels, "rows", split_axis=0, concat_axis=0, tiled=True),
    )
    chosen = (
        lax.broadcasted_iota(jnp.int32, (share, arrived.shape[0]), 0)
        == arrived_labels.astype(jnp.int32)[None, :]
    )
    part_sums = jnp.dot(chosen.astype(jnp.bfloat16), arrived, preferred_element_type=jnp.float32)
    part_counts = jnp.sum(chosen.astype(jnp.float32), axis=1)
    updated = lax.all_gather(renew(part_sums, part_counts, own), "rows", axis=0, tiled=True)
    second = smallest(points, pnorm, updated)
    nearest = jnp.stack([first, block_min(second)])
    return (nearest, updated)


PLANE = 4
LANES = 128
VMEM_BYTES = 44 * 1024 * 1024
PARTS = 2
TALL = ((64, 32), (0, 0))


def nt_dot(a, b):
    return lax.dot_general(a, b, (((1,), (1,)), ((), ())), preferred_element_type=jnp.float32)


def column_min(cents, points):
    wide = cents.astype(jnp.float32)
    cnorm = jnp.sum(wide * wide, axis=1, keepdims=True)
    return jnp.min(cnorm - 2.0 * nt_dot(cents, points), axis=0, keepdims=True)


def flip(index, bits):
    low, high = index % 2, index // 2
    if bits % 2:
        low = 1 - low
    if bits // 2:
        high = 1 - high
    return high * 2 + low


def lloyd_kernel(
    rows, cap, share, assign_hbm, points_hbm, cents_hbm, near_ref, gath,
    assign_ref, points_ref, cents_ref, load_sem,
    placing_ref, send, lab_send, arrived, lab_arrived, klab,
    part_send, meta_send, part_got, meta_got, part_in, meta_in, held, tally, mine, theirs, low,
    sent_pts, got_pts, sent_lab, got_lab, sent_part, got_part, sent_meta, got_in,
    sent_gath, sent_col, sent_tall, got_col, got_tall, got_side, got_diag, spare_sem, sent_min, got_min,
):
    count_pts, width = points_ref.shape
    blocksize = cents_ref.shape[0]
    planes = rows // PLANE
    wide = width // PARTS
    chunk = planes * cap
    me = lax.axis_index("rows")
    core = lax.axis_index("cent")
    z, q = me // PLANE, me % PLANE
    xpeer = z * PLANE + flip(q, 1)
    ypeer = z * PLANE + flip(q, 2)
    diag = z * PLANE + flip(q, 3)
    partner = 1 - core

    assign_in = pltpu.make_async_copy(assign_hbm, assign_ref, load_sem.at[2])
    assign_in.start()
    points_in = pltpu.make_async_copy(points_hbm, points_ref, load_sem.at[0])
    points_in.start()
    barrier = pltpu.get_barrier_semaphore()
    for bits in range(1, 4):
        pl.semaphore_signal(barrier, inc=1, device_id={"rows": z * PLANE + flip(q, bits)})
        pl.semaphore_signal(barrier, inc=1, device_id={"rows": flip(z, bits) * PLANE + q})
    pl.semaphore_signal(barrier, inc=1, device_id={"cent": partner})

    assign_in.wait()
    relative = (assign_ref[...] - core * blocksize).astype(jnp.float32)
    inside = (relative >= 0.0) & (relative < float(blocksize))
    owner = jnp.where(inside, jnp.floor(relative * (1.0 / share)), float(rows))
    offset1 = jnp.where(inside, relative - owner * share + 1.0, 0.0)
    hot = lax.broadcasted_iota(jnp.int32, (rows, count_pts), 0).astype(jnp.float32) == owner
    hot_f = jnp.where(hot, 1.0, 0.0)
    seg = 256
    tri = jnp.where(
        lax.broadcasted_iota(jnp.int32, (seg, seg), 0) < lax.broadcasted_iota(jnp.int32, (seg, seg), 1),
        1.0, 0.0,
    ).astype(jnp.bfloat16)
    carry = jnp.zeros((rows, 1), jnp.float32)
    pieces = []
    for s in range(count_pts // seg):
        part = hot_f[:, s * seg:(s + 1) * seg]
        before = jnp.dot(part.astype(jnp.bfloat16), tri, preferred_element_type=jnp.float32) + carry
        pieces.append(jnp.sum(part * before, axis=0, keepdims=True))
        carry = carry + jnp.sum(part, axis=1, keepdims=True)
    ranking = jnp.concatenate(pieces, axis=1)
    side_to = jnp.floor(owner * (1.0 / (2 * PLANE)))
    pair_to = jnp.floor(owner * 0.5)
    column_to, lane_to = pair_to - side_to * PLANE, side_to * 2.0 + owner - pair_to * 2.0
    slot = jnp.where(inside, column_to * chunk + lane_to * cap + ranking, -1.0)
    labels8 = jnp.broadcast_to(offset1, (8, count_pts)).astype(jnp.bfloat16)

    def ship(src, dst, ss, rs, axis, target):
        copy = pltpu.make_async_remote_copy(
            src_ref=src, dst_ref=dst, send_sem=ss, recv_sem=rs, device_id={axis: target}
        )
        copy.start()
        return copy

    def landed(ref, sem):
        pltpu.make_async_remote_copy(
            src_ref=ref, dst_ref=ref, send_sem=spare_sem.at[0], recv_sem=sem, device_id={"rows": xpeer}
        ).wait_recv()

    def sent_all(ref, sem):
        pltpu.make_async_remote_copy(
            src_ref=ref, dst_ref=ref, send_sem=sem, recv_sem=spare_sem.at[0], device_id={"rows": xpeer}
        ).wait_send()

    reach = (3, 1, 2)
    side = z // 2
    inner = (z > 0) & (z < planes - 1)
    outer = jnp.logical_not(inner)
    beside, across = flip(z, 1) * PLANE + q, (planes - 1 - z) * PLANE + q
    order = (2 - 2 * side, 3 - 2 * side, 2 * side, 2 * side + 1)

    def place(k):
        i = flip(q, k)
        hit = (
            lax.broadcasted_iota(jnp.int32, (chunk, count_pts), 0) + i * chunk
        ).astype(jnp.float32) == slot
        placing = jnp.where(hit, 1.0, 0.0).astype(jnp.bfloat16)
        placing_ref[k] = placing
        lab = nt_dot(labels8, placing)
        for t in range(chunk // LANES):
            piece = lab[:, t * LANES:(t + 1) * LANES]
            if k:
                lab_send[k, t] = piece
            else:
                lab_arrived[q, t] = piece

    def fill(h, k):
        rows_out = jnp.dot(
            placing_ref[k], points_ref[:, h * wide:(h + 1) * wide], preferred_element_type=jnp.float32
        ).astype(jnp.bfloat16)
        if k:
            send[h, k] = rows_out
        else:
            for t in range(planes):
                arrived[h, t, pl.ds(pl.multiple_of(q * cap, cap), cap), :] = rows_out[t * cap:(t + 1) * cap]

    def dispatch(h, j, k):
        t = order[j]
        spot = pl.ds(pl.multiple_of(q * cap, cap), cap)
        ship(
            send.at[h, k, pl.ds(pl.multiple_of(t * cap, cap), cap)], arrived.at[h, t, spot],
            sent_pts.at[0], got_pts.at[h, t], "rows", z * PLANE + flip(q, k),
        )

    place(reach[0])
    points_in.wait()
    cents_in = pltpu.make_async_copy(cents_hbm, cents_ref, load_sem.at[1])
    cents_in.start()
    for k in reach:
        if k != reach[0]:
            place(k)
        fill(0, k)
        if k == reach[0]:
            pl.semaphore_wait(barrier, 7)
        ship(
            lab_send.at[k], lab_arrived.at[q], sent_lab.at[0], got_lab.at[0], "rows", z * PLANE + flip(q, k)
        )
        dispatch(0, 0, k)
    for j in range(1, planes):
        for k in reach:
            dispatch(0, j, k)
    for h in range(1, PARTS):
        for k in reach:
            fill(h, k)
        for j in range(planes):
            for k in reach:
                dispatch(h, j, k)
    place(0)
    for h in range(PARTS):
        fill(h, 0)

    kb = 512
    pieces_first = blocksize // kb
    low[...] = jnp.full(low.shape, jnp.inf, jnp.float32)
    min_copies = []

    def first_piece(i):
        low[0:1, :] = jnp.minimum(low[0:1, :], column_min(cents_ref[i * kb:(i + 1) * kb, :], points_ref[...]))

    def point_norms():
        squares = jnp.square(points_ref[...].astype(jnp.float32))
        high = squares.astype(jnp.bfloat16)
        rest = (squares - high.astype(jnp.float32)).astype(jnp.bfloat16)
        ones = jnp.ones((8, width), jnp.bfloat16)
        return (nt_dot(ones, high) + nt_dot(ones, rest))[0:1, :]

    landed(lab_arrived.at[0:PLANE - 1], got_lab.at[0])
    lane = lax.broadcasted_iota(jnp.int32, (8, LANES), 1)
    for t in range(planes):
        for p in range(PLANE // 2):
            left, right = lab_arrived[2 * p, t // 2], lab_arrived[2 * p + 1, t // 2]
            if t % 2:
                left = pltpu.roll(left, cap, 1)
            else:
                right = pltpu.roll(right, cap, 1)
            klab[t, :, p * LANES:(p + 1) * LANES] = jnp.where(lane < cap, left, right)

    rowid1 = lax.broadcasted_iota(jnp.int32, (share, PLANE * cap), 0).astype(jnp.float32) + 1.0
    eye = lax.broadcasted_iota(jnp.int32, (share, LANES), 0) == lax.broadcasted_iota(
        jnp.int32, (share, LANES), 1
    )

    def to_row(column):
        return jnp.sum(jnp.where(eye, column, 0.0), axis=0, keepdims=True)

    def to_column(row):
        return jnp.sum(jnp.where(eye, row, 0.0), axis=1, keepdims=True)

    def gather_in(h, t):
        landed(arrived.at[h, t, 0:(PLANE - 1) * cap], got_pts.at[h, t])
        chosen = jnp.where(rowid1 == klab[t][0:1, :], 1.0, 0.0)
        counts = jnp.sum(chosen, axis=1, keepdims=True)
        total = jnp.dot(chosen.astype(jnp.bfloat16), arrived[h, t], preferred_element_type=jnp.float32)
        return total, counts

    def send_part(h, j, total, counts, part_to, meta_to, got, target):
        peak = jnp.maximum(jnp.max(jnp.abs(total), axis=1, keepdims=True), 1e-30)
        grow = jnp.exp2(14.0 - jnp.floor(jnp.log2(peak)))
        grow = jnp.where(peak * grow >= 32767.0, grow * 0.5, grow)
        scaled = jnp.clip(jnp.round(total * grow), -32767.0, 32767.0)
        part_send[h, j] = scaled.astype(jnp.int32).astype(jnp.int16)
        first_row = lax.broadcasted_iota(jnp.int32, (8, LANES), 0) == 0
        meta_send[h, j] = jnp.where(first_row, to_row(1.0 / grow), to_row(counts))
        ship(meta_send.at[h, j], meta_to, sent_meta.at[0], got.at[1], "rows", target)
        ship(part_send.at[h, j], part_to, sent_part.at[0], got.at[0], "rows", target)

    def take_part(part_from, meta_from, got):
        landed(meta_from, got.at[1])
        landed(part_from, got.at[0])
        meta = meta_from[...]
        return part_from[...].astype(jnp.int32).astype(jnp.float32) * to_column(meta[0:1, :]), to_column(meta[1:2, :])

    def reduce_in(h, j):
        t = order[j]
        total, counts = gather_in(h, t)

        @pl.when(outer)
        def _():
            send_part(h, j, total, counts, part_got.at[h, t], meta_got.at[h, t], got_part.at[h, t], beside)

        @pl.when(inner)
        def _():
            held[h, j] = total
            tally[h, j] = counts

    def reduce_far(h, j):
        @pl.when(inner)
        def _():
            t = order[j]
            more, extra = take_part(part_got.at[h, t], meta_got.at[h, t], got_part.at[h, t])
            send_part(
                h, j, held[h, j] + more, tally[h, j] + extra, part_in.at[h, j], meta_in.at[h, j], got_in.at[h, j], across
            )

    def renew(h):
        @pl.when(inner)
        def _():
            for p in range(2):
                block, t = side * 2 * PLANE + 2 * q + p, order[2 + p]
                rows_own = cents_ref[pl.ds(pl.multiple_of(block * share, share), share), h * wide:(h + 1) * wide]
                total, counts = held[h, 2 + p] + rows_own.astype(jnp.float32), tally[h, 2 + p]
                more, extra = take_part(part_got.at[h, t], meta_got.at[h, t], got_part.at[h, t])
                total, counts = total + more, counts + extra
                more, extra = take_part(part_in.at[h, p], meta_in.at[h, p], got_in.at[h, p])
                total, counts = total + more, counts + extra
                gath[block, :, h * wide:(h + 1) * wide] = (total / (counts + 1.0)).astype(jnp.bfloat16)

    def sides(n):
        return (side, 1 - side)[n]

    def cols(h):
        return slice(h * wide, (h + 1) * wide)

    def pair(h, n, mate, first=0, count=share):
        return gath.at[pl.ds(sides(n) * 2 * PLANE + 2 * (mate % PLANE), 2), pl.ds(first, count), cols(h)]

    def one(h, n, mate, p, first=0, count=share):
        return gath.at[sides(n) * 2 * PLANE + 2 * (mate % PLANE) + p, pl.ds(first, count), cols(h)]

    def pile(h, blocks, count):
        return gath.at[0:blocks, pl.ds(0, count), cols(h)]

    def flat(h, n, within):
        if within:
            return share - TALL[h][0] * n
        return share - TALL[h][1]

    def pass_block(h, n, p, within):
        part = one(h, n, me, p, 0, flat(h, n, within))
        for target in (xpeer, ypeer):
            ship(part, part, sent_gath.at[h], got_side.at[h, n, p], "rows", target)

    def pass_on(h, n, within):
        for p in range(2):
            pass_block(h, n, p, within)

    def own_start(h):
        for p in range(2):
            part = one(h, 0, me, p)
            ship(part, part, sent_col.at[h], got_col.at[h, 1, p], "rows", across)
            ship(part, part, sent_col.at[h], got_col.at[h, 0, p], "rows", beside)

    def column_in(h, n, within):
        for p in range(2):
            part = one(h, n, me, p)
            landed(part, got_col.at[h, n, p])
            if within:
                ship(part, part, sent_col.at[h], got_col.at[h, n, p], "rows", beside)
            pass_block(h, n, p, within)

    def cross(h, n, within):
        count = flat(h, n, within)
        for p in range(2):
            landed(pile(h, 2, count), got_side.at[h, n, p])
            for mate, first, target in ((ypeer, 0, xpeer), (xpeer, count // 2, ypeer)):
                part = one(h, n, mate, p, first, count // 2)
                ship(part, part, sent_gath.at[h], got_diag.at[h, n], "rows", target)

    def spread_tall(h, n, within):
        near, far = TALL[h][1], TALL[h][0]
        if not within or n:
            landed(pile(h, 6, far if within else near), got_tall.at[h, n])
        if within:
            for mate in (xpeer, ypeer, diag):
                if n == 0:
                    part = pair(h, n, mate, share - far, far)
                    ship(part, part, sent_tall.at[h], got_tall.at[h, 1], "rows", across)
            if n:
                tall_out(h, n)

    def tall_out(h, n):
        near = TALL[h][1]
        for mate in (xpeer, ypeer, diag):
            part = pair(h, n, mate, share - near, near)
            ship(part, part, sent_tall.at[h], got_tall.at[h, n], "rows", beside)

    def run(within, steps):
        missing = {}
        for n in range(2):
            missing[n, "q"] = 1 + (n and not within)
            for kind in "xyd":
                missing[n, kind] = PARTS + (0 if within and n == 0 else sum(1 for r in TALL if r[0]))

        def settle(n, kinds):
            for kind in kinds:
                missing[n, kind] -= 1
                if missing[n, kind] == 0:
                    mate = {"q": me, "x": xpeer, "y": ypeer, "d": diag}[kind]
                    first = sides(n) * 2 * PLANE + 2 * (mate % PLANE)
                    block = jnp.concatenate([gath[first], gath[first + 1]], axis=0)
                    low[1:2, :] = jnp.minimum(low[1:2, :], column_min(block, points_ref[...]))

        for what, h, n in steps:
            if what == "S":
                own_start(h)
                settle(n, "q")
            elif what == "I":
                column_in(h, n, within)
                settle(n, "q")
            elif what == "P":
                pass_on(h, n, within)
            elif what == "X":
                cross(h, n, within)
                settle(n, "xy")
            elif what == "D":
                landed(pile(h, 2, flat(h, n, within)), got_diag.at[h, n])
                settle(n, "d")
            elif what == "U":
                tall_out(h, n)
            else:
                spread_tall(h, n, within)
                if not (within and n == 0):
                    settle(n, "xyd")

    cents_in.wait()
    reduce_in(0, 0)
    first_piece(0)
    reduce_in(0, 1)
    first_piece(1)
    reduce_far(0, 0)
    reduce_in(0, 2)
    first_piece(2)
    reduce_far(0, 1)
    reduce_in(0, 3)
    for i in range(planes - 1, pieces_first):
        first_piece(i)
    renew(0)

    @pl.when(inner)
    def _():
        own_start(0)
        pass_on(0, 0, True)

    reduce_in(1, 0)
    pnorm = point_norms()
    mine[0] = (pnorm + low[0:1, :]) / width
    min_copies.append(ship(mine.at[0], theirs.at[0], sent_min.at[0], got_min.at[0], "cent", partner))
    reduce_in(1, 1)
    reduce_far(1, 0)
    reduce_in(1, 2)
    reduce_far(1, 1)

    @pl.when(inner)
    def _():
        column_in(0, 1, True)

    reduce_in(1, 3)

    @pl.when(outer)
    def _():
        column_in(0, 0, False)

    renew(1)

    @pl.when(inner)
    def _():
        run(True, (
            ("S", 1, 0), ("X", 0, 0), ("P", 1, 0), ("D", 0, 0), ("T", 0, 0), ("I", 1, 1), ("X", 1, 0), ("U", 0, 0),
            ("X", 0, 1), ("T", 0, 1), ("D", 1, 0), ("D", 0, 1), ("X", 1, 1), ("D", 1, 1),
        ))

    @pl.when(outer)
    def _():
        run(False, (
            ("I", 0, 1), ("X", 0, 0), ("I", 1, 0), ("X", 0, 1), ("I", 1, 1), ("X", 1, 0), ("X", 1, 1), ("T", 0, 0),
            ("D", 0, 0), ("D", 0, 1), ("T", 0, 1), ("D", 1, 0), ("D", 1, 1),
        ))

    mine[1] = (pnorm + low[1:2, :]) / width
    min_copies.append(ship(mine.at[1], theirs.at[1], sent_min.at[1], got_min.at[1], "cent", partner))
    sent_all(send.at[:, 1:], sent_pts.at[0])
    sent_all(lab_send.at[1:], sent_lab.at[0])

    @pl.when(outer)
    def _():
        sent_all(part_send, sent_part.at[0])
        sent_all(meta_send, sent_meta.at[0])
        for h in range(PARTS):
            sent_all(pile(h, 3 * PLANE, flat(h, 0, False)), sent_gath.at[h])

    @pl.when(inner)
    def _():
        sent_all(part_send.at[:, 0:2], sent_part.at[0])
        sent_all(meta_send.at[:, 0:2], sent_meta.at[0])
        for h in range(PARTS):
            sent_all(pile(h, 3 * PLANE, (share + flat(h, 1, True)) // 2), sent_gath.at[h])
            sent_all(pile(h, 6, share), sent_col.at[h])
            if TALL[h][0]:
                sent_all(pile(h, 6, TALL[h][0] + 2 * TALL[h][1]), sent_tall.at[h])

    for n, copy in enumerate(min_copies):
        copy.wait()
        near_ref[n:n + 1, :] = jnp.minimum(mine[n], theirs[n])


def deliver(near_ref, gath_ref, near_out, upd_out, sems):
    copies = [
        pltpu.make_async_copy(gath_ref, upd_out, sems.at[0]),
        pltpu.make_async_copy(near_ref, near_out, sems.at[1]),
    ]
    for copy in copies:
        copy.start()
    for copy in copies:
        copy.wait()


def fused(points, centroids, assign, rows, cap, share):
    count_pts, width = points.shape
    planes = rows // PLANE
    hbm = pl.BlockSpec(memory_space=pltpu.HBM)
    vmem = pl.BlockSpec(memory_space=pltpu.VMEM)
    dma = pltpu.SemaphoreType.DMA
    chunk = planes * cap
    wide = width // PARTS
    shapes = (
        jax.ShapeDtypeStruct((2, count_pts), jnp.float32),
        jax.ShapeDtypeStruct((rows, share, width), jnp.bfloat16),
    )
    near, upd = pl.pallas_call(
        functools.partial(lloyd_kernel, rows, cap, share),
        out_shape=shapes,
        in_specs=[hbm, hbm, hbm],
        out_specs=(vmem, vmem),
        scratch_shapes=[
            pltpu.VMEM((1, count_pts), jnp.int32),
            pltpu.VMEM((count_pts, width), jnp.bfloat16),
            pltpu.VMEM(centroids.shape, jnp.bfloat16),
            dma((3,)),
            pltpu.VMEM((PLANE, chunk, count_pts), jnp.bfloat16),
            pltpu.VMEM((PARTS, PLANE, chunk, wide), jnp.bfloat16),
            pltpu.VMEM((PLANE, chunk // LANES, 8, LANES), jnp.float32),
            pltpu.VMEM((PARTS, planes, PLANE * cap, wide), jnp.bfloat16),
            pltpu.VMEM((PLANE, chunk // LANES, 8, LANES), jnp.float32),
            pltpu.VMEM((planes, 8, PLANE * cap), jnp.float32),
            pltpu.VMEM((PARTS, planes, share, wide), jnp.int16),
            pltpu.VMEM((PARTS, planes, 8, LANES), jnp.float32),
            pltpu.VMEM((PARTS, planes, share, wide), jnp.int16),
            pltpu.VMEM((PARTS, planes, 8, LANES), jnp.float32),
            pltpu.VMEM((PARTS, 2, share, wide), jnp.int16),
            pltpu.VMEM((PARTS, 2, 8, LANES), jnp.float32),
            pltpu.VMEM((PARTS, planes, share, wide), jnp.float32),
            pltpu.VMEM((PARTS, planes, share, 1), jnp.float32),
            pltpu.VMEM((2, 1, count_pts), jnp.float32),
            pltpu.VMEM((2, 1, count_pts), jnp.float32),
            pltpu.VMEM((8, count_pts), jnp.float32),
            dma((1,)), dma((PARTS, planes)), dma((1,)), dma((1,)),
            dma((1,)), dma((PARTS, planes, 2)), dma((1,)), dma((PARTS, 2, 2)),
            dma((PARTS,)), dma((PARTS,)), dma((PARTS,)),
            dma((PARTS, 2, 2)), dma((PARTS, 2)), dma((PARTS, 2, 2)), dma((PARTS, 2)),
            dma((1,)), dma((2,)), dma((2,)),
        ],
        compiler_params=pltpu.CompilerParams(
            collective_id=0, has_side_effects=True, vmem_limit_bytes=VMEM_BYTES
        ),
    )(
        pltpu.with_memory_space_constraint(assign[None, :], pltpu.HBM),
        pltpu.with_memory_space_constraint(points, pltpu.HBM),
        pltpu.with_memory_space_constraint(centroids, pltpu.HBM),
    )
    near, upd = pl.pallas_call(
        deliver,
        out_shape=shapes,
        in_specs=[vmem, vmem],
        out_specs=(hbm, hbm),
        scratch_shapes=[dma((2,))],
        compiler_params=pltpu.CompilerParams(vmem_limit_bytes=1024 * 1024),
    )(near, upd)
    return near, upd.reshape(rows * share, width)


def step(rows, cent, points, centroids, assign):
    count_pts = points.shape[0]
    blocksize = centroids.shape[0]
    share = blocksize // rows
    cap = max(2, 2 * count_pts // (rows * cent))
    fits = cent == 2 and rows == 4 * PLANE and share == LANES and 2 * cap == LANES
    even = count_pts % 256 == 0 and blocksize % 512 == 0 and points.shape[1] % (PARTS * LANES) == 0
    if fits and even:
        return fused(points, centroids, assign, rows, cap, share)
    return per_device(points, centroids, assign)


def solution(mesh):
    return jax.shard_map(
        functools.partial(step, mesh.shape["rows"], mesh.shape["cent"]),
        mesh=mesh,
        in_specs=(P("rows", None), P("cent", None), P("rows")),
        out_specs=(P(None, "rows"), P("cent", None)),
        check_vma=False,
    )
```
